32 devices in a mesh: band: 8 (over z, x), img: 4 (over y, core).
Axes of the slice: x: 2, y: 2, z: 4, core: 2. Of those that a mesh axis runs over, the one named last changes fastest.
Arguments:
- pixels: bfloat16 [256, 256, 180], P(('img', 'band')), parts along dimension 0, may hold values from -12 to 12
- keep_mask: int32 [32, 32], P(('img', 'band')), parts along dimension 0, may hold values from 0 to 1, as said below
- band_counts: int32 [32], P(('img', 'band')), parts along dimension 0, may hold values from 0 to 32, as said below
- plan_dest: int32 [32, 16], P(('img', 'band')), parts along dimension 0, may hold values from 0 to 7, as said below
- plan_slot: int32 [32, 16], P(('img', 'band')), parts along dimension 0, may hold values from 0 to 8, as said below
- bias_table: float32 [225, 6], replicated, may hold values from -4 to 4
- gain_attn: float32 [180], replicated, may hold values from 0.25 to 1.75
- qkv_weight: bfloat16 [180, 540], replicated, may hold values from -5 to 5
- proj_weight: bfloat16 [180, 180], replicated, may hold values from -0.4375 to 0.4375
- gain_mlp: float32 [180], replicated, may hold values from 0.25 to 1.75
- hidden_weight: bfloat16 [180, 360], replicated, may hold values from -0.4375 to 0.4375
- output_weight: bfloat16 [360, 180], replicated, may hold values from -0.3125 to 0.3125
Outputs:
- restored: bfloat16 [256, 256, 180], P(('img', 'band')), parts along dimension 0
- work_tiles: bfloat16 [256, 128, 180], P(('img', 'band')), parts along dimension 0
The draws below stay inside these ranges and needn't reach their ends.
There are 4 independent parts, one for each index of `img`. The reference program is written for one: setup_inputs(seed, part) draws one part's arguments, and reference() takes and returns one part's arrays. A program takes and returns all parts, laid end to end along the dimension named above; an argument that names none is the same for every part. Nothing has to cross between parts.
Inputs may be any that keep to these rules, and one draw needn't show every extreme that they name: `keep_mask`: the number of ones in a band varies strongly from band to band. band_counts[b] equals the number of ones among band b's windows in keep_mask. A band's live tiles are those with 2 t < band_counts[b]; their number summed over bands lies between 57 and 64, and some band has all 16 tiles live. `plan_dest`: within each aligned group of 8 consecutive tiles of a band (equal t // 8) the destinations are all different. `plan_slot`: 8 for tiles that are not live; a live tile has a slot below 8, no two live tiles of the image share destination and slot, and some destination receives 8 live tiles.
All inputs are finite; a program needn't handle non-finite values.
Results may differ from the reference program's by a relative error of at most 0.0044.
Values may be sent and summed in bfloat16 or wider, within the bound.
A program may use at most 64 MiB of HBM per device.

```python
import math
import jax
import jax.numpy as jnp
from jax import lax

CHAN = 180
HEADS = 6
FF_WIDTH = 360
WIN = 8
TILE = 2
ROWS = 8
WIDTH = 256
SHIFT = 4
TABLE = 225
HEIGHT = 64
WIN_DEV = 32
TILES_DEV = 16
CAP = 8
N_BAND = 8


def shuffle_band(band_key):
    return jax.random.permutation(band_key, WIN_DEV)


def plan_tables(key):
    key_perm = jax.random.fold_in(key, 101)
    key_share = jax.random.fold_in(key, 102)
    key_cut = jax.random.fold_in(key, 103)
    key_rest = jax.random.fold_in(key, 104)
    key_rank = jax.random.fold_in(key, 105)
    key_turn = jax.random.fold_in(key, 106)
    half_bands = N_BAND // 2
    band_order = jax.random.permutation(key_perm, N_BAND)
    shares = jax.random.randint(key_share, (half_bands,), 1, TILES_DEV + 1).astype(jnp.int32)
    shares = shares.at[0].set(TILES_DEV)
    trimmed = jax.random.randint(key_cut, (), 0, half_bands)
    pair_ids = jnp.arange(half_bands, dtype=jnp.int32)
    lowered = shares - ((pair_ids >= 1) & (pair_ids <= trimmed)).astype(jnp.int32)
    live_tiles = jnp.zeros((N_BAND,), jnp.int32).at[band_order[0::2]].set(lowered).at[band_order[1::2]].set(TILES_DEV - shares)
    spare_windows = jax.random.randint(key_rest, (N_BAND,), 0, TILE).astype(jnp.int32)
    kept_windows = jnp.where(live_tiles > 0, live_tiles * TILE - spare_windows, 0).astype(jnp.int32)
    window_ranks = jax.vmap(shuffle_band)(jax.random.split(key_rank, N_BAND))
    keep_table = (window_ranks < kept_windows[:, None]).astype(jnp.int32).reshape(HEIGHT // WIN, WIDTH // WIN)
    offsets = (jnp.cumsum(live_tiles) - live_tiles).astype(jnp.int32)
    rotation = jax.random.randint(key_turn, (), 0, N_BAND).astype(jnp.int32)
    tile_ids = jnp.arange(TILES_DEV, dtype=jnp.int32)
    global_tile = offsets[:, None] + tile_ids[None, :]
    dest_table = ((global_tile + rotation) % N_BAND).astype(jnp.int32)
    slot_table = jnp.where(tile_ids[None, :] < live_tiles[:, None], global_tile // N_BAND, CAP).astype(jnp.int32)
    return (keep_table, kept_windows, dest_table, slot_table)


def draw_keep_mask(key, part):
    return plan_tables(key)[0]


def draw_band_counts(key, part):
    return plan_tables(key)[1]


def draw_plan_dest(key, part):
    return plan_tables(key)[2]


def draw_plan_slot(key, part):
    return plan_tables(key)[3]


def draw_pixels(key, part):
    base_key = jax.random.fold_in(key, 201)
    values = jnp.clip(jax.random.normal(base_key, (HEIGHT, WIDTH, CHAN), jnp.float32), -6.0, 6.0)
    return values.astype(jnp.bfloat16)


def draw_qkv_weight(key, part):
    main_key = jax.random.fold_in(key, 301)
    weight = jax.random.normal(main_key, (CHAN, 3 * CHAN), jnp.float32) / math.sqrt(CHAN)
    return jnp.clip(weight, -5.0, 5.0).astype(jnp.bfloat16)


def noise(stream_key, shape, width, reach, kind=jnp.bfloat16):
    values = width * jax.random.normal(stream_key, shape, jnp.float32)
    return jnp.clip(values, min=-reach, max=reach).astype(kind)


def setup_inputs(seed: int = 0, part: int = 0) -> dict:
    seeds = jax.random.split(jax.random.key(seed), 13)
    part_keys = jax.random.split(jax.random.fold_in(seeds[12], part), 13)
    return {
        "pixels": draw_pixels(jax.random.fold_in(jax.random.fold_in(seeds[12], part), 71), part),
        "keep_mask": draw_keep_mask(jax.random.fold_in(jax.random.fold_in(seeds[12], part), 71), part),
        "band_counts": draw_band_counts(jax.random.fold_in(jax.random.fold_in(seeds[12], part), 71), part),
        "plan_dest": draw_plan_dest(jax.random.fold_in(jax.random.fold_in(seeds[12], part), 71), part),
        "plan_slot": draw_plan_slot(jax.random.fold_in(jax.random.fold_in(seeds[12], part), 71), part),
        "bias_table": noise(seeds[5], (TABLE, HEADS), 1.0, 4.0, jnp.float32),
        "gain_attn": jnp.clip(1.0 + 0.15 * jax.random.normal(seeds[6], (CHAN,), jnp.float32), 0.25, 1.75),
        "qkv_weight": draw_qkv_weight(jax.random.fold_in(seeds[12], 71), part),
        "proj_weight": noise(seeds[8], (CHAN, CHAN), CHAN ** -0.5, 0.4375),
        "gain_mlp": jnp.clip(1.0 + 0.15 * jax.random.normal(seeds[9], (CHAN,), jnp.float32), 0.25, 1.75),
        "hidden_weight": noise(seeds[10], (CHAN, FF_WIDTH), CHAN ** -0.5, 0.4375),
        "output_weight": noise(seeds[11], (FF_WIDTH, CHAN), FF_WIDTH ** -0.5, 0.3125),
    }


EPSILON = 1e-05

def layer_norm(values, gain_vec):
    values = values.astype(jnp.float32)
    center = values - lax.optimization_barrier(jnp.mean(values, axis=-1, keepdims=True))
    spread = lax.optimization_barrier(jnp.mean(center * center, axis=-1, keepdims=True))
    return center * lax.rsqrt(spread + EPSILON) * gain_vec

def position_bias(bias_table):
    coords = jnp.arange(WIN * WIN, dtype=jnp.int32)
    row_pos = coords // WIN
    col_pos = coords % WIN
    table_index = (row_pos[:, None] - row_pos[None, :] + WIN - 1) * (2 * WIN - 1) + (col_pos[:, None] - col_pos[None, :] + WIN - 1)
    return jnp.transpose(bias_table[table_index], (2, 0, 1))

def region_codes(first_row, row_count, height, col_count):
    rows_global = first_row + jnp.arange(row_count, dtype=jnp.int32)
    row_region = (rows_global >= height - WIN).astype(jnp.int32) + (rows_global >= height - SHIFT).astype(jnp.int32)
    col_global = jnp.arange(col_count, dtype=jnp.int32)
    col_region = (col_global >= col_count - WIN).astype(jnp.int32) + (col_global >= col_count - SHIFT).astype(jnp.int32)
    return 3 * row_region[:, None] + col_region[None, :]

def attend(windows, window_codes, head_bias, gain_attn, qkv_weight, proj_weight):
    window_count = windows.shape[0]
    head_dim = CHAN // HEADS
    normed = layer_norm(windows, gain_attn).astype(jnp.bfloat16).reshape(-1, CHAN)
    mixed_all = jnp.dot(normed, qkv_weight, preferred_element_type=jnp.float32).reshape(window_count, WIN * WIN, 3, HEADS, head_dim)
    queries = mixed_all[:, :, 0] * head_dim ** (-0.5)
    key_part = mixed_all[:, :, 1]
    value_part = lax.optimization_barrier(mixed_all[:, :, 2].astype(jnp.bfloat16)).astype(jnp.float32)
    scores = jnp.einsum('wqhd,wkhd->whqk', queries, key_part, precision=lax.Precision.HIGHEST)
    differ = window_codes[:, :, None] != window_codes[:, None, :]
    scores = scores + head_bias[None] + jnp.where(differ, -100.0, 0.0)[:, None]
    weights = jax.nn.softmax(scores, axis=-1).astype(jnp.bfloat16)
    weights = lax.optimization_barrier(weights).astype(jnp.float32)
    mixed = jnp.einsum('whqk,wkhd->wqhd', weights, value_part, precision=lax.Precision.HIGHEST)
    mixed = mixed.reshape(-1, CHAN).astype(jnp.bfloat16)
    projected = jnp.dot(mixed, proj_weight, preferred_element_type=jnp.float32)
    summed = windows.reshape(-1, CHAN).astype(jnp.float32) + projected
    return summed.astype(jnp.bfloat16).reshape(window_count, WIN * WIN, CHAN)

def feed(states, gain_mlp, hidden_weight, output_weight):
    flat_rows = states.reshape(-1, CHAN)
    normed = layer_norm(flat_rows, gain_mlp).astype(jnp.bfloat16)
    inner_act = jax.nn.gelu(jnp.dot(normed, hidden_weight, preferred_element_type=jnp.float32)).astype(jnp.bfloat16)
    summed = flat_rows.astype(jnp.float32) + jnp.dot(inner_act, output_weight, preferred_element_type=jnp.float32)
    return summed.astype(jnp.bfloat16).reshape(states.shape)

def reference(pixels, keep_mask, band_counts, plan_dest, plan_slot, bias_table, gain_attn, qkv_weight, proj_weight, gain_mlp, hidden_weight, output_weight):
    height = ROWS * N_BAND
    win_rows = ROWS // WIN
    win_cols = WIDTH // WIN
    shifted = jnp.roll(pixels, (-SHIFT, -SHIFT), axis=(0, 1))
    windows = shifted.reshape(N_BAND, win_rows, WIN, win_cols, WIN, CHAN).transpose(0, 1, 3, 2, 4, 5).reshape(N_BAND, WIN_DEV, WIN * WIN, CHAN)
    region_map = region_codes(0, height, height, WIDTH)
    window_codes = region_map.reshape(N_BAND, win_rows, WIN, win_cols, WIN).transpose(0, 1, 3, 2, 4).reshape(N_BAND, WIN_DEV, WIN * WIN)
    keep_rows = keep_mask.reshape(N_BAND, WIN_DEV)
    head_bias = position_bias(bias_table)

    def one_band(band_inputs):
        band_windows, band_codes, band_keep, band_count = band_inputs
        packed_order = (jnp.cumsum(band_keep) - 1).astype(jnp.int32)
        active = (band_keep == 1) & (packed_order < band_count)
        target = jnp.where(active, packed_order, WIN_DEV).astype(jnp.int32)
        packed = jnp.zeros((WIN_DEV + 1, WIN * WIN, CHAN), jnp.bfloat16).at[target].set(band_windows)[:WIN_DEV]
        packed_codes = jnp.zeros((WIN_DEV + 1, WIN * WIN), jnp.int32).at[target].set(band_codes)[:WIN_DEV]
        attended = attend(packed, packed_codes, head_bias, gain_attn, qkv_weight, proj_weight)
        finished = feed(attended, gain_mlp, hidden_weight, output_weight)
        unpacked = finished[jnp.clip(packed_order, 0, WIN_DEV - 1)]
        result = jnp.where(active[:, None, None], unpacked, band_windows)
        return (result, attended.reshape(TILES_DEV, TILE * WIN * WIN, CHAN))
    results, attended_all = lax.map(one_band, (windows, window_codes, keep_rows, band_counts))
    updated = results.reshape(N_BAND, win_rows, win_cols, WIN, WIN, CHAN).transpose(0, 1, 3, 2, 4, 5).reshape(height, WIDTH, CHAN)
    restored = jnp.roll(updated, (SHIFT, SHIFT), axis=(0, 1))
    tile_ids = jnp.arange(TILES_DEV, dtype=jnp.int32)
    tile_live = (tile_ids[None, :] * TILE < band_counts[:, None]) & (plan_slot < CAP)
    target = jnp.where(tile_live, plan_dest * CAP + plan_slot, N_BAND * CAP).astype(jnp.int32).reshape(-1)
    work_tiles = jnp.zeros((N_BAND * CAP + 1, TILE * WIN * WIN, CHAN), jnp.bfloat16)
    work_tiles = work_tiles.at[target].set(attended_all.reshape(-1, TILE * WIN * WIN, CHAN))[:N_BAND * CAP]
    return (restored, work_tiles)
```

```python
import jax
import jax.numpy as jnp
from jax import lax
from jax.experimental import pallas as pl
from jax.experimental.pallas import tpu as pltpu
from jax.sharding import PartitionSpec as P

CHAN = 180
HEADS = 6
WIN = 8
TILE = 2
SHIFT = 4
CAP = 8
TOK = WIN * WIN
HALF = TOK // 2
HEAD_DIM = CHAN // HEADS
GROUP = 4
LANES = 128
SLOT_LANE = 120

EPSILON = 1e-05
BF = jnp.bfloat16
F32 = jnp.float32


def layer_norm(values, gain_vec):
    center = values - jnp.sum(values, axis=-1, keepdims=True) * (1.0 / CHAN)
    spread = jnp.sum(center * center, axis=-1, keepdims=True) * (1.0 / CHAN)
    return (center * lax.rsqrt(spread + EPSILON) * gain_vec).astype(BF)


def dot(a, b):
    return jnp.dot(a, b, preferred_element_type=F32)


def dot_t(a, b):
    return lax.dot_general(a, b, (((1,), (1,)), ((), ())), preferred_element_type=F32)


def bias_strips(table, strips):
    heads, entries = table.shape
    values = jnp.concatenate([table[...], jnp.zeros((8 - heads, entries), F32)], axis=0)
    high = values.astype(BF).astype(F32)
    middle = (values - high).astype(BF).astype(F32)
    low = values - high - middle
    parts = jnp.concatenate([high, middle, low], axis=0).astype(BF)
    shape = (entries, WIN * LANES)
    entry = lax.broadcasted_iota(jnp.int32, shape, 0)
    lane = lax.broadcasted_iota(jnp.int32, shape, 1)
    step = (lane % LANES) // WIN
    wanted = (2 * WIN - 2 - step) * (2 * WIN - 1) + lane // LANES - lane % WIN + WIN - 1
    pick = jnp.where((entry == wanted) & (step < 2 * WIN - 1), 1.0, 0.0).astype(BF)
    found = dot(parts, pick)
    found = found[0:8] + found[8:16] + found[16:24]
    for c in range(WIN):
        strips[pl.ds(c, 8, stride=WIN), :] = found[:, c * LANES : (c + 1) * LANES]


def bias_base(strips, queries):
    tiles = []
    for h in range(HEADS):
        strip = strips[h * WIN : (h + 1) * WIN, :]
        for r in range(WIN - queries // WIN, WIN):
            by = (WIN - 1 - r) * WIN
            tiles.append(pltpu.roll(strip, (LANES - by) % LANES, 1)[:, :TOK])
    return jnp.concatenate(tiles, axis=0)


def biases(strips, last_row, queries):
    first = TOK - queries
    base = bias_base(strips, queries)
    shape = (HEADS * queries, TOK)
    key = lax.broadcasted_iota(jnp.int32, shape, 1)
    query = lax.broadcasted_iota(jnp.int32, shape, 0) % queries + first
    rows_differ = (key // WIN >= SHIFT) != (query // WIN >= SHIFT)
    cols_differ = (key % WIN >= SHIFT) != (query % WIN >= SHIFT)
    row_pen = jnp.where(rows_differ, jnp.where(last_row, -100.0, 0.0).astype(F32), 0.0)
    plain = base + row_pen
    both = base + jnp.where(cols_differ, -100.0, row_pen)
    return plain, both


def head_masks():
    lane = lax.broadcasted_iota(jnp.int32, (1, CHAN), 1)
    return [
        ((lane >= h * HEAD_DIM) & (lane < (h + 1) * HEAD_DIM)).astype(F32) for h in range(HEADS)
    ]


def attend(x, gain, wq, wk, wv, wp, bias_of, queries):
    masks = head_masks()
    low_masks = [m.astype(BF) for m in masks]
    normed = layer_norm(x, gain)
    if queries == TOK:
        x_q, n_q = x, normed
    else:
        pick = lambda a: jnp.concatenate(
            [a[g * TOK + TOK - queries : (g + 1) * TOK] for g in range(GROUP)], axis=0
        )
        x_q, n_q = pick(x), pick(normed)
    q = (dot(n_q, wq) * HEAD_DIM ** (-0.5)).astype(BF)
    k = dot(normed, wk).astype(BF)
    v = dot(normed, wv).astype(BF)
    mixed = []
    for g in range(GROUP):
        q_w = q[g * queries : (g + 1) * queries]
        stacked = jnp.concatenate([q_w * low_masks[h] for h in range(HEADS)], axis=0)
        scores = dot_t(stacked, k[g * TOK : (g + 1) * TOK]) + bias_of(g)
        top = jnp.max(scores, axis=1, keepdims=True)
        grown = jnp.exp(scores - top)
        weights = (grown * (1.0 / jnp.sum(grown, axis=1, keepdims=True))).astype(BF)
        wide = dot(weights, v[g * TOK : (g + 1) * TOK])
        total = wide[:queries] * masks[0]
        for h in range(1, HEADS):
            total = total + wide[h * queries : (h + 1) * queries] * masks[h]
        mixed.append(total)
    mixed = jnp.concatenate(mixed, axis=0).astype(BF)
    return (x_q + dot(mixed, wp)).astype(BF)


def feed(states, gain, wh, wo):
    flat = states.astype(F32)
    normed = layer_norm(flat, gain)
    inner = jax.nn.gelu(dot(normed, wh)).astype(BF)
    return (flat + dot_t(inner, wo)).astype(BF)


def window_at(image, i, g, row):
    start = pl.multiple_of((i * GROUP + g) * WIN, WIN)
    return image[row : row + WIN, pl.ds(start, WIN), :].reshape(TOK, CHAN)


def group_at(image, i, row):
    return jnp.concatenate([window_at(image, i, g, row) for g in range(GROUP)], axis=0)


def plane_row(planes, row, channels):
    halves = planes.shape[0]
    return jnp.concatenate(
        [planes[h, pl.ds(row, channels, stride=WIN), :] for h in range(halves)], axis=1
    )


def block_kernel(
    keep, count, dests, slots, keep_row, pixels, table, gain_a, wqkv, wp, gain_m, wh, wo,
    restored, incoming,
    planes, image, nxt_out, prv_out, nxt_buf, prv_buf, told, told_buf, weights, strips,
    bias_own, bias_prev, first, rest, upper, result, active, outgoing, following, order,
    halo_send, halo_recv, tile_send, tile_recv,
):
    bands = lax.axis_size("band")
    me = lax.axis_index("band")
    right, left = lax.rem(me + 1, bands), lax.rem(me + bands - 1, bands)
    channels, rows, cols = pixels.shape
    windows = cols // WIN
    groups = windows // GROUP
    halves = cols // LANES
    tiles = windows // TILE
    pairs = -(-tiles // bands)
    span = min(bands, tiles)
    mesh_id = pl.DeviceIdType.MESH

    barrier = pltpu.get_barrier_semaphore()

    def greet(i, _):
        peer = lax.rem(me + i, bands)
        pl.semaphore_signal(barrier, inc=1, device_id={"band": peer}, device_id_type=mesh_id)
        return 0

    lax.fori_loop(1, bands, greet, 0)

    for h in range(halves):
        part = pixels[:, :, h * LANES : (h + 1) * LANES].astype(F32)
        planes[h] = part.reshape(channels * rows, LANES)
    for r in range(SHIFT):
        nxt_out[r] = pltpu.roll(plane_row(planes, r, channels), cols - SHIFT, 1).astype(BF)
    pl.semaphore_wait(barrier, bands - 1)

    def nxt_copy(c):
        part = pl.ds(pl.multiple_of(c * LANES, LANES), LANES)
        return pltpu.make_async_remote_copy(
            src_ref=nxt_out.at[:, :, part],
            dst_ref=nxt_buf.at[:, :, part],
            send_sem=halo_send.at[c],
            recv_sem=halo_recv.at[c],
            device_id={"band": left},
            device_id_type=mesh_id,
        )

    prv_copy = pltpu.make_async_remote_copy(
        src_ref=prv_out,
        dst_ref=prv_buf,
        send_sem=halo_send.at[halves],
        recv_sem=halo_recv.at[halves],
        device_id={"band": right},
        device_id_type=mesh_id,
    )
    told_copy = pltpu.make_async_remote_copy(
        src_ref=told,
        dst_ref=told_buf,
        send_sem=halo_send.at[halves + 1],
        recv_sem=halo_recv.at[halves + 1],
        device_id={"band": right},
        device_id_type=mesh_id,
    )
    for c in range(halves):
        nxt_copy(c).start()

    for r in range(rows):
        row = pltpu.roll(plane_row(planes, r, channels), cols - SHIFT, 1)
        if r >= rows - SHIFT:
            prv_out[r - rows + SHIFT] = row.astype(BF)
        image[SHIFT + r] = row.T
    for i in range(3):
        weights[i] = wqkv[:, i * CHAN : (i + 1) * CHAN]
    bias_strips(table, strips)
    bias_own[0], bias_own[1] = biases(strips, me == bands - 1, TOK)
    bias_prev[0], bias_prev[1] = biases(strips, me == 0, HALF)

    told[...] = jnp.zeros(told.shape, jnp.int32)
    told[:, 0:windows] = jnp.broadcast_to(keep_row[...], (8, windows))
    kept = told[...]
    tri = (LANES, LANES)
    before = lax.broadcasted_iota(jnp.int32, tri, 0) < lax.broadcasted_iota(jnp.int32, tri, 1)
    place = dot(kept.astype(F32).astype(BF), jnp.where(before, 1.0, 0.0).astype(BF))
    told[...] = jnp.where(place < count[0].astype(F32), kept, 0)

    def spread(flags):
        own_lane = (windows, LANES)
        diagonal = lax.broadcasted_iota(jnp.int32, own_lane, 0) == lax.broadcasted_iota(
            jnp.int32, own_lane, 1
        )
        chosen = jnp.where(diagonal, jnp.broadcast_to(flags[0:1].astype(F32), own_lane), 0.0)
        return dot(chosen.astype(BF), jnp.ones((LANES, channels), BF))

    active[0] = spread(told[...])

    following[windows] = jnp.int32(windows)

    def scan(i, kept_so_far):
        w = windows - 1 - i
        following[w] = jnp.where(keep[0, w] == 1, w, following[w + 1])
        return kept_so_far + keep[0, w]

    live = jnp.minimum(lax.fori_loop(0, windows, scan, jnp.int32(0)), count[0])

    def rank(p, window):
        order[p] = jnp.minimum(window, windows - 1)
        return following[jnp.minimum(window + 1, windows)]

    lax.fori_loop(0, windows, rank, following[0])

    def step(i, _):
        def edge(g):
            return bias_own[(i * GROUP + g == windows - 1).astype(jnp.int32)]

        own = attend(
            group_at(image, i, WIN), gain_a[...], weights[0], weights[1], weights[2], wp[...],
            edge, TOK,
        )
        wide = own.astype(F32)
        for g in range(GROUP):
            w = i * GROUP + g
            upper[w] = own[g * TOK : g * TOK + HALF]
            first[w] = own[g * TOK : (g + 1) * TOK, :LANES]
            tail = wide[g * TOK : (g + 1) * TOK, LANES:]
            rest[w] = jnp.concatenate([tail, jnp.zeros((TOK, 2 * LANES - CHAN), F32)], axis=1)
        return 0

    for c in range(halves):
        nxt_copy(c).wait()
        if c == halves - 1:
            told_copy.start()
            prv_copy.start()
        for r in range(SHIFT):
            block = nxt_buf[r, :, c * LANES : (c + 1) * LANES].astype(F32)
            image[SHIFT + rows + r, c * LANES : (c + 1) * LANES, :] = block.T
        lax.fori_loop(c * groups // halves, (c + 1) * groups // halves, step, 0)

    lane = lax.broadcasted_iota(jnp.int32, (TOK, LANES), 1)

    def pack(index, peer, j):
        t = jnp.int32(0)
        found = jnp.int32(0)
        for i in range(span):
            hit = dests[0, j * span + i] == peer
            t = jnp.where(hit, j * span + i, t)
            found = jnp.where(hit, 1, found)
        live_tile = (found > 0) & (t * TILE < live)
        slot = jnp.where(live_tile, slots[0, t], CAP).astype(F32)
        halves_of = []
        for p in range(TILE):
            position = t * TILE + p
            valid = live_tile & (position < live)
            source = order[position]
            value = first[source]
            outgoing[index, p * TOK : (p + 1) * TOK] = jnp.where(valid, value, jnp.zeros_like(value))
            halves_of.append(jnp.where(valid, rest[source], 0.0))
        both = jnp.where(lane < TOK, halves_of[0], pltpu.roll(halves_of[1], TOK, 1))
        outgoing[index, TILE * TOK :] = jnp.where(lane >= SLOT_LANE, slot, both).astype(BF)

    def tile_copy(i):
        return pltpu.make_async_remote_copy(
            src_ref=outgoing.at[pl.ds(i * pairs, pairs)],
            dst_ref=incoming.at[pl.ds(me * pairs, pairs)],
            send_sem=tile_send.at[i],
            recv_sem=tile_recv.at[i],
            device_id={"band": lax.rem(me + i, bands)},
            device_id_type=mesh_id,
        )

    def dispatch(i, _):
        for j in range(pairs):
            pack(i * pairs + j, lax.rem(me + i, bands), j)
        tile_copy(i).start()
        return 0

    lax.fori_loop(1, bands, dispatch, 0)
    for j in range(pairs):
        pack(j, me, j)
    incoming[pl.ds(me * pairs, pairs)] = outgoing[0:pairs]

    def blend(done, flags, w, row):
        cols_w = pl.ds(pl.multiple_of(w * WIN, WIN), WIN)
        chosen = active[flags, pl.ds(w, 1), :].reshape(1, 1, channels) > 0.5
        value = done.reshape(SHIFT, WIN, CHAN)
        result[row : row + SHIFT, cols_w, :] = jnp.where(
            chosen, value, image[SHIFT + row : 2 * SHIFT + row, cols_w, :]
        )

    def finish_own(i, _):
        span_w = 2 * GROUP
        states = jnp.concatenate([upper[i * span_w + g] for g in range(span_w)], axis=0)
        done = feed(states, gain_m[...], wh[...], wo[...]).astype(F32)
        for g in range(span_w):
            blend(done[g * HALF : (g + 1) * HALF], 0, i * span_w + g, SHIFT)
        return 0

    lax.fori_loop(0, groups // 2, finish_own, 0)

    told_copy.wait()
    active[1] = spread(told_buf[...])
    prv_copy.wait()
    for r in range(SHIFT):
        image[r] = prv_buf[r].astype(F32).T

    def finish_prev(i, _):
        def edge(g):
            return bias_prev[(i * GROUP + g == windows - 1).astype(jnp.int32)]

        prev = attend(
            group_at(image, i, 0), gain_a[...], weights[0], weights[1], weights[2], wp[...],
            edge, HALF,
        )
        done = feed(prev, gain_m[...], wh[...], wo[...]).astype(F32)
        for g in range(GROUP):
            blend(done[g * HALF : (g + 1) * HALF], 1, i * GROUP + g, 0)
        return 0

    lax.fori_loop(0, groups, finish_prev, 0)
    for r in range(rows):
        row = pltpu.roll(result[r].T, SHIFT, 1)
        for h in range(halves):
            planes[h, pl.ds(r, channels, stride=WIN), :] = row[:, h * LANES : (h + 1) * LANES]
    for h in range(halves):
        restored[:, :, h * LANES : (h + 1) * LANES] = (
            planes[h].reshape(channels, rows, LANES).astype(BF)
        )

    def collect(i, _):
        tile_copy(i).wait()
        return 0

    lax.fori_loop(1, bands, collect, 0)


def place_kernel(incoming, work, planes):
    total = incoming.shape[0]
    channels = work.shape[0]
    head = jnp.max(incoming[:, TILE * TOK : TILE * TOK + 16, :].astype(F32), axis=1)
    lane = lax.broadcasted_iota(jnp.int32, (total, LANES), 1)
    slot = jnp.max(jnp.where(lane >= SLOT_LANE, head, 0.0), axis=1, keepdims=True).astype(jnp.int32)
    match = slot == lane
    index = lax.broadcasted_iota(jnp.int32, (total, LANES), 0)
    source = jnp.max(jnp.where(match, index, -1).astype(F32), axis=0, keepdims=True).astype(jnp.int32)
    for k in range(CAP):
        known = source[0, k] >= 0
        t = jnp.maximum(source[0, k], 0)
        main = incoming[t, : TILE * TOK].astype(F32)
        tail = incoming[t, TILE * TOK :].astype(F32)
        tails = jnp.concatenate([tail, pltpu.roll(tail, TOK, 1)], axis=0)
        block = jnp.concatenate([main.T, tails.T[: channels - LANES]], axis=0)
        planes[pl.ds(k, channels, stride=CAP), :] = jnp.where(known, block, 0.0)
    work[...] = planes[...].reshape(channels, CAP, TILE * TOK).astype(BF)


def shards(
    pixels, keep_mask, band_counts, plan_dest, plan_slot, bias_table, gain_attn, qkv_weight,
    proj_weight, gain_mlp, hidden_weight, output_weight,
):
    bands = lax.axis_size("band")
    rows, cols, channels = pixels.shape
    windows = cols // WIN
    halves = cols // LANES
    tiles = windows // TILE
    pairs = -(-tiles // bands)
    smem = pl.BlockSpec(memory_space=pltpu.SMEM)
    vmem = pl.BlockSpec(memory_space=pltpu.VMEM)
    tile_shape = (bands * pairs, TILE * TOK + TOK, LANES)
    restored, incoming = pl.pallas_call(
        block_kernel,
        out_shape=(
            jax.ShapeDtypeStruct((channels, rows, cols), BF),
            jax.ShapeDtypeStruct(tile_shape, BF),
        ),
        in_specs=[smem] * 4 + [vmem] * 9,
        out_specs=(vmem, vmem),
        scratch_shapes=[
            pltpu.VMEM((halves, channels * rows, LANES), F32),
            pltpu.VMEM((rows + 2 * SHIFT, cols, channels), F32),
            pltpu.VMEM((SHIFT, channels, cols), BF),
            pltpu.VMEM((SHIFT, channels, cols), BF),
            pltpu.VMEM((SHIFT, channels, cols), BF),
            pltpu.VMEM((SHIFT, channels, cols), BF),
            pltpu.VMEM((8, LANES), jnp.int32),
            pltpu.VMEM((8, LANES), jnp.int32),
            pltpu.VMEM((3, channels, channels), BF),
            pltpu.VMEM((8 * WIN, LANES), F32),
            pltpu.VMEM((2, HEADS * TOK, TOK), F32),
            pltpu.VMEM((2, HEADS * HALF, TOK), F32),
            pltpu.VMEM((windows, TOK, LANES), BF),
            pltpu.VMEM((windows, TOK, LANES), F32),
            pltpu.VMEM((windows, HALF, channels), BF),
            pltpu.VMEM((rows, cols, channels), F32),
            pltpu.VMEM((2, windows, channels), F32),
            pltpu.VMEM(tile_shape, BF),
            pltpu.SMEM((windows + 1,), jnp.int32),
            pltpu.SMEM((windows,), jnp.int32),
            pltpu.SemaphoreType.DMA((halves + 2,)),
            pltpu.SemaphoreType.DMA((halves + 2,)),
            pltpu.SemaphoreType.DMA((bands,)),
            pltpu.SemaphoreType.DMA((bands,)),
        ],
        compiler_params=pltpu.CompilerParams(
            vmem_limit_bytes=63 * 1024 * 1024, collective_id=0, has_side_effects=True
        ),
        cost_estimate=pl.CostEstimate(flops=10**10, bytes_accessed=10**7, transcendentals=10**6),
        name="block",
    )(
        keep_mask, band_counts, plan_dest, plan_slot, keep_mask, jnp.transpose(pixels, (2, 0, 1)),
        bias_table.T, gain_attn[None], qkv_weight, proj_weight, gain_mlp[None], hidden_weight,
        output_weight.T,
    )
    work = pl.pallas_call(
        place_kernel,
        out_shape=jax.ShapeDtypeStruct((channels, CAP, TILE * TOK), BF),
        in_specs=[vmem],
        out_specs=vmem,
        scratch_shapes=[pltpu.VMEM((channels * CAP, TILE * TOK), F32)],
        compiler_params=pltpu.CompilerParams(vmem_limit_bytes=16 * 1024 * 1024),
        name="place",
    )(incoming)
    return jnp.transpose(restored, (1, 2, 0)), jnp.transpose(work, (1, 2, 0))


def solution(mesh):
    split = P(("img", "band"))
    in_specs = (split,) * 5 + (P(),) * 7
    return jax.shard_map(shards, mesh=mesh, in_specs=in_specs, out_specs=(split, split), check_vma=False)
```

```python
import jax
import jax.numpy as jnp
from jax import lax
from jax.experimental import pallas as pl
from jax.experimental.pallas import tpu as pltpu
from jax.sharding import PartitionSpec as P

CHAN = 180
HEADS = 6
WIN = 8
TILE = 2
SHIFT = 4
CAP = 8
TOK = WIN * WIN
HALF = TOK // 2
HEAD_DIM = CHAN // HEADS
GROUP = 16
SIZE = GROUP * TOK
PAD = 32
DEPTH = HEADS * PAD
QUERIES = HEADS * TOK
LANES = 128
SLOT_LANE = 120

EPSILON = 1e-05
BF = jnp.bfloat16
F32 = jnp.float32


def layer_norm(values, gain):
    center = values - jnp.sum(values, axis=0, keepdims=True) * (1.0 / CHAN)
    spread = jnp.sum(center * center, axis=0, keepdims=True) * (1.0 / CHAN)
    return (center * lax.rsqrt(spread + EPSILON) * gain).astype(BF)


def dot(a, b):
    return jnp.dot(a, b, preferred_element_type=F32)


def dot_t(a, b):
    return lax.dot_general(a, b, (((1,), (1,)), ((), ())), preferred_element_type=F32)


def iota(shape, axis):
    return lax.broadcasted_iota(jnp.int32, shape, axis)


def bias_strips(table, strips):
    heads, entries = table.shape
    values = jnp.concatenate([table[...], jnp.zeros((8 - heads, entries), F32)], axis=0)
    high = values.astype(BF).astype(F32)
    middle = (values - high).astype(BF).astype(F32)
    low = values - high - middle
    parts = jnp.concatenate([high, middle, low], axis=0).astype(BF)
    shape = (entries, WIN * LANES)
    entry, lane = iota(shape, 0), iota(shape, 1)
    step = (lane % LANES) // WIN
    wanted = step * (2 * WIN - 1) + lane % WIN - lane // LANES + WIN - 1
    pick = jnp.where((entry == wanted) & (step < 2 * WIN - 1), 1.0, 0.0).astype(BF)
    found = dot(parts, pick)
    found = found[0:8] + found[8:16] + found[16:24]
    for c in range(WIN):
        strips[pl.ds(c, 8, stride=WIN), :] = found[:, c * LANES : (c + 1) * LANES]


def bias_fill(strips, bias, own_last, prev_last):
    first_half = iota((WIN, LANES), 1) < TOK
    for r in range(WIN):
        by = 2 * LANES - (WIN - 1 - r) * WIN
        tiles = []
        for h in range(0, HEADS, 2):
            even = strips[h * WIN : (h + 1) * WIN, :]
            odd = strips[(h + 1) * WIN : (h + 2) * WIN, :]
            tiles.append(
                jnp.where(
                    first_half,
                    pltpu.roll(even, by % LANES, 1),
                    pltpu.roll(odd, (by + TOK) % LANES, 1),
                )
            )
        base = jnp.concatenate(tiles, axis=1)
        shape = (WIN, QUERIES)
        key, query = iota(shape, 0), iota(shape, 1) % TOK
        rows_differ = (query // WIN >= SHIFT) != (r >= SHIFT)
        cols_differ = (key >= SHIFT) != (query % WIN >= SHIFT)
        rows = slice(r * WIN, (r + 1) * WIN)
        for k, last in enumerate((own_last, prev_last)):
            row_pen = jnp.where(rows_differ, jnp.where(last, -100.0, 0.0).astype(F32), 0.0)
            bias[2 * k, rows] = base + row_pen
            bias[2 * k + 1, rows] = base + jnp.where(cols_differ, -100.0, row_pen)


def spread_heads(rows, cols):
    row, col = iota((rows, cols), 0), iota((rows, cols), 1)
    inside = row % DEPTH
    wanted = row // DEPTH * CHAN + inside // PAD * HEAD_DIM + inside % PAD
    return jnp.where((inside % PAD < HEAD_DIM) & (wanted == col), 1.0, 0.0).astype(BF)


def attend(x, gain, w_in, w_out, bias_of):
    normed = layer_norm(x, gain)
    mixed = dot(w_in, normed)
    q = mixed[0:DEPTH] * HEAD_DIM ** (-0.5)
    k = mixed[DEPTH : 2 * DEPTH].T.astype(BF)
    v = mixed[2 * DEPTH :].astype(BF)
    low = iota((PAD, LANES), 1) < TOK
    blank = jnp.zeros((PAD, LANES), F32)
    joined = []
    for pair in range(GROUP // 2):
        lanes = slice(pair * LANES, (pair + 1) * LANES)
        q_pair = q[:, lanes]
        q_turn = pltpu.roll(q_pair, TOK, 1)
        weights = []
        for side in range(2):
            g = 2 * pair + side
            blocks = []
            for h in range(HEADS):
                part = slice(h * PAD, (h + 1) * PAD)
                value = q_pair[part] if h % 2 == side else q_turn[part]
                value = jnp.where(low if h % 2 == 0 else ~low, value, 0.0)
                row = [blank] * (HEADS // 2)
                row[h // 2] = value
                blocks.append(jnp.concatenate(row, axis=1))
            spread_q = jnp.concatenate(blocks, axis=0).astype(BF)
            scores = dot(k[g * TOK : (g + 1) * TOK], spread_q) + bias_of(g)
            top = jnp.max(scores, axis=0, keepdims=True)
            grown = jnp.exp(scores - top)
            weights.append((grown * (1.0 / jnp.sum(grown, axis=0, keepdims=True))).astype(BF))
        rows = []
        none = jnp.zeros((TOK, LANES), BF)
        for j in range(HEADS // 2):
            cut = slice(j * LANES, (j + 1) * LANES)
            both = jnp.concatenate(
                [
                    jnp.concatenate([weights[0][:, cut], none], axis=1),
                    jnp.concatenate([none, weights[1][:, cut]], axis=1),
                ],
                axis=0,
            )
            found = dot(v[2 * j * PAD : 2 * (j + 1) * PAD, lanes], both)
            one, two = found[:, :LANES], found[:, LANES:]
            rows.append(jnp.where(low, one[:PAD], pltpu.roll(two[:PAD], TOK, 1)))
            rows.append(jnp.where(low, pltpu.roll(one[PAD:], TOK, 1), two[PAD:]))
        joined.append(jnp.concatenate(rows, axis=0))
    joined = jnp.concatenate(joined, axis=1).astype(BF)
    return (x + dot(w_out, joined)).astype(BF)


def feed(states, gain, wh, wo):
    flat = states.astype(F32)
    normed = layer_norm(flat, gain)
    inner = jax.nn.gelu(dot(wh, normed)).astype(BF)
    return (flat + dot(wo, inner)).astype(BF)


def window_at(image, i, g, row):
    start = pl.multiple_of((i * GROUP + g) * WIN, WIN)
    return image[row : row + WIN, pl.ds(start, WIN), :].reshape(TOK, CHAN)


def group_at(image, i, row):
    return jnp.concatenate([window_at(image, i, g, row) for g in range(GROUP)], axis=0).T


def plane_row(planes, row, channels):
    halves = planes.shape[0]
    return jnp.concatenate(
        [planes[h, pl.ds(row, channels, stride=WIN), :] for h in range(halves)], axis=1
    )


def block_kernel(
    keep, count, dests, slots, keep_row, pixels, table, gain_a, wqkv, wp, gain_m, wh, wo,
    restored, incoming,
    planes, image, nxt_out, prv_out, nxt_buf, prv_buf, told, told_buf, w_in, w_out, w_hid, gains,
    strips, bias, states, doubled, result, active, outgoing, following, order,
    halo_send, halo_recv, tile_send, tile_recv,
):
    bands = lax.axis_size("band")
    me = lax.axis_index("band")
    right, left = lax.rem(me + 1, bands), lax.rem(me + bands - 1, bands)
    channels, rows, cols = pixels.shape
    windows = cols // WIN
    groups = windows // GROUP
    halves = cols // LANES
    tiles = windows // TILE
    pairs = -(-tiles // bands)
    span = min(bands, tiles)
    mesh_id = pl.DeviceIdType.MESH

    barrier = pltpu.get_barrier_semaphore()

    def greet(i, _):
        peer = lax.rem(me + i, bands)
        pl.semaphore_signal(barrier, inc=1, device_id={"band": peer}, device_id_type=mesh_id)
        return 0

    lax.fori_loop(1, bands, greet, 0)

    for h in range(halves):
        part = pixels[:, :, h * LANES : (h + 1) * LANES].astype(F32)
        planes[h] = part.reshape(channels * rows, LANES)
    for r in range(SHIFT):
        nxt_out[r] = pltpu.roll(plane_row(planes, r, channels), cols - SHIFT, 1).astype(BF)
    pl.semaphore_wait(barrier, bands - 1)

    def nxt_copy(c):
        part = pl.ds(pl.multiple_of(c * LANES, LANES), LANES)
        return pltpu.make_async_remote_copy(
            src_ref=nxt_out.at[:, :, part],
            dst_ref=nxt_buf.at[:, :, part],
            send_sem=halo_send.at[c],
            recv_sem=halo_recv.at[c],
            device_id={"band": left},
            device_id_type=mesh_id,
        )

    prv_copy = pltpu.make_async_remote_copy(
        src_ref=prv_out,
        dst_ref=prv_buf,
        send_sem=halo_send.at[halves],
        recv_sem=halo_recv.at[halves],
        device_id={"band": right},
        device_id_type=mesh_id,
    )
    told_copy = pltpu.make_async_remote_copy(
        src_ref=told,
        dst_ref=told_buf,
        send_sem=halo_send.at[halves + 1],
        recv_sem=halo_recv.at[halves + 1],
        device_id={"band": right},
        device_id_type=mesh_id,
    )
    for c in range(halves):
        nxt_copy(c).start()

    for r in range(rows):
        row = pltpu.roll(plane_row(planes, r, channels), cols - SHIFT, 1)
        if r >= rows - SHIFT:
            prv_out[r - rows + SHIFT] = row.astype(BF)
        image[SHIFT + r] = row.T
    w_in[...] = dot_t(spread_heads(3 * DEPTH, 3 * CHAN), wqkv[...]).astype(BF)
    w_out[...] = dot(spread_heads(DEPTH, CHAN), wp[...]).T.astype(BF)
    w_hid[...] = wh[...].astype(F32).T.astype(BF)
    gains[0] = jnp.broadcast_to(gain_a[...], (SIZE, channels)).T
    gains[1] = jnp.broadcast_to(gain_m[...], (SIZE, channels)).T
    bias_strips(table, strips)
    bias_fill(strips, bias, me == bands - 1, me == 0)

    told[...] = jnp.zeros(told.shape, jnp.int32)
    told[:, 0:windows] = jnp.broadcast_to(keep_row[...], (8, windows))
    kept = told[...]
    tri = (LANES, LANES)
    before = lax.broadcasted_iota(jnp.int32, tri, 0) < lax.broadcasted_iota(jnp.int32, tri, 1)
    place = dot(kept.astype(F32).astype(BF), jnp.where(before, 1.0, 0.0).astype(BF))
    told[...] = jnp.where(place < count[0].astype(F32), kept, 0)

    def spread(flags):
        own_lane = (windows, LANES)
        diagonal = lax.broadcasted_iota(jnp.int32, own_lane, 0) == lax.broadcasted_iota(
            jnp.int32, own_lane, 1
        )
        chosen = jnp.where(diagonal, jnp.broadcast_to(flags[0:1].astype(F32), own_lane), 0.0)
        return dot(chosen.astype(BF), jnp.ones((LANES, channels), BF))

    active[0] = spread(told[...])

    following[windows] = jnp.int32(windows)

    def scan(i, kept_so_far):
        w = windows - 1 - i
        following[w] = jnp.where(keep[0, w] == 1, w, following[w + 1])
        return kept_so_far + keep[0, w]

    live = jnp.minimum(lax.fori_loop(0, windows, scan, jnp.int32(0)), count[0])

    def rank(p, window):
        order[p] = jnp.minimum(window, windows - 1)
        return following[jnp.minimum(window + 1, windows)]

    lax.fori_loop(0, windows, rank, following[0])

    early = iota((channels, LANES), 1) < TOK

    def attend_group(i, kind, row):
        def edge(g):
            return bias[2 * kind + (i * GROUP + g == windows - 1).astype(jnp.int32)]

        return attend(group_at(image, i, row), gains[0], w_in[...], w_out[...], edge)

    def step(i, _):
        own = attend_group(i, 0, WIN)
        states[i] = own
        wide = own.astype(F32)
        for pair in range(GROUP // 2):
            block = wide[:, pair * LANES : (pair + 1) * LANES]
            turned = pltpu.roll(block, TOK, 1)
            w = i * GROUP + 2 * pair
            doubled[w] = jnp.where(early, block, turned).astype(BF)
            doubled[w + 1] = jnp.where(early, turned, block).astype(BF)
        return 0

    for c in range(halves):
        nxt_copy(c).wait()
        if c == halves - 1:
            told_copy.start()
            prv_copy.start()
        for r in range(SHIFT):
            block = nxt_buf[r, :, c * LANES : (c + 1) * LANES].astype(F32)
            image[SHIFT + rows + r, c * LANES : (c + 1) * LANES, :] = block.T
        lax.fori_loop(c * groups // halves, (c + 1) * groups // halves, step, 0)

    def pack(index, peer, j):
        t = jnp.int32(0)
        found = jnp.int32(0)
        for i in range(span):
            hit = dests[0, j * span + i] == peer
            t = jnp.where(hit, j * span + i, t)
            found = jnp.where(hit, 1, found)
        live_tile = (found > 0) & (t * TILE < live)
        slot = jnp.where(live_tile, slots[0, t], CAP).astype(F32)
        halves_of = []
        for p in range(TILE):
            position = t * TILE + p
            valid = live_tile & (position < live)
            value = doubled[order[position]]
            halves_of.append(jnp.where(valid, value, jnp.zeros_like(value)))
        outgoing[index, :channels] = jnp.where(early, halves_of[0], halves_of[1])
        outgoing[index, DEPTH - 8 :] = jnp.full((8, LANES), slot, F32).astype(BF)

    def tile_copy(i):
        return pltpu.make_async_remote_copy(
            src_ref=outgoing.at[pl.ds(i * pairs, pairs)],
            dst_ref=incoming.at[pl.ds(me * pairs, pairs)],
            send_sem=tile_send.at[i],
            recv_sem=tile_recv.at[i],
            device_id={"band": lax.rem(me + i, bands)},
            device_id_type=mesh_id,
        )

    def dispatch(i, _):
        for j in range(pairs):
            pack(i * pairs + j, lax.rem(me + i, bands), j)
        tile_copy(i).start()
        return 0

    lax.fori_loop(1, bands, dispatch, 0)
    for j in range(pairs):
        pack(j, me, j)
    incoming[pl.ds(me * pairs, pairs)] = outgoing[0:pairs]

    def blend(done, flags, w, row):
        cols_w = pl.ds(pl.multiple_of(w * WIN, WIN), WIN)
        chosen = active[flags, pl.ds(w, 1), :].reshape(1, 1, channels) > 0.5
        result[row : row + SHIFT, cols_w, :] = jnp.where(
            chosen,
            done.reshape(SHIFT, WIN, CHAN),
            image[SHIFT + row : 2 * SHIFT + row, cols_w, :],
        )

    told_copy.wait()
    active[1] = spread(told_buf[...])
    prv_copy.wait()
    for r in range(SHIFT):
        image[r] = prv_buf[r].astype(F32).T
    upper = iota((channels, SIZE), 1) % TOK < HALF

    def finish(i, _):
        prev = attend_group(i, 1, 0)
        mine = jnp.where(upper, states[i], prev)
        done = feed(mine, gains[1], w_hid[...], wo[...]).astype(F32).T
        for g in range(GROUP):
            w = i * GROUP + g
            blend(done[g * TOK : g * TOK + HALF], 0, w, SHIFT)
            blend(done[g * TOK + HALF : (g + 1) * TOK], 1, w, 0)
        return 0

    lax.fori_loop(0, groups, finish, 0)
    for r in range(rows):
        row = pltpu.roll(result[r].T, SHIFT, 1)
        for h in range(halves):
            planes[h, pl.ds(r, channels, stride=WIN), :] = row[:, h * LANES : (h + 1) * LANES]
    for h in range(halves):
        restored[:, :, h * LANES : (h + 1) * LANES] = (
            planes[h].reshape(channels, rows, LANES).astype(BF)
        )

    def collect(i, _):
        tile_copy(i).wait()
        return 0

    lax.fori_loop(1, bands, collect, 0)


def place_kernel(incoming, work, planes):
    total = incoming.shape[0]
    channels = work.shape[0]
    head = jnp.max(incoming[:, DEPTH - 8 :, :].astype(F32), axis=1)
    slot = jnp.max(head, axis=1, keepdims=True).astype(jnp.int32)
    match = slot == iota((total, LANES), 1)
    source = jnp.where(match, iota((total, LANES), 0), -1).astype(F32)
    source = jnp.max(source, axis=0, keepdims=True).astype(jnp.int32)
    for k in range(CAP):
        known = source[0, k] >= 0
        block = incoming[jnp.maximum(source[0, k], 0), :channels].astype(F32)
        planes[pl.ds(k, channels, stride=CAP), :] = jnp.where(known, block, 0.0)
    work[...] = planes[...].reshape(channels, CAP, TILE * TOK).astype(BF)


def shards(
    pixels, keep_mask, band_counts, plan_dest, plan_slot, bias_table, gain_attn, qkv_weight,
    proj_weight, gain_mlp, hidden_weight, output_weight,
):
    bands = lax.axis_size("band")
    rows, cols, channels = pixels.shape
    windows = cols // WIN
    halves = cols // LANES
    tiles = windows // TILE
    pairs = -(-tiles // bands)
    smem = pl.BlockSpec(memory_space=pltpu.SMEM)
    vmem = pl.BlockSpec(memory_space=pltpu.VMEM)
    tile_shape = (bands * pairs, DEPTH, LANES)
    restored, incoming = pl.pallas_call(
        block_kernel,
        out_shape=(
            jax.ShapeDtypeStruct((channels, rows, cols), BF),
            jax.ShapeDtypeStruct(tile_shape, BF),
        ),
        in_specs=[smem] * 4 + [vmem] * 9,
        out_specs=(vmem, vmem),
        scratch_shapes=[
            pltpu.VMEM((halves, channels * rows, LANES), F32),
            pltpu.VMEM((rows + 2 * SHIFT, cols, channels), F32),
            pltpu.VMEM((SHIFT, channels, cols), BF),
            pltpu.VMEM((SHIFT, channels, cols), BF),
            pltpu.VMEM((SHIFT, channels, cols), BF),
            pltpu.VMEM((SHIFT, channels, cols), BF),
            pltpu.VMEM((8, LANES), jnp.int32),
            pltpu.VMEM((8, LANES), jnp.int32),
            pltpu.VMEM((3 * DEPTH, channels), BF),
            pltpu.VMEM((channels, DEPTH), BF),
            pltpu.VMEM((hidden_weight.shape[1], channels), BF),
            pltpu.VMEM((2, channels, SIZE), F32),
            pltpu.VMEM((8 * WIN, LANES), F32),
            pltpu.VMEM((4, TOK, QUERIES), F32),
            pltpu.VMEM((windows // GROUP, channels, SIZE), BF),
            pltpu.VMEM((windows, channels, LANES), BF),
            pltpu.VMEM((rows, cols, channels), F32),
            pltpu.VMEM((2, windows, channels), F32),
            pltpu.VMEM(tile_shape, BF),
            pltpu.SMEM((windows + 1,), jnp.int32),
            pltpu.SMEM((windows,), jnp.int32),
            pltpu.SemaphoreType.DMA((halves + 2,)),
            pltpu.SemaphoreType.DMA((halves + 2,)),
            pltpu.SemaphoreType.DMA((bands,)),
            pltpu.SemaphoreType.DMA((bands,)),
        ],
        compiler_params=pltpu.CompilerParams(
            vmem_limit_bytes=63 * 1024 * 1024, collective_id=0, has_side_effects=True
        ),
        cost_estimate=pl.CostEstimate(flops=10**10, bytes_accessed=10**7, transcendentals=10**6),
        name="block",
    )(
        keep_mask, band_counts, plan_dest, plan_slot, keep_mask, jnp.transpose(pixels, (2, 0, 1)),
        bias_table.T, gain_attn[None], qkv_weight, proj_weight, gain_mlp[None], hidden_weight,
        output_weight.T,
    )
    work = pl.pallas_call(
        place_kernel,
        out_shape=jax.ShapeDtypeStruct((channels, CAP, TILE * TOK), BF),
        in_specs=[vmem],
        out_specs=vmem,
        scratch_shapes=[pltpu.VMEM((channels * CAP, TILE * TOK), F32)],
        compiler_params=pltpu.CompilerParams(vmem_limit_bytes=16 * 1024 * 1024),
        name="place",
    )(incoming)
    return jnp.transpose(restored, (1, 2, 0)), jnp.transpose(work, (1, 2, 0))


def solution(mesh):
    split = P(("img", "band"))
    in_specs = (split,) * 5 + (P(),) * 7
    return jax.shard_map(shards, mesh=mesh, in_specs=in_specs, out_specs=(split, split), check_vma=False)
```

```python
import jax
import jax.numpy as jnp
from jax import lax
from jax.experimental import pallas as pl
from jax.experimental.pallas import tpu as pltpu
from jax.sharding import PartitionSpec as P

CHAN = 180
HEADS = 6
WIN = 8
TILE = 2
SHIFT = 4
CAP = 8
TOK = WIN * WIN
HALF = TOK // 2
HEAD_DIM = CHAN // HEADS
GROUP = 8
WIDER = 2
SIZE = GROUP * TOK
PART = GROUP * WIN
PAD = 32
DEPTH = HEADS * PAD
QUERIES = HEADS * TOK
LANES = 128
SLOT_LANE = 120

EPSILON = 1e-05
BF = jnp.bfloat16
F32 = jnp.float32


def layer_norm(values, gain):
    center = values - jnp.sum(values, axis=0, keepdims=True) * (1.0 / CHAN)
    spread = jnp.sum(center * center, axis=0, keepdims=True) * (1.0 / CHAN)
    scaled = center * lax.rsqrt(spread + EPSILON)
    parts = [scaled[:, i : i + LANES] * gain for i in range(0, values.shape[1], LANES)]
    return jnp.concatenate(parts, axis=1).astype(BF)


def dot(a, b):
    return jnp.dot(a, b, preferred_element_type=F32)


def dot_t(a, b):
    return lax.dot_general(a, b, (((1,), (1,)), ((), ())), preferred_element_type=F32)


def iota(shape, axis):
    return lax.broadcasted_iota(jnp.int32, shape, axis)


def bias_strips(table, strips):
    heads, entries = table.shape
    values = jnp.concatenate([table[...], jnp.zeros((8 - heads, entries), F32)], axis=0)
    high = values.astype(BF).astype(F32)
    middle = (values - high).astype(BF).astype(F32)
    low = values - high - middle
    parts = jnp.concatenate([high, middle, low], axis=0).astype(BF)
    shape = (entries, WIN * LANES)
    entry, lane = iota(shape, 0), iota(shape, 1)
    step = (lane % LANES) // WIN
    wanted = step * (2 * WIN - 1) + lane % WIN - lane // LANES + WIN - 1
    pick = jnp.where((entry == wanted) & (step < 2 * WIN - 1), 1.0, 0.0).astype(BF)
    found = dot(parts, pick)
    found = found[0:8] + found[8:16] + found[16:24]
    for c in range(WIN):
        strips[pl.ds(c, 8, stride=WIN), :] = found[:, c * LANES : (c + 1) * LANES]


def bias_fill(strips, bias, own_last, prev_last):
    first_half = iota((WIN, LANES), 1) < TOK
    for r in range(WIN):
        by = 2 * LANES - (WIN - 1 - r) * WIN
        tiles = []
        for h in range(0, HEADS, 2):
            even = strips[h * WIN : (h + 1) * WIN, :]
            odd = strips[(h + 1) * WIN : (h + 2) * WIN, :]
            tiles.append(
                jnp.where(
                    first_half,
                    pltpu.roll(even, by % LANES, 1),
                    pltpu.roll(odd, (by + TOK) % LANES, 1),
                )
            )
        base = jnp.concatenate(tiles, axis=1)
        shape = (WIN, QUERIES)
        key, query = iota(shape, 0), iota(shape, 1) % TOK
        rows_differ = (query // WIN >= SHIFT) != (r >= SHIFT)
        cols_differ = (key >= SHIFT) != (query % WIN >= SHIFT)
        rows = slice(r * WIN, (r + 1) * WIN)
        for k, last in enumerate((own_last, prev_last)):
            row_pen = jnp.where(rows_differ, jnp.where(last, -100.0, 0.0).astype(F32), 0.0)
            bias[2 * k, rows] = base + row_pen
            bias[2 * k + 1, rows] = base + jnp.where(cols_differ, -100.0, row_pen)


def spread_heads(rows, cols):
    row, col = iota((rows, cols), 0), iota((rows, cols), 1)
    inside = row % DEPTH
    wanted = row // DEPTH * CHAN + inside // PAD * HEAD_DIM + inside % PAD
    return jnp.where((inside % PAD < HEAD_DIM) & (wanted == col), 1.0, 0.0).astype(BF)


def attend(x, gain, w_in, w_out, bias_of):
    normed = layer_norm(x, gain)
    mixed = dot(w_in, normed)
    q = mixed[0:DEPTH] * HEAD_DIM ** (-0.5)
    k = mixed[DEPTH : 2 * DEPTH].T.astype(BF)
    v = mixed[2 * DEPTH :].astype(BF)
    low = iota((PAD, LANES), 1) < TOK
    blank = jnp.zeros((PAD, LANES), F32)
    joined = []
    for pair in range(x.shape[1] // LANES):
        lanes = slice(pair * LANES, (pair + 1) * LANES)
        q_pair = q[:, lanes]
        q_turn = pltpu.roll(q_pair, TOK, 1)
        weights = []
        for side in range(2):
            g = 2 * pair + side
            blocks = []
            for h in range(HEADS):
                part = slice(h * PAD, (h + 1) * PAD)
                value = q_pair[part] if h % 2 == side else q_turn[part]
                value = jnp.where(low if h % 2 == 0 else ~low, value, 0.0)
                row = [blank] * (HEADS // 2)
                row[h // 2] = value
                blocks.append(jnp.concatenate(row, axis=1))
            spread_q = jnp.concatenate(blocks, axis=0).astype(BF)
            scores = dot(k[g * TOK : (g + 1) * TOK], spread_q) + bias_of(g)
            top = jnp.max(scores, axis=0, keepdims=True)
            grown = jnp.exp(scores - top)
            weights.append((grown * (1.0 / jnp.sum(grown, axis=0, keepdims=True))).astype(BF))
        rows = []
        none = jnp.zeros((TOK, LANES), BF)
        for j in range(HEADS // 2):
            cut = slice(j * LANES, (j + 1) * LANES)
            both = jnp.concatenate(
                [
                    jnp.concatenate([weights[0][:, cut], none], axis=1),
                    jnp.concatenate([none, weights[1][:, cut]], axis=1),
                ],
                axis=0,
            )
            found = dot(v[2 * j * PAD : 2 * (j + 1) * PAD, lanes], both)
            one, two = found[:, :LANES], found[:, LANES:]
            rows.append(jnp.where(low, one[:PAD], pltpu.roll(two[:PAD], TOK, 1)))
            rows.append(jnp.where(low, pltpu.roll(one[PAD:], TOK, 1), two[PAD:]))
        joined.append(jnp.concatenate(rows, axis=0))
    joined = jnp.concatenate(joined, axis=1).astype(BF)
    return (x + dot(w_out, joined)).astype(BF)


def feed(states, gain, wh, wo):
    flat = states.astype(F32)
    normed = layer_norm(flat, gain)
    inner = jax.nn.gelu(dot(wh, normed)).astype(BF)
    return (flat + dot(wo, inner)).astype(BF)


def window_at(image, w, row):
    start = pl.multiple_of(w * WIN, WIN)
    return image[row : row + WIN, pl.ds(start, WIN), :].reshape(TOK, CHAN)


def windows_at(image, start, number, row):
    return jnp.concatenate([window_at(image, start + g, row) for g in range(number)], axis=0).T


def plane_row(planes, row, channels):
    halves = planes.shape[0]
    return jnp.concatenate(
        [planes[h, pl.ds(row, channels, stride=WIN), :] for h in range(halves)], axis=1
    )


def block_kernel(
    count, keep_in, dests_in, slots_in, pixels_in, table_in, gain_a_in, wqkv_in, wp_in,
    gain_m_in, wh_in, wo_in,
    restored, incoming,
    keep, dests, slots, keep_row, pixels, table, gain_a, wqkv, wp, gain_m, wh, wo, loads,
    planes, image, nxt_out, prv_out, nxt_buf, prv_buf, told, told_buf, w_in, w_out, w_hid, gains,
    strips, bias, states, doubled, result, active, outgoing, following, order,
    halo_send, halo_recv, tile_send, tile_recv,
):
    bands = lax.axis_size("band")
    me = lax.axis_index("band")
    right, left = lax.rem(me + 1, bands), lax.rem(me + bands - 1, bands)
    channels, rows, cols = pixels.shape
    windows = cols // WIN
    groups = windows // GROUP
    half = bands // 2
    far = jnp.where(me < half, half, 0)
    near = half - far
    halves = cols // LANES
    tiles = windows // TILE
    pairs = -(-tiles // bands)
    span = min(bands, tiles)
    mesh_id = pl.DeviceIdType.MESH
    moves = [
        pltpu.make_async_copy(source, target, loads.at[i])
        for i, (source, target) in enumerate(
            (
                (pixels_in, pixels), (wqkv_in, wqkv), (wp_in, wp), (table_in, table),
                (gain_a_in, gain_a), (gain_m_in, gain_m), (wh_in, wh), (wo_in, wo),
                (keep_in, keep_row), (keep_in, keep), (dests_in, dests),
                (slots_in, slots),
            )
        )
    ]
    for move in moves:
        move.start()

    barrier = pltpu.get_barrier_semaphore()

    def greet(i, _):
        peer = lax.rem(me + i, bands)
        pl.semaphore_signal(barrier, inc=1, device_id={"band": peer}, device_id_type=mesh_id)
        return 0

    lax.fori_loop(1, bands, greet, 0)

    moves[0].wait()
    for h in range(halves):
        part = pixels[:, :, h * LANES : (h + 1) * LANES].astype(F32)
        planes[h] = part.reshape(channels * rows, LANES)
    front = iota((channels, LANES), 1) < PART
    for r in range(0, SHIFT, 2):
        one = pltpu.roll(plane_row(planes, r, channels), cols - SHIFT, 1)
        two = pltpu.roll(plane_row(planes, r + 1, channels), cols - SHIFT, 1)
        lanes = slice(r * PART, (r + 2) * PART)
        for h in range(halves):
            a, b = one[:, h * LANES : (h + 1) * LANES], two[:, h * LANES : (h + 1) * LANES]
            nxt_out[2 * h, :, lanes] = jnp.where(front, a, pltpu.roll(b, PART, 1)).astype(BF)
            nxt_out[2 * h + 1, :, lanes] = jnp.where(front, pltpu.roll(a, PART, 1), b).astype(BF)
    pl.semaphore_wait(barrier, bands - 1)

    def nxt_copy(c):
        return pltpu.make_async_remote_copy(
            src_ref=nxt_out.at[c],
            dst_ref=nxt_buf.at[c],
            send_sem=halo_send.at[c],
            recv_sem=halo_recv.at[c],
            device_id={"band": left},
            device_id_type=mesh_id,
        )

    prv_copy = pltpu.make_async_remote_copy(
        src_ref=prv_out,
        dst_ref=prv_buf,
        send_sem=halo_send.at[groups],
        recv_sem=halo_recv.at[groups],
        device_id={"band": right},
        device_id_type=mesh_id,
    )
    told_copy = pltpu.make_async_remote_copy(
        src_ref=told,
        dst_ref=told_buf,
        send_sem=halo_send.at[groups + 1],
        recv_sem=halo_recv.at[groups + 1],
        device_id={"band": right},
        device_id_type=mesh_id,
    )
    for c in range(groups):
        nxt_copy(c).start()

    for r in range(rows):
        row = pltpu.roll(plane_row(planes, r, channels), cols - SHIFT, 1)
        if r >= rows - SHIFT:
            prv_out[r - rows + SHIFT] = row.astype(BF)
        image[SHIFT + r] = row.T
    prv_copy.start()
    for move in moves[1:]:
        move.wait()
    w_in[...] = dot_t(spread_heads(3 * DEPTH, 3 * CHAN), wqkv[...]).astype(BF)
    w_out[...] = dot(spread_heads(DEPTH, CHAN), wp[...]).T.astype(BF)
    w_hid[...] = wh[...].astype(F32).T.astype(BF)
    gains[0] = jnp.broadcast_to(gain_a[...], (LANES, channels)).T
    gains[1] = jnp.broadcast_to(gain_m[...], (LANES, channels)).T
    bias_strips(table, strips)
    bias_fill(strips, bias, me == bands - 1, me == 0)

    told[...] = jnp.zeros(told.shape, jnp.int32)
    told[:, 0:windows] = jnp.broadcast_to(keep_row[...], (8, windows))
    kept = told[...]
    tri = (LANES, LANES)
    before = lax.broadcasted_iota(jnp.int32, tri, 0) < lax.broadcasted_iota(jnp.int32, tri, 1)
    place = dot(kept.astype(F32).astype(BF), jnp.where(before, 1.0, 0.0).astype(BF))
    told[...] = jnp.where(place < count[0].astype(F32), kept, 0)

    def spread(flags):
        own_lane = (windows, LANES)
        diagonal = lax.broadcasted_iota(jnp.int32, own_lane, 0) == lax.broadcasted_iota(
            jnp.int32, own_lane, 1
        )
        chosen = jnp.where(diagonal, jnp.broadcast_to(flags[0:1].astype(F32), own_lane), 0.0)
        return dot(chosen.astype(BF), jnp.ones((LANES, channels), BF))

    told_copy.start()
    active[0] = spread(told[...])

    following[windows] = jnp.int32(windows)

    def scan(i, kept_so_far):
        w = windows - 1 - i
        following[w] = jnp.where(keep[0, w] == 1, w, following[w + 1])
        return kept_so_far + keep[0, w]

    live = jnp.minimum(lax.fori_loop(0, windows, scan, jnp.int32(0)), count[0])

    def rank(p, window):
        order[p] = jnp.minimum(window, windows - 1)
        return following[jnp.minimum(window + 1, windows)]

    lax.fori_loop(0, windows, rank, following[0])

    padded = channels + 4
    early = iota((padded, LANES), 1) < TOK

    def attend_windows(start, number, kind, row):
        def edge(g):
            return bias[2 * kind + (start + g == windows - 1).astype(jnp.int32)]

        x = windows_at(image, start, number, row)
        return attend(x, gains[0], w_in[...], w_out[...], edge)

    def step(c, _):
        nxt_copy(c).wait()
        block = nxt_buf[c].astype(F32).T
        cut = pl.ds(pl.multiple_of(c * PART, PART), PART)
        for r in range(SHIFT):
            image[SHIFT + rows + r, cut, :] = block[r * PART : (r + 1) * PART]
        own = attend_windows(c * GROUP, GROUP, 0, WIN)
        states[c] = own
        wide = jnp.concatenate([own.astype(F32), jnp.zeros((4, SIZE), F32)], axis=0)
        for pair in range(GROUP // 2):
            both = wide[:, pair * LANES : (pair + 1) * LANES]
            turned = pltpu.roll(both, TOK, 1)
            w = c * GROUP + 2 * pair
            doubled[w] = jnp.where(early, both, turned).astype(BF)
            doubled[w + 1] = jnp.where(early, turned, both).astype(BF)
        return 0

    lax.fori_loop(0, groups, step, 0)
    slot_row = iota((padded, LANES), 0) >= channels

    def pack(index, peer, j):
        t = jnp.int32(0)
        found = jnp.int32(0)
        for i in range(span):
            hit = dests[0, j * span + i] == peer
            t = jnp.where(hit, j * span + i, t)
            found = jnp.where(hit, 1, found)
        live_tile = (found > 0) & (t * TILE < live)
        slot = jnp.where(live_tile, slots[0, t], CAP).astype(F32)
        halves_of = []
        for p in range(TILE):
            position = t * TILE + p
            valid = live_tile & (position < live)
            value = doubled[order[position]]
            halves_of.append(jnp.where(valid, value, jnp.zeros_like(value)))
        value = jnp.where(early, halves_of[0], halves_of[1])
        outgoing[index] = jnp.where(slot_row, jnp.full((padded, LANES), slot, F32).astype(BF), value)

    def peer_of(n):
        return jnp.where(
            n < half, far + lax.rem(me + n, half), near + lax.rem(me - near + n - half + 1, half)
        )

    def tile_copy(n):
        return pltpu.make_async_remote_copy(
            src_ref=outgoing.at[pl.ds(n * pairs, pairs)],
            dst_ref=incoming.at[pl.ds(me * pairs, pairs)],
            send_sem=tile_send.at[n],
            recv_sem=tile_recv.at[n],
            device_id={"band": peer_of(n)},
            device_id_type=mesh_id,
        )

    def dispatch(n, _):
        for j in range(pairs):
            pack(n * pairs + j, peer_of(n), j)
        tile_copy(n).start()
        return 0

    lax.fori_loop(0, bands - 1, dispatch, 0)
    kept_here = (bands - 1) * pairs
    for j in range(pairs):
        pack(kept_here + j, me, j)
    incoming[pl.ds(me * pairs, pairs)] = outgoing[kept_here : kept_here + pairs]

    def blend(done, flags, w, row):
        cols_w = pl.ds(pl.multiple_of(w * WIN, WIN), WIN)
        chosen = active[flags, pl.ds(w, 1), :].reshape(1, 1, channels) > 0.5
        result[row : row + SHIFT, cols_w, :] = jnp.where(
            chosen,
            done.reshape(SHIFT, WIN, CHAN),
            image[SHIFT + row : 2 * SHIFT + row, cols_w, :],
        )

    told_copy.wait()
    active[1] = spread(told_buf[...])
    prv_copy.wait()
    for r in range(SHIFT):
        image[r] = prv_buf[r].astype(F32).T
    upper = iota((channels, WIDER * SIZE), 1) % TOK < HALF

    def finish(i, _):
        number = WIDER * GROUP
        prev = attend_windows(i * number, number, 1, 0)
        own = jnp.concatenate([states[i * WIDER + k] for k in range(WIDER)], axis=1)
        mine = jnp.where(upper, own, prev)
        done = feed(mine, gains[1], w_hid[...], wo[...]).astype(F32).T
        for g in range(number):
            w = i * number + g
            blend(done[g * TOK : g * TOK + HALF], 0, w, SHIFT)
            blend(done[g * TOK + HALF : (g + 1) * TOK], 1, w, 0)
        return 0

    lax.fori_loop(0, groups // WIDER, finish, 0)
    for r in range(rows):
        row = pltpu.roll(result[r].T, SHIFT, 1)
        for h in range(halves):
            planes[h, pl.ds(r, channels, stride=WIN), :] = row[:, h * LANES : (h + 1) * LANES]
    for h in range(halves):
        restored[:, :, h * LANES : (h + 1) * LANES] = (
            planes[h].reshape(channels, rows, LANES).astype(BF)
        )

    def collect(i, _):
        tile_copy(i).wait()
        return 0

    lax.fori_loop(0, bands - 1, collect, 0)


def place_kernel(incoming, restored, restored_out, work, planes, sem):
    total, padded, _ = incoming.shape
    channels = work.shape[0]
    move = pltpu.make_async_copy(restored, restored_out, sem)
    move.start()
    head = incoming[:, padded - 8 :, :].astype(F32)
    head = jnp.max(jnp.where(iota(head.shape, 1) >= 4, head, 0.0), axis=1)
    slot = jnp.max(head, axis=1, keepdims=True).astype(jnp.int32)
    match = slot == iota((total, LANES), 1)
    source = jnp.where(match, iota((total, LANES), 0), -1).astype(F32)
    source = jnp.max(source, axis=0, keepdims=True).astype(jnp.int32)
    for k in range(CAP):
        known = source[0, k] >= 0
        block = incoming[jnp.maximum(source[0, k], 0)].astype(F32)[:channels]
        planes[pl.ds(k, channels, stride=CAP), :] = jnp.where(known, block, 0.0)
    work[...] = planes[...].reshape(channels, CAP, TILE * TOK).astype(BF)
    move.wait()


def shards(
    pixels, keep_mask, band_counts, plan_dest, plan_slot, bias_table, gain_attn, qkv_weight,
    proj_weight, gain_mlp, hidden_weight, output_weight,
):
    bands = lax.axis_size("band")
    rows, cols, channels = pixels.shape
    windows = cols // WIN
    halves = cols // LANES
    tiles = windows // TILE
    pairs = -(-tiles // bands)
    smem = pl.BlockSpec(memory_space=pltpu.SMEM)
    vmem = pl.BlockSpec(memory_space=pltpu.VMEM)
    tile_shape = (bands * pairs, channels + 4, LANES)
    groups = windows // GROUP
    nxt_shape = (groups, channels, SHIFT * PART)
    operands = (
        keep_mask, plan_dest, plan_slot, jnp.transpose(pixels, (2, 0, 1)),
        bias_table.T, gain_attn[None], qkv_weight, proj_weight, gain_mlp[None], hidden_weight,
        output_weight.T,
    )
    restored, incoming = pl.pallas_call(
        block_kernel,
        out_shape=(
            jax.ShapeDtypeStruct((channels, rows, cols), BF),
            jax.ShapeDtypeStruct(tile_shape, BF),
        ),
        in_specs=[smem] + [pl.BlockSpec(memory_space=pltpu.HBM)] * len(operands),
        out_specs=(vmem, vmem),
        scratch_shapes=[
            pltpu.SMEM(operands[0].shape, jnp.int32),
            pltpu.SMEM(operands[1].shape, jnp.int32),
            pltpu.SMEM(operands[2].shape, jnp.int32),
            pltpu.VMEM(operands[0].shape, jnp.int32),
            *(pltpu.VMEM(operand.shape, operand.dtype) for operand in operands[3:]),
            pltpu.SemaphoreType.DMA((len(operands) + 1,)),
            pltpu.VMEM((halves, channels * rows, LANES), F32),
            pltpu.VMEM((rows + 2 * SHIFT, cols, channels), F32),
            pltpu.VMEM(nxt_shape, BF),
            pltpu.VMEM((SHIFT, channels, cols), BF),
            pltpu.VMEM(nxt_shape, BF),
            pltpu.VMEM((SHIFT, channels, cols), BF),
            pltpu.VMEM((8, LANES), jnp.int32),
            pltpu.VMEM((8, LANES), jnp.int32),
            pltpu.VMEM((3 * DEPTH, channels), BF),
            pltpu.VMEM((channels, DEPTH), BF),
            pltpu.VMEM((hidden_weight.shape[1], channels), BF),
            pltpu.VMEM((2, channels, LANES), F32),
            pltpu.VMEM((8 * WIN, LANES), F32),
            pltpu.VMEM((4, TOK, QUERIES), F32),
            pltpu.VMEM((groups, channels, SIZE), BF),
            pltpu.VMEM((windows, channels + 4, LANES), BF),
            pltpu.VMEM((rows, cols, channels), F32),
            pltpu.VMEM((2, windows, channels), F32),
            pltpu.VMEM(tile_shape, BF),
            pltpu.SMEM((windows + 1,), jnp.int32),
            pltpu.SMEM((windows,), jnp.int32),
            pltpu.SemaphoreType.DMA((groups + 2,)),
            pltpu.SemaphoreType.DMA((groups + 2,)),
            pltpu.SemaphoreType.DMA((bands,)),
            pltpu.SemaphoreType.DMA((bands,)),
        ],
        compiler_params=pltpu.CompilerParams(
            vmem_limit_bytes=40 * 1024 * 1024, collective_id=0, has_side_effects=True
        ),
        cost_estimate=pl.CostEstimate(flops=10**10, bytes_accessed=10**7, transcendentals=10**6),
        name="block",
    )(band_counts, *(pltpu.with_memory_space_constraint(value, pltpu.HBM) for value in operands))
    restored, work = pl.pallas_call(
        place_kernel,
        out_shape=(
            jax.ShapeDtypeStruct((channels, rows, cols), BF),
            jax.ShapeDtypeStruct((channels, CAP, TILE * TOK), BF),
        ),
        in_specs=[vmem, vmem],
        out_specs=(pl.BlockSpec(memory_space=pl.ANY), vmem),
        scratch_shapes=[
            pltpu.VMEM((channels * CAP, TILE * TOK), F32),
            pltpu.SemaphoreType.DMA,
        ],
        compiler_params=pltpu.CompilerParams(vmem_limit_bytes=16 * 1024 * 1024),
        name="place",
    )(incoming, restored)
    return jnp.transpose(restored, (1, 2, 0)), jnp.transpose(work, (1, 2, 0))


def solution(mesh):
    split = P(("img", "band"))
    in_specs = (split,) * 5 + (P(),) * 7
    return jax.shard_map(shards, mesh=mesh, in_specs=in_specs, out_specs=(split, split), check_vma=False)
```

```python
import jax
import jax.numpy as jnp
from jax import lax
from jax.experimental import pallas as pl
from jax.experimental.pallas import tpu as pltpu
from jax.sharding import PartitionSpec as P

CHAN = 180
HEADS = 6
WIN = 8
TILE = 2
SHIFT = 4
CAP = 8
TOK = WIN * WIN
HALF = TOK // 2
HEAD_DIM = CHAN // HEADS
GROUP = 8
WIDER = 2
SIZE = GROUP * TOK
PART = GROUP * WIN
PAD = 32
DEPTH = HEADS * PAD
QUERIES = HEADS * TOK
LANES = 128
SLOT_LANE = 120

EPSILON = 1e-05
BF = jnp.bfloat16
F32 = jnp.float32


def layer_norm(values, gain):
    center = values - jnp.sum(values, axis=0, keepdims=True) * (1.0 / CHAN)
    spread = jnp.sum(center * center, axis=0, keepdims=True) * (1.0 / CHAN)
    scaled = center * lax.rsqrt(spread + EPSILON)
    parts = [scaled[:, i : i + LANES] * gain for i in range(0, values.shape[1], LANES)]
    return jnp.concatenate(parts, axis=1).astype(BF)


def dot(a, b):
    return jnp.dot(a, b, preferred_element_type=F32)


def dot_t(a, b):
    return lax.dot_general(a, b, (((1,), (1,)), ((), ())), preferred_element_type=F32)


def iota(shape, axis):
    return lax.broadcasted_iota(jnp.int32, shape, axis)


def bias_strips(table, strips):
    heads, entries = table.shape
    values = jnp.concatenate([table[...], jnp.zeros((8 - heads, entries), F32)], axis=0)
    high = values.astype(BF).astype(F32)
    middle = (values - high).astype(BF).astype(F32)
    low = values - high - middle
    parts = jnp.concatenate([high, middle, low], axis=0).astype(BF)
    shape = (entries, WIN * LANES)
    entry, lane = iota(shape, 0), iota(shape, 1)
    step = (lane % LANES) // WIN
    wanted = step * (2 * WIN - 1) + lane % WIN - lane // LANES + WIN - 1
    pick = jnp.where((entry == wanted) & (step < 2 * WIN - 1), 1.0, 0.0).astype(BF)
    found = dot(parts, pick)
    found = found[0:8] + found[8:16] + found[16:24]
    for c in range(WIN):
        strips[pl.ds(c, 8, stride=WIN), :] = found[:, c * LANES : (c + 1) * LANES]


def bias_fill(strips, bias, own_last, prev_last):
    first_half = iota((WIN, LANES), 1) < TOK
    for r in range(WIN):
        by = 2 * LANES - (WIN - 1 - r) * WIN
        tiles = []
        for h in range(0, HEADS, 2):
            even = strips[h * WIN : (h + 1) * WIN, :]
            odd = strips[(h + 1) * WIN : (h + 2) * WIN, :]
            tiles.append(
                jnp.where(
                    first_half,
                    pltpu.roll(even, by % LANES, 1),
                    pltpu.roll(odd, (by + TOK) % LANES, 1),
                )
            )
        base = jnp.concatenate(tiles, axis=1)
        shape = (WIN, QUERIES)
        key, query = iota(shape, 0), iota(shape, 1) % TOK
        rows_differ = (query // WIN >= SHIFT) != (r >= SHIFT)
        cols_differ = (key >= SHIFT) != (query % WIN >= SHIFT)
        rows = slice(r * WIN, (r + 1) * WIN)
        for k, last in enumerate((own_last, prev_last)):
            row_pen = jnp.where(rows_differ, jnp.where(last, -100.0, 0.0).astype(F32), 0.0)
            bias[2 * k, rows] = base + row_pen
            bias[2 * k + 1, rows] = base + jnp.where(cols_differ, -100.0, row_pen)


def spread_heads(rows, cols):
    row, col = iota((rows, cols), 0), iota((rows, cols), 1)
    inside = row % DEPTH
    wanted = row // DEPTH * CHAN + inside // PAD * HEAD_DIM + inside % PAD
    return jnp.where((inside % PAD < HEAD_DIM) & (wanted == col), 1.0, 0.0).astype(BF)


def attend(x, gain, w_in, w_out, bias_of):
    normed = layer_norm(x, gain)
    mixed = dot(w_in, normed)
    q = mixed[0:DEPTH] * HEAD_DIM ** (-0.5)
    k = mixed[DEPTH : 2 * DEPTH].T.astype(BF)
    v = mixed[2 * DEPTH :].astype(BF)
    low = iota((PAD, LANES), 1) < TOK
    blank = jnp.zeros((PAD, LANES), F32)
    joined = []
    for pair in range(x.shape[1] // LANES):
        lanes = slice(pair * LANES, (pair + 1) * LANES)
        q_pair = q[:, lanes]
        q_turn = pltpu.roll(q_pair, TOK, 1)
        weights = []
        for side in range(2):
            g = 2 * pair + side
            blocks = []
            for h in range(HEADS):
                part = slice(h * PAD, (h + 1) * PAD)
                value = q_pair[part] if h % 2 == side else q_turn[part]
                value = jnp.where(low if h % 2 == 0 else ~low, value, 0.0)
                row = [blank] * (HEADS // 2)
                row[h // 2] = value
                blocks.append(jnp.concatenate(row, axis=1))
            spread_q = jnp.concatenate(blocks, axis=0).astype(BF)
            scores = dot(k[g * TOK : (g + 1) * TOK], spread_q) + bias_of(g)
            top = jnp.max(scores, axis=0, keepdims=True)
            grown = jnp.exp(scores - top)
            weights.append((grown * (1.0 / jnp.sum(grown, axis=0, keepdims=True))).astype(BF))
        rows = []
        none = jnp.zeros((TOK, LANES), BF)
        for j in range(HEADS // 2):
            cut = slice(j * LANES, (j + 1) * LANES)
            both = jnp.concatenate(
                [
                    jnp.concatenate([weights[0][:, cut], none], axis=1),
                    jnp.concatenate([none, weights[1][:, cut]], axis=1),
                ],
                axis=0,
            )
            found = dot(v[2 * j * PAD : 2 * (j + 1) * PAD, lanes], both)
            one, two = found[:, :LANES], found[:, LANES:]
            rows.append(jnp.where(low, one[:PAD], pltpu.roll(two[:PAD], TOK, 1)))
            rows.append(jnp.where(low, pltpu.roll(one[PAD:], TOK, 1), two[PAD:]))
        joined.append(jnp.concatenate(rows, axis=0))
    joined = jnp.concatenate(joined, axis=1).astype(BF)
    return (x + dot(w_out, joined)).astype(BF)


def feed(states, gain, wh, wo):
    flat = states.astype(F32)
    normed = layer_norm(flat, gain)
    inner = jax.nn.gelu(dot(wh, normed)).astype(BF)
    return (flat + dot(wo, inner)).astype(BF)


def window_at(image, w, row):
    start = pl.multiple_of(w * WIN, WIN)
    return image[row : row + WIN, pl.ds(start, WIN), :].reshape(TOK, CHAN)


def windows_at(image, start, number, row):
    return jnp.concatenate([window_at(image, start + g, row) for g in range(number)], axis=0).T


def plane_row(planes, row, channels):
    halves = planes.shape[0]
    return jnp.concatenate(
        [planes[h, pl.ds(row, channels, stride=WIN), :] for h in range(halves)], axis=1
    )


def block_kernel(
    count, keep_in, dests_in, slots_in, pixels_in, table_in, gain_a_in, wqkv_in, wp_in,
    gain_m_in, wh_in, wo_in,
    restored, incoming,
    keep, dests, slots, keep_row, pixels, table, gain_a, wqkv, wp, gain_m, wh, wo, loads,
    planes, image, nxt_out, prv_out, nxt_buf, prv_buf, told, told_buf, w_in, w_out, w_hid, gains,
    strips, bias, states, doubled, result, active, outgoing, following, order,
    halo_send, halo_recv, tile_send, tile_recv,
):
    bands = lax.axis_size("band")
    me = lax.axis_index("band")
    right, left = lax.rem(me + 1, bands), lax.rem(me + bands - 1, bands)
    channels, rows, cols = pixels.shape
    windows = cols // WIN
    groups = windows // GROUP
    half = bands // 2
    fourth = half // 2
    far = jnp.where(me < half, half, 0)
    near = half - far
    halves = cols // LANES
    tiles = windows // TILE
    pairs = -(-tiles // bands)
    span = min(bands, tiles)
    mesh_id = pl.DeviceIdType.MESH
    moves = [
        pltpu.make_async_copy(source, target, loads.at[i])
        for i, (source, target) in enumerate(
            (
                (pixels_in, pixels), (wqkv_in, wqkv), (wp_in, wp), (table_in, table),
                (gain_a_in, gain_a), (gain_m_in, gain_m), (wh_in, wh), (wo_in, wo),
                (keep_in, keep_row), (keep_in, keep), (dests_in, dests),
                (slots_in, slots),
            )
        )
    ]
    for move in moves:
        move.start()

    barrier = pltpu.get_barrier_semaphore()

    def greet(i, _):
        peer = lax.rem(me + i, bands)
        pl.semaphore_signal(barrier, inc=1, device_id={"band": peer}, device_id_type=mesh_id)
        return 0

    lax.fori_loop(1, bands, greet, 0)

    moves[0].wait()
    for h in range(halves):
        part = pixels[:, :, h * LANES : (h + 1) * LANES].astype(F32)
        planes[h] = part.reshape(channels * rows, LANES)
    front = iota((channels, LANES), 1) < PART
    for r in range(0, SHIFT, 2):
        one = pltpu.roll(plane_row(planes, r, channels), cols - SHIFT, 1)
        two = pltpu.roll(plane_row(planes, r + 1, channels), cols - SHIFT, 1)
        lanes = slice(r * PART, (r + 2) * PART)
        for h in range(halves):
            a, b = one[:, h * LANES : (h + 1) * LANES], two[:, h * LANES : (h + 1) * LANES]
            nxt_out[2 * h, :, lanes] = jnp.where(front, a, pltpu.roll(b, PART, 1)).astype(BF)
            nxt_out[2 * h + 1, :, lanes] = jnp.where(front, pltpu.roll(a, PART, 1), b).astype(BF)
    pl.semaphore_wait(barrier, bands - 1)

    def nxt_copy(c):
        return pltpu.make_async_remote_copy(
            src_ref=nxt_out.at[c],
            dst_ref=nxt_buf.at[c],
            send_sem=halo_send.at[c],
            recv_sem=halo_recv.at[c],
            device_id={"band": left},
            device_id_type=mesh_id,
        )

    odd = lax.rem(me, 2) == 1
    fold = SHIFT // 2

    def prv_send(part, source, start, device, mark):
        first = part * fold
        return pltpu.make_async_remote_copy(
            src_ref=source.at[first : first + fold],
            dst_ref=prv_buf.at[start + first : start + first + fold],
            send_sem=halo_send.at[groups + 1 + 2 * mark + part],
            recv_sem=halo_recv.at[groups + 1 + 2 * mark + part],
            device_id={"band": device},
            device_id_type=mesh_id,
        )

    direct = [prv_send(part, prv_out, 0, right, 0) for part in range(2)]
    relay = [prv_send(part, prv_out, SHIFT, lax.rem(me + 2, bands), 1) for part in range(2)]
    held = prv_buf.at[SHIFT:]
    forward = [prv_send(part, held, 0, left, 0) for part in range(2)]
    told_copy = pltpu.make_async_remote_copy(
        src_ref=told,
        dst_ref=told_buf,
        send_sem=halo_send.at[groups],
        recv_sem=halo_recv.at[groups],
        device_id={"band": right},
        device_id_type=mesh_id,
    )
    for c in range(groups):
        nxt_copy(c).start()

    for r in range(rows):
        row = pltpu.roll(plane_row(planes, r, channels), cols - SHIFT, 1)
        if r >= rows - SHIFT:
            prv_out[r - rows + SHIFT] = row.astype(BF)
        image[SHIFT + r] = row.T
    @pl.when(odd)
    def _():
        for part in range(2):
            relay[part].start()

    for move in moves[1:]:
        move.wait()
    w_in[...] = dot_t(spread_heads(3 * DEPTH, 3 * CHAN), wqkv[...]).astype(BF)
    w_out[...] = dot(spread_heads(DEPTH, CHAN), wp[...]).T.astype(BF)
    w_hid[...] = wh[...].astype(F32).T.astype(BF)
    gains[0] = jnp.broadcast_to(gain_a[...], (LANES, channels)).T
    gains[1] = jnp.broadcast_to(gain_m[...], (LANES, channels)).T
    bias_strips(table, strips)
    bias_fill(strips, bias, me == bands - 1, me == 0)

    told[...] = jnp.zeros(told.shape, jnp.int32)
    told[:, 0:windows] = jnp.broadcast_to(keep_row[...], (8, windows))
    kept = told[...]
    tri = (LANES, LANES)
    before = lax.broadcasted_iota(jnp.int32, tri, 0) < lax.broadcasted_iota(jnp.int32, tri, 1)
    place = dot(kept.astype(F32).astype(BF), jnp.where(before, 1.0, 0.0).astype(BF))
    told[...] = jnp.where(place < count[0].astype(F32), kept, 0)

    def spread(flags):
        own_lane = (windows, LANES)
        diagonal = lax.broadcasted_iota(jnp.int32, own_lane, 0) == lax.broadcasted_iota(
            jnp.int32, own_lane, 1
        )
        chosen = jnp.where(diagonal, jnp.broadcast_to(flags[0:1].astype(F32), own_lane), 0.0)
        return dot(chosen.astype(BF), jnp.ones((LANES, channels), BF))

    told_copy.start()
    active[0] = spread(told[...])

    following[windows] = jnp.int32(windows)

    def scan(i, kept_so_far):
        w = windows - 1 - i
        following[w] = jnp.where(keep[0, w] == 1, w, following[w + 1])
        return kept_so_far + keep[0, w]

    live = jnp.minimum(lax.fori_loop(0, windows, scan, jnp.int32(0)), count[0])

    def rank(p, window):
        order[p] = jnp.minimum(window, windows - 1)
        return following[jnp.minimum(window + 1, windows)]

    lax.fori_loop(0, windows, rank, following[0])

    padded = channels + 4
    early = iota((padded, LANES), 1) < TOK

    def attend_windows(start, number, kind, row):
        def edge(g):
            return bias[2 * kind + (start + g == windows - 1).astype(jnp.int32)]

        x = windows_at(image, start, number, row)
        return attend(x, gains[0], w_in[...], w_out[...], edge)

    def step(c, _):
        nxt_copy(c).wait()

        @pl.when((c == groups - 1) & odd)
        def _():
            relay[0].wait()
            forward[0].start()

        @pl.when((c == groups - 1) & ~odd)
        def _():
            for part in range(2):
                direct[part].start()

        block = nxt_buf[c].astype(F32).T
        cut = pl.ds(pl.multiple_of(c * PART, PART), PART)
        for r in range(SHIFT):
            image[SHIFT + rows + r, cut, :] = block[r * PART : (r + 1) * PART]
        own = attend_windows(c * GROUP, GROUP, 0, WIN)
        states[c] = own
        wide = jnp.concatenate([own.astype(F32), jnp.zeros((4, SIZE), F32)], axis=0)
        for pair in range(GROUP // 2):
            both = wide[:, pair * LANES : (pair + 1) * LANES]
            turned = pltpu.roll(both, TOK, 1)
            w = c * GROUP + 2 * pair
            doubled[w] = jnp.where(early, both, turned).astype(BF)
            doubled[w + 1] = jnp.where(early, turned, both).astype(BF)
        return 0

    lax.fori_loop(0, groups, step, 0)

    @pl.when(odd)
    def _():
        relay[1].wait()
        forward[1].start()

    slot_row = iota((padded, LANES), 0) >= channels

    def pack(index, peer, j):
        t = jnp.int32(0)
        found = jnp.int32(0)
        for i in range(span):
            hit = dests[0, j * span + i] == peer
            t = jnp.where(hit, j * span + i, t)
            found = jnp.where(hit, 1, found)
        live_tile = (found > 0) & (t * TILE < live)
        slot = jnp.where(live_tile, slots[0, t], CAP).astype(F32)
        halves_of = []
        for p in range(TILE):
            position = t * TILE + p
            valid = live_tile & (position < live)
            value = doubled[order[position]]
            halves_of.append(jnp.where(valid, value, jnp.zeros_like(value)))
        value = jnp.where(early, halves_of[0], halves_of[1])
        outgoing[index] = jnp.where(slot_row, jnp.full((padded, LANES), slot, F32).astype(BF), value)

    def peer_of(n):
        away = n >= half
        m = jnp.where(away, n - half + 1, n)
        cross = (m >= fourth).astype(jnp.int32)
        row = lax.rem(lax.div(lax.rem(me, half), 2) + m, fourth)
        side = lax.rem(lax.rem(me, 2) + cross, 2)
        return jnp.where(away, near, far) + 2 * row + side

    def tile_copy(n):
        return pltpu.make_async_remote_copy(
            src_ref=outgoing.at[pl.ds(n * pairs, pairs)],
            dst_ref=incoming.at[pl.ds(me * pairs, pairs)],
            send_sem=tile_send.at[n],
            recv_sem=tile_recv.at[n],
            device_id={"band": peer_of(n)},
            device_id_type=mesh_id,
        )

    def dispatch(n, _):
        for j in range(pairs):
            pack(n * pairs + j, peer_of(n), j)
        tile_copy(n).start()
        return 0

    lax.fori_loop(0, bands - 1, dispatch, 0)
    kept_here = (bands - 1) * pairs
    for j in range(pairs):
        pack(kept_here + j, me, j)
    incoming[pl.ds(me * pairs, pairs)] = outgoing[kept_here : kept_here + pairs]

    def blend(done, flags, w, row):
        cols_w = pl.ds(pl.multiple_of(w * WIN, WIN), WIN)
        chosen = active[flags, pl.ds(w, 1), :].reshape(1, 1, channels) > 0.5
        result[row : row + SHIFT, cols_w, :] = jnp.where(
            chosen,
            done.reshape(SHIFT, WIN, CHAN),
            image[SHIFT + row : 2 * SHIFT + row, cols_w, :],
        )

    told_copy.wait()
    active[1] = spread(told_buf[...])
    for part in range(2):
        direct[part].wait_recv()

    @pl.when(~odd)
    def _():
        for part in range(2):
            direct[part].wait_send()

    @pl.when(odd)
    def _():
        for part in range(2):
            forward[part].wait_send()

    for r in range(SHIFT):
        image[r] = prv_buf[r].astype(F32).T
    upper = iota((channels, WIDER * SIZE), 1) % TOK < HALF

    def finish(i, _):
        number = WIDER * GROUP
        prev = attend_windows(i * number, number, 1, 0)
        own = jnp.concatenate([states[i * WIDER + k] for k in range(WIDER)], axis=1)
        mine = jnp.where(upper, own, prev)
        done = feed(mine, gains[1], w_hid[...], wo[...]).astype(F32).T
        for g in range(number):
            w = i * number + g
            blend(done[g * TOK : g * TOK + HALF], 0, w, SHIFT)
            blend(done[g * TOK + HALF : (g + 1) * TOK], 1, w, 0)
        return 0

    lax.fori_loop(0, groups // WIDER, finish, 0)
    for r in range(rows):
        row = pltpu.roll(result[r].T, SHIFT, 1)
        for h in range(halves):
            planes[h, pl.ds(r, channels, stride=WIN), :] = row[:, h * LANES : (h + 1) * LANES]
    for h in range(halves):
        restored[:, :, h * LANES : (h + 1) * LANES] = (
            planes[h].reshape(channels, rows, LANES).astype(BF)
        )

    def collect(i, _):
        tile_copy(i).wait()
        return 0

    lax.fori_loop(0, bands - 1, collect, 0)


def place_kernel(incoming, restored, restored_out, work, planes, sem):
    total, padded, _ = incoming.shape
    channels = work.shape[0]
    move = pltpu.make_async_copy(restored, restored_out, sem)
    move.start()
    head = incoming[:, padded - 8 :, :].astype(F32)
    head = jnp.max(jnp.where(iota(head.shape, 1) >= 4, head, 0.0), axis=1)
    slot = jnp.max(head, axis=1, keepdims=True).astype(jnp.int32)
    match = slot == iota((total, LANES), 1)
    source = jnp.where(match, iota((total, LANES), 0), -1).astype(F32)
    source = jnp.max(source, axis=0, keepdims=True).astype(jnp.int32)
    for k in range(CAP):
        known = source[0, k] >= 0
        block = incoming[jnp.maximum(source[0, k], 0)].astype(F32)[:channels]
        planes[pl.ds(k, channels, stride=CAP), :] = jnp.where(known, block, 0.0)
    work[...] = planes[...].reshape(channels, CAP, TILE * TOK).astype(BF)
    move.wait()


def shards(
    pixels, keep_mask, band_counts, plan_dest, plan_slot, bias_table, gain_attn, qkv_weight,
    proj_weight, gain_mlp, hidden_weight, output_weight,
):
    bands = lax.axis_size("band")
    rows, cols, channels = pixels.shape
    windows = cols // WIN
    halves = cols // LANES
    tiles = windows // TILE
    pairs = -(-tiles // bands)
    smem = pl.BlockSpec(memory_space=pltpu.SMEM)
    vmem = pl.BlockSpec(memory_space=pltpu.VMEM)
    tile_shape = (bands * pairs, channels + 4, LANES)
    groups = windows // GROUP
    nxt_shape = (groups, channels, SHIFT * PART)
    operands = (
        keep_mask, plan_dest, plan_slot, jnp.transpose(pixels, (2, 0, 1)),
        bias_table.T, gain_attn[None], qkv_weight, proj_weight, gain_mlp[None], hidden_weight,
        output_weight.T,
    )
    restored, incoming = pl.pallas_call(
        block_kernel,
        out_shape=(
            jax.ShapeDtypeStruct((channels, rows, cols), BF),
            jax.ShapeDtypeStruct(tile_shape, BF),
        ),
        in_specs=[smem] + [pl.BlockSpec(memory_space=pltpu.HBM)] * len(operands),
        out_specs=(vmem, vmem),
        scratch_shapes=[
            pltpu.SMEM(operands[0].shape, jnp.int32),
            pltpu.SMEM(operands[1].shape, jnp.int32),
            pltpu.SMEM(operands[2].shape, jnp.int32),
            pltpu.VMEM(operands[0].shape, jnp.int32),
            *(pltpu.VMEM(operand.shape, operand.dtype) for operand in operands[3:]),
            pltpu.SemaphoreType.DMA((len(operands) + 1,)),
            pltpu.VMEM((halves, channels * rows, LANES), F32),
            pltpu.VMEM((rows + 2 * SHIFT, cols, channels), F32),
            pltpu.VMEM(nxt_shape, BF),
            pltpu.VMEM((SHIFT, channels, cols), BF),
            pltpu.VMEM(nxt_shape, BF),
            pltpu.VMEM((2 * SHIFT, channels, cols), BF),
            pltpu.VMEM((8, LANES), jnp.int32),
            pltpu.VMEM((8, LANES), jnp.int32),
            pltpu.VMEM((3 * DEPTH, channels), BF),
            pltpu.VMEM((channels, DEPTH), BF),
            pltpu.VMEM((hidden_weight.shape[1], channels), BF),
            pltpu.VMEM((2, channels, LANES), F32),
            pltpu.VMEM((8 * WIN, LANES), F32),
            pltpu.VMEM((4, TOK, QUERIES), F32),
            pltpu.VMEM((groups, channels, SIZE), BF),
            pltpu.VMEM((windows, channels + 4, LANES), BF),
            pltpu.VMEM((rows, cols, channels), F32),
            pltpu.VMEM((2, windows, channels), F32),
            pltpu.VMEM(tile_shape, BF),
            pltpu.SMEM((windows + 1,), jnp.int32),
            pltpu.SMEM((windows,), jnp.int32),
            pltpu.SemaphoreType.DMA((groups + 5,)),
            pltpu.SemaphoreType.DMA((groups + 5,)),
            pltpu.SemaphoreType.DMA((bands,)),
            pltpu.SemaphoreType.DMA((bands,)),
        ],
        compiler_params=pltpu.CompilerParams(
            vmem_limit_bytes=40 * 1024 * 1024, collective_id=0, has_side_effects=True
        ),
        cost_estimate=pl.CostEstimate(flops=10**10, bytes_accessed=10**7, transcendentals=10**6),
        name="block",
    )(band_counts, *(pltpu.with_memory_space_constraint(value, pltpu.HBM) for value in operands))
    restored, work = pl.pallas_call(
        place_kernel,
        out_shape=(
            jax.ShapeDtypeStruct((channels, rows, cols), BF),
            jax.ShapeDtypeStruct((channels, CAP, TILE * TOK), BF),
        ),
        in_specs=[vmem, vmem],
        out_specs=(pl.BlockSpec(memory_space=pl.ANY), vmem),
        scratch_shapes=[
            pltpu.VMEM((channels * CAP, TILE * TOK), F32),
            pltpu.SemaphoreType.DMA,
        ],
        compiler_params=pltpu.CompilerParams(vmem_limit_bytes=16 * 1024 * 1024),
        name="place",
    )(incoming, restored)
    return jnp.transpose(restored, (1, 2, 0)), jnp.transpose(work, (1, 2, 0))


def solution(mesh):
    split = P(("img", "band"))
    in_specs = (split,) * 5 + (P(),) * 7
    return jax.shard_map(shards, mesh=mesh, in_specs=in_specs, out_specs=(split, split), check_vma=False)
```

```python
import jax
import jax.numpy as jnp
from jax import lax
from jax.experimental import pallas as pl
from jax.experimental.pallas import tpu as pltpu
from jax.sharding import PartitionSpec as P

CHAN = 180
HEADS = 6
WIN = 8
TILE = 2
SHIFT = 4
CAP = 8
TOK = WIN * WIN
HALF = TOK // 2
HEAD_DIM = CHAN // HEADS
GROUP = 8
WIDER = 2
SIZE = GROUP * TOK
PART = GROUP * WIN
PAD = 32
DEPTH = HEADS * PAD
QUERIES = HEADS * TOK
LANES = 128
SLOT_LANE = 120

EPSILON = 1e-05
BF = jnp.bfloat16
F32 = jnp.float32


def layer_norm(values, gain):
    center = values - jnp.sum(values, axis=0, keepdims=True) * (1.0 / CHAN)
    spread = jnp.sum(center * center, axis=0, keepdims=True) * (1.0 / CHAN)
    scaled = center * lax.rsqrt(spread + EPSILON)
    parts = [scaled[:, i : i + LANES] * gain for i in range(0, values.shape[1], LANES)]
    return jnp.concatenate(parts, axis=1).astype(BF)


def dot(a, b):
    return jnp.dot(a, b, preferred_element_type=F32)


def dot_t(a, b):
    return lax.dot_general(a, b, (((1,), (1,)), ((), ())), preferred_element_type=F32)


def iota(shape, axis):
    return lax.broadcasted_iota(jnp.int32, shape, axis)


def bias_strips(table, strips):
    heads, entries = table.shape
    values = jnp.concatenate([table[...], jnp.zeros((8 - heads, entries), F32)], axis=0)
    high = values.astype(BF).astype(F32)
    middle = (values - high).astype(BF).astype(F32)
    low = values - high - middle
    parts = jnp.concatenate([high, middle, low], axis=0).astype(BF)
    shape = (entries, WIN * LANES)
    entry, lane = iota(shape, 0), iota(shape, 1)
    step = (lane % LANES) // WIN
    wanted = step * (2 * WIN - 1) + lane % WIN - lane // LANES + WIN - 1
    pick = jnp.where((entry == wanted) & (step < 2 * WIN - 1), 1.0, 0.0).astype(BF)
    found = dot(parts, pick)
    found = found[0:8] + found[8:16] + found[16:24]
    for c in range(WIN):
        strips[pl.ds(c, 8, stride=WIN), :] = found[:, c * LANES : (c + 1) * LANES]


def bias_fill(strips, bias, own_last, prev_last):
    first_half = iota((WIN, LANES), 1) < TOK
    for r in range(WIN):
        by = 2 * LANES - (WIN - 1 - r) * WIN
        tiles = []
        for h in range(0, HEADS, 2):
            even = strips[h * WIN : (h + 1) * WIN, :]
            odd = strips[(h + 1) * WIN : (h + 2) * WIN, :]
            tiles.append(
                jnp.where(
                    first_half,
                    pltpu.roll(even, by % LANES, 1),
                    pltpu.roll(odd, (by + TOK) % LANES, 1),
                )
            )
        base = jnp.concatenate(tiles, axis=1)
        shape = (WIN, QUERIES)
        key, query = iota(shape, 0), iota(shape, 1) % TOK
        rows_differ = (query // WIN >= SHIFT) != (r >= SHIFT)
        cols_differ = (key >= SHIFT) != (query % WIN >= SHIFT)
        rows = slice(r * WIN, (r + 1) * WIN)
        for k, last in enumerate((own_last, prev_last)):
            row_pen = jnp.where(rows_differ, jnp.where(last, -100.0, 0.0).astype(F32), 0.0)
            bias[2 * k, rows] = base + row_pen
            bias[2 * k + 1, rows] = base + jnp.where(cols_differ, -100.0, row_pen)


def spread_heads(rows, cols):
    row, col = iota((rows, cols), 0), iota((rows, cols), 1)
    inside = row % DEPTH
    wanted = row // DEPTH * CHAN + inside // PAD * HEAD_DIM + inside % PAD
    return jnp.where((inside % PAD < HEAD_DIM) & (wanted == col), 1.0, 0.0).astype(BF)


def attend(x, gain, w_in, w_out, bias_of):
    normed = layer_norm(x, gain)
    mixed = dot(w_in, normed)
    q = mixed[0:DEPTH] * HEAD_DIM ** (-0.5)
    k = mixed[DEPTH : 2 * DEPTH].T.astype(BF)
    v = mixed[2 * DEPTH :].astype(BF)
    low = iota((PAD, LANES), 1) < TOK
    blank = jnp.zeros((PAD, LANES), F32)
    joined = []
    for pair in range(x.shape[1] // LANES):
        lanes = slice(pair * LANES, (pair + 1) * LANES)
        q_pair = q[:, lanes]
        q_turn = pltpu.roll(q_pair, TOK, 1)
        weights = []
        for side in range(2):
            g = 2 * pair + side
            blocks = []
            for h in range(HEADS):
                part = slice(h * PAD, (h + 1) * PAD)
                value = q_pair[part] if h % 2 == side else q_turn[part]
                value = jnp.where(low if h % 2 == 0 else ~low, value, 0.0)
                row = [blank] * (HEADS // 2)
                row[h // 2] = value
                blocks.append(jnp.concatenate(row, axis=1))
            spread_q = jnp.concatenate(blocks, axis=0).astype(BF)
            scores = dot(k[g * TOK : (g + 1) * TOK], spread_q) + bias_of(g)
            top = jnp.max(scores, axis=0, keepdims=True)
            grown = jnp.exp(scores - top)
            weights.append((grown * (1.0 / jnp.sum(grown, axis=0, keepdims=True))).astype(BF))
        rows = []
        none = jnp.zeros((TOK, LANES), BF)
        for j in range(HEADS // 2):
            cut = slice(j * LANES, (j + 1) * LANES)
            both = jnp.concatenate(
                [
                    jnp.concatenate([weights[0][:, cut], none], axis=1),
                    jnp.concatenate([none, weights[1][:, cut]], axis=1),
                ],
                axis=0,
            )
            found = dot(v[2 * j * PAD : 2 * (j + 1) * PAD, lanes], both)
            one, two = found[:, :LANES], found[:, LANES:]
            rows.append(jnp.where(low, one[:PAD], pltpu.roll(two[:PAD], TOK, 1)))
            rows.append(jnp.where(low, pltpu.roll(one[PAD:], TOK, 1), two[PAD:]))
        joined.append(jnp.concatenate(rows, axis=0))
    joined = jnp.concatenate(joined, axis=1).astype(BF)
    return (x + dot(w_out, joined)).astype(BF)


def feed(states, gain, wh, wo):
    flat = states.astype(F32)
    normed = layer_norm(flat, gain)
    inner = jax.nn.gelu(dot(wh, normed)).astype(BF)
    return (flat + dot(wo, inner)).astype(BF)


def window_order():
    shape = (SIZE, SIZE)
    source, target = iota(shape, 0), iota(shape, 1)
    col = source % PART
    row = source // (SIZE // 2) * SHIFT + source % (SIZE // 2) // PART
    wanted = col // WIN * TOK + row * WIN + col % WIN
    return jnp.where(wanted == target, 1.0, 0.0).astype(BF)


def ranks(flags, windows):
    kept = flags.astype(F32)
    other = jnp.where(iota(flags.shape, 1) < windows, 1.0, 0.0) - kept
    tri = (LANES, LANES)
    before = jnp.where(iota(tri, 0) < iota(tri, 1), 1.0, 0.0).astype(BF)
    total = dot(kept.astype(BF), jnp.ones(tri, BF))
    ahead = dot(kept.astype(BF), before)
    return jnp.where(flags == 1, ahead, total + dot(other.astype(BF), before))


def column_order(rank, cols):
    shape = (cols, LANES)
    shifted = (iota(shape, 0) + cols - SHIFT) % cols
    spread = jnp.where(shifted // WIN == iota(shape, 1), jnp.broadcast_to(rank[0:1], shape), 0.0)
    first = dot(spread.astype(BF), jnp.ones((LANES, cols), BF))
    shape = (cols, cols)
    inside = ((iota(shape, 0) + cols - SHIFT) % WIN).astype(F32)
    wanted = first * WIN + inside
    return jnp.where(wanted == iota(shape, 1).astype(F32), 1.0, 0.0).astype(BF)


def swap_parts(one, two):
    front = iota(one.shape, 1) < PART
    even = jnp.where(front, one, pltpu.roll(two, PART, 1))
    return even, jnp.where(front, pltpu.roll(one, PART, 1), two)


def plane_row(planes, row, channels):
    halves = planes.shape[0]
    return jnp.concatenate(
        [planes[h, pl.ds(row, channels, stride=WIN), :] for h in range(halves)], axis=1
    )


def block_kernel(
    count, keep_in, dests_in, slots_in, pixels_in, table_in, gain_a_in, wqkv_in, wp_in,
    gain_m_in, wh_in, wo_in,
    restored, incoming,
    keep, dests, slots, keep_row, pixels, table, gain_a, wqkv, wp, gain_m, wh, wo, loads,
    planes, nxt_out, prv_out, nxt_buf, prv_buf, told, told_buf, w_in, w_out, w_hid, gains,
    strips, bias, order, columns, states, origin, done_rows, packed, outgoing,
    halo_send, halo_recv, tile_send, tile_recv,
):
    bands = lax.axis_size("band")
    me = lax.axis_index("band")
    right, left = lax.rem(me + 1, bands), lax.rem(me + bands - 1, bands)
    channels, rows, cols = pixels.shape
    windows = cols // WIN
    groups = windows // GROUP
    half = bands // 2
    fourth = half // 2
    far = jnp.where(me < half, half, 0)
    near = half - far
    halves = cols // LANES
    tiles = windows // TILE
    pairs = -(-tiles // bands)
    span = min(bands, tiles)
    mesh_id = pl.DeviceIdType.MESH
    moves = [
        pltpu.make_async_copy(source, target, loads.at[i])
        for i, (source, target) in enumerate(
            (
                (keep_in, keep_row), (pixels_in, pixels), (wqkv_in, wqkv), (wp_in, wp),
                (table_in, table), (gain_a_in, gain_a), (gain_m_in, gain_m), (wh_in, wh),
                (wo_in, wo), (keep_in, keep), (dests_in, dests), (slots_in, slots),
            )
        )
    ]
    for move in moves:
        move.start()

    barrier = pltpu.get_barrier_semaphore()

    def greet(i, _):
        peer = lax.rem(me + i, bands)
        pl.semaphore_signal(barrier, inc=1, device_id={"band": peer}, device_id_type=mesh_id)
        return 0

    lax.fori_loop(1, bands, greet, 0)

    live = count[0]
    moves[0].wait()
    told[...] = jnp.zeros(told.shape, jnp.int32)
    told[:, 0:windows] = jnp.broadcast_to(keep_row[...], (8, windows))
    mine = told[...]
    rank = ranks(mine, windows)
    final = jnp.max(jnp.where(iota(rank.shape, 1) == windows - 1, rank, 0.0), axis=1, keepdims=True)
    line = iota(told.shape, 0)
    extra = jnp.where(line == 1, jnp.broadcast_to(final, told.shape).astype(jnp.int32), live)
    told[...] = jnp.where(line == 0, mine, extra)

    def nxt_copy(c):
        return pltpu.make_async_remote_copy(
            src_ref=nxt_out.at[c],
            dst_ref=nxt_buf.at[c],
            send_sem=halo_send.at[c],
            recv_sem=halo_recv.at[c],
            device_id={"band": left},
            device_id_type=mesh_id,
        )

    odd = lax.rem(me, 2) == 1
    fold = groups // 2

    def prv_send(part, source, start, device, mark):
        first = part * fold
        return pltpu.make_async_remote_copy(
            src_ref=source.at[first : first + fold],
            dst_ref=prv_buf.at[start + first : start + first + fold],
            send_sem=halo_send.at[groups + 1 + 2 * mark + part],
            recv_sem=halo_recv.at[groups + 1 + 2 * mark + part],
            device_id={"band": device},
            device_id_type=mesh_id,
        )

    direct = [prv_send(part, prv_out, 0, right, 0) for part in range(2)]
    relay = [prv_send(part, prv_out, groups, lax.rem(me + 2, bands), 1) for part in range(2)]
    held = prv_buf.at[groups:]
    forward = [prv_send(part, held, 0, left, 0) for part in range(2)]
    told_copy = pltpu.make_async_remote_copy(
        src_ref=told,
        dst_ref=told_buf,
        send_sem=halo_send.at[groups],
        recv_sem=halo_recv.at[groups],
        device_id={"band": right},
        device_id_type=mesh_id,
    )
    pl.semaphore_wait(barrier, bands - 1)
    told_copy.start()
    moves[1].wait()
    for h in range(halves):
        part = pixels[:, :, h * LANES : (h + 1) * LANES].astype(F32)
        planes[h] = part.reshape(channels * rows, LANES)

    def arrange(first, matrix, target):
        for r in range(0, SHIFT, 2):
            one, two = (
                dot(plane_row(planes, first + r + k, channels).astype(BF), matrix) for k in range(2)
            )
            lanes = slice(r * PART, (r + 2) * PART)
            for h in range(halves):
                cols_h = slice(h * LANES, (h + 1) * LANES)
                even, uneven = swap_parts(one[:, cols_h], two[:, cols_h])
                target[2 * h, :, lanes] = even.astype(BF)
                target[2 * h + 1, :, lanes] = uneven.astype(BF)

    columns[0] = column_order(rank, cols)
    arrange(rows - SHIFT, columns[0], prv_out)

    @pl.when(odd)
    def _():
        for part in range(2):
            relay[part].start()

    order[...] = window_order()
    for move in moves[2:]:
        move.wait()
    w_in[...] = dot_t(spread_heads(3 * DEPTH, 3 * CHAN), wqkv[...]).astype(BF)
    w_out[...] = dot(spread_heads(DEPTH, CHAN), wp[...]).T.astype(BF)
    w_hid[...] = wh[...].astype(F32).T.astype(BF)
    gains[0] = jnp.broadcast_to(gain_a[...], (LANES, channels)).T
    gains[1] = jnp.broadcast_to(gain_m[...], (LANES, channels)).T
    bias_strips(table, strips)
    bias_fill(strips, bias, me == bands - 1, me == 0)

    told_copy.wait()
    news = told_buf[...]
    columns[1] = column_order(ranks(jnp.broadcast_to(news[0:1], told.shape), windows), cols)
    arrange(0, columns[1], nxt_out)
    for c in range(groups):
        nxt_copy(c).start()
    live_prev, final_prev = news[2, 0], news[1, 0]
    final_own = jnp.where(keep[0, windows - 1] == 1, live - 1, windows - 1)

    padded = channels + 4

    def windows_of(upper_part, lower_part):
        return dot(jnp.concatenate([upper_part, lower_part], axis=1), order[...])

    def attend_windows(x, start, kind, last):
        def edge(g):
            return bias[2 * kind + (start + g == last).astype(jnp.int32)]

        return attend(x, gains[0], w_in[...], w_out[...], edge)

    def step(c, _):
        nxt_copy(c).wait()

        @pl.when((c == groups - 1) & odd)
        def _():
            relay[0].wait()
            forward[0].start()

        @pl.when((c == groups - 1) & ~odd)
        def _():
            for part in range(2):
                direct[part].start()

        x = windows_of(prv_out[c], nxt_buf[c])
        origin[c] = x.astype(BF)
        own = attend_windows(x, c * GROUP, 0, final_own)
        states[c] = own
        wide = jnp.concatenate([own.astype(F32), jnp.zeros((4, SIZE), F32)], axis=0)
        for k in range(SIZE // LANES):
            packed[c * (SIZE // LANES) + k] = wide[:, k * LANES : (k + 1) * LANES].astype(BF)
        return 0

    slot_row = iota((padded, LANES), 0) >= channels
    member = iota((padded, LANES), 1) // TOK

    def pack(index, peer, j):
        t = jnp.int32(0)
        found = jnp.int32(0)
        for i in range(span):
            hit = dests[0, j * span + i] == peer
            t = jnp.where(hit, j * span + i, t)
            found = jnp.where(hit, 1, found)
        known = jnp.where(found > 0, live - t * TILE, 0)
        slot = jnp.where(known > 0, slots[0, t], CAP).astype(F32)
        value = packed[t]
        value = jnp.where(member < known, value, jnp.zeros_like(value))
        outgoing[index] = jnp.where(slot_row, jnp.full((padded, LANES), slot, F32).astype(BF), value)

    def peer_of(n):
        away = n >= half
        m = jnp.where(away, n - half + 1, n)
        cross = (m >= fourth).astype(jnp.int32)
        row = lax.rem(lax.div(lax.rem(me, half), 2) + m, fourth)
        side = lax.rem(lax.rem(me, 2) + cross, 2)
        return jnp.where(away, near, far) + 2 * row + side

    def tile_copy(n, j):
        return pltpu.make_async_remote_copy(
            src_ref=outgoing.at[n * pairs + j],
            dst_ref=incoming.at[me * pairs + j],
            send_sem=tile_send.at[n * pairs + j],
            recv_sem=tile_recv.at[n * pairs + j],
            device_id={"band": peer_of(n)},
            device_id_type=mesh_id,
        )

    stage = groups // pairs

    def round_of(j, _):
        lax.fori_loop(j * stage, (j + 1) * stage, step, 0)

        def dispatch(n, _):
            pack(n * pairs + j, peer_of(n), j)
            tile_copy(n, j).start()
            return 0

        lax.fori_loop(0, bands - 1, dispatch, 0)
        kept_here = (bands - 1) * pairs + j
        pack(kept_here, me, j)
        incoming[me * pairs + j] = outgoing[kept_here]
        return 0

    lax.fori_loop(0, pairs, round_of, 0)

    @pl.when(odd)
    def _():
        relay[1].wait()
        forward[1].start()

    for part in range(2):
        direct[part].wait_recv()

    @pl.when(~odd)
    def _():
        for part in range(2):
            direct[part].wait_send()

    @pl.when(odd)
    def _():
        for part in range(2):
            forward[part].wait_send()

    lane = iota((channels, WIDER * SIZE), 1)
    upper = lane % TOK < HALF

    def finish(i, _):
        number = WIDER * GROUP
        chunks = [i * WIDER + k for k in range(WIDER)]
        x = jnp.concatenate([windows_of(prv_buf[c], nxt_out[c]) for c in chunks], axis=1)
        prev = attend_windows(x, i * number, 1, final_prev)
        own = jnp.concatenate([states[c] for c in chunks], axis=1)
        done = feed(jnp.where(upper, own, prev), gains[1], w_hid[...], wo[...])
        before = jnp.concatenate([origin[c] for c in chunks], axis=1)
        before = jnp.where(upper, before, x.astype(BF))
        position = i * number + lane // TOK
        chosen = position < jnp.where(upper, live, live_prev)
        after = jnp.where(chosen, done, before)
        one, two = (dot_t(after[:, k * SIZE : (k + 1) * SIZE], order[...]) for k in range(WIDER))
        for k in range(SIZE // LANES):
            cut = slice(k * LANES, (k + 1) * LANES)
            even, uneven = swap_parts(one[:, cut], two[:, cut])
            r = (2 * k + SHIFT) % rows
            done_rows[i, r] = even.astype(BF)
            done_rows[i, r + 1] = uneven.astype(BF)
        return 0

    lax.fori_loop(0, groups // WIDER, finish, 0)
    for r in range(rows):
        row = jnp.concatenate([done_rows[h, r] for h in range(halves)], axis=1)
        row = dot_t(row, columns[0] if r >= rows - SHIFT else columns[1])
        for h in range(halves):
            planes[h, pl.ds(r, channels, stride=WIN), :] = row[:, h * LANES : (h + 1) * LANES]
    for h in range(halves):
        restored[:, :, h * LANES : (h + 1) * LANES] = (
            planes[h].reshape(channels, rows, LANES).astype(BF)
        )

    def collect(i, _):
        for j in range(pairs):
            tile_copy(i, j).wait()
        return 0

    lax.fori_loop(0, bands - 1, collect, 0)


def place_kernel(incoming, restored, restored_out, work, planes, sem):
    total, padded, _ = incoming.shape
    channels = work.shape[0]
    move = pltpu.make_async_copy(restored, restored_out, sem)
    move.start()
    head = incoming[:, padded - 8 :, :].astype(F32)
    head = jnp.max(jnp.where(iota(head.shape, 1) >= 4, head, 0.0), axis=1)
    slot = jnp.max(head, axis=1, keepdims=True).astype(jnp.int32)
    match = slot == iota((total, LANES), 1)
    source = jnp.where(match, iota((total, LANES), 0), -1).astype(F32)
    source = jnp.max(source, axis=0, keepdims=True).astype(jnp.int32)
    for k in range(CAP):
        known = source[0, k] >= 0
        block = incoming[jnp.maximum(source[0, k], 0)].astype(F32)[:channels]
        planes[pl.ds(k, channels, stride=CAP), :] = jnp.where(known, block, 0.0)
    work[...] = planes[...].reshape(channels, CAP, TILE * TOK).astype(BF)
    move.wait()


def shards(
    pixels, keep_mask, band_counts, plan_dest, plan_slot, bias_table, gain_attn, qkv_weight,
    proj_weight, gain_mlp, hidden_weight, output_weight,
):
    bands = lax.axis_size("band")
    rows, cols, channels = pixels.shape
    windows = cols // WIN
    halves = cols // LANES
    tiles = windows // TILE
    pairs = -(-tiles // bands)
    smem = pl.BlockSpec(memory_space=pltpu.SMEM)
    vmem = pl.BlockSpec(memory_space=pltpu.VMEM)
    tile_shape = (bands * pairs, channels + 4, LANES)
    groups = windows // GROUP
    nxt_shape = (groups, channels, SHIFT * PART)
    operands = (
        keep_mask, plan_dest, plan_slot, jnp.transpose(pixels, (2, 0, 1)),
        bias_table.T, gain_attn[None], qkv_weight, proj_weight, gain_mlp[None], hidden_weight,
        output_weight.T,
    )
    restored, incoming = pl.pallas_call(
        block_kernel,
        out_shape=(
            jax.ShapeDtypeStruct((channels, rows, cols), BF),
            jax.ShapeDtypeStruct(tile_shape, BF),
        ),
        in_specs=[smem] + [pl.BlockSpec(memory_space=pltpu.HBM)] * len(operands),
        out_specs=(vmem, vmem),
        scratch_shapes=[
            pltpu.SMEM(operands[0].shape, jnp.int32),
            pltpu.SMEM(operands[1].shape, jnp.int32),
            pltpu.SMEM(operands[2].shape, jnp.int32),
            pltpu.VMEM(operands[0].shape, jnp.int32),
            *(pltpu.VMEM(operand.shape, operand.dtype) for operand in operands[3:]),
            pltpu.SemaphoreType.DMA((len(operands) + 1,)),
            pltpu.VMEM((halves, channels * rows, LANES), F32),
            pltpu.VMEM(nxt_shape, BF),
            pltpu.VMEM(nxt_shape, BF),
            pltpu.VMEM(nxt_shape, BF),
            pltpu.VMEM((2 * groups, channels, SHIFT * PART), BF),
            pltpu.VMEM((8, LANES), jnp.int32),
            pltpu.VMEM((8, LANES), jnp.int32),
            pltpu.VMEM((3 * DEPTH, channels), BF),
            pltpu.VMEM((channels, DEPTH), BF),
            pltpu.VMEM((hidden_weight.shape[1], channels), BF),
            pltpu.VMEM((2, channels, LANES), F32),
            pltpu.VMEM((8 * WIN, LANES), F32),
            pltpu.VMEM((4, TOK, QUERIES), F32),
            pltpu.VMEM((SIZE, SIZE), BF),
            pltpu.VMEM((2, cols, cols), BF),
            pltpu.VMEM((groups, channels, SIZE), BF),
            pltpu.VMEM((groups, channels, SIZE), BF),
            pltpu.VMEM((halves, rows, channels, LANES), BF),
            pltpu.VMEM((tiles, channels + 4, LANES), BF),
            pltpu.VMEM(tile_shape, BF),
            pltpu.SemaphoreType.DMA((groups + 5,)),
            pltpu.SemaphoreType.DMA((groups + 5,)),
            pltpu.SemaphoreType.DMA((bands * pairs,)),
            pltpu.SemaphoreType.DMA((bands * pairs,)),
        ],
        compiler_params=pltpu.CompilerParams(
            vmem_limit_bytes=40 * 1024 * 1024, collective_id=0, has_side_effects=True
        ),
        cost_estimate=pl.CostEstimate(flops=10**10, bytes_accessed=10**7, transcendentals=10**6),
        name="block",
    )(band_counts, *(pltpu.with_memory_space_constraint(value, pltpu.HBM) for value in operands))
    restored, work = pl.pallas_call(
        place_kernel,
        out_shape=(
            jax.ShapeDtypeStruct((channels, rows, cols), BF),
            jax.ShapeDtypeStruct((channels, CAP, TILE * TOK), BF),
        ),
        in_specs=[vmem, vmem],
        out_specs=(pl.BlockSpec(memory_space=pl.ANY), vmem),
        scratch_shapes=[
            pltpu.VMEM((channels * CAP, TILE * TOK), F32),
            pltpu.SemaphoreType.DMA,
        ],
        compiler_params=pltpu.CompilerParams(vmem_limit_bytes=16 * 1024 * 1024),
        name="place",
    )(incoming, restored)
    return jnp.transpose(restored, (1, 2, 0)), jnp.transpose(work, (1, 2, 0))


def solution(mesh):
    split = P(("img", "band"))
    in_specs = (split,) * 5 + (P(),) * 7
    return jax.shard_map(shards, mesh=mesh, in_specs=in_specs, out_specs=(split, split), check_vma=False)
```

```python
import jax
import jax.numpy as jnp
from jax import lax
from jax.experimental import pallas as pl
from jax.experimental.pallas import tpu as pltpu
from jax.sharding import PartitionSpec as P

CHAN = 180
HEADS = 6
WIN = 8
TILE = 2
SHIFT = 4
CAP = 8
TOK = WIN * WIN
HALF = TOK // 2
HEAD_DIM = CHAN // HEADS
GROUP = 8
WIDER = 2
SIZE = GROUP * TOK
AHEAD = 4
PART = GROUP * WIN
PAD = 32
DEPTH = HEADS * PAD
QUERIES = HEADS * TOK
LANES = 128
SLOT_LANE = 120

EPSILON = 1e-05
BF = jnp.bfloat16
F32 = jnp.float32


def layer_norm(values, gain):
    center = values - jnp.sum(values, axis=0, keepdims=True) * (1.0 / CHAN)
    spread = jnp.sum(center * center, axis=0, keepdims=True) * (1.0 / CHAN)
    scaled = center * lax.rsqrt(spread + EPSILON)
    parts = [scaled[:, i : i + LANES] * gain for i in range(0, values.shape[1], LANES)]
    return jnp.concatenate(parts, axis=1).astype(BF)


def dot(a, b):
    return jnp.dot(a, b, preferred_element_type=F32)


def dot_t(a, b):
    return lax.dot_general(a, b, (((1,), (1,)), ((), ())), preferred_element_type=F32)


def iota(shape, axis):
    return lax.broadcasted_iota(jnp.int32, shape, axis)


def bias_strips(table, strips):
    heads, entries = table.shape
    values = jnp.concatenate([table[...], jnp.zeros((8 - heads, entries), F32)], axis=0)
    high = values.astype(BF).astype(F32)
    middle = (values - high).astype(BF).astype(F32)
    low = values - high - middle
    parts = jnp.concatenate([high, middle, low], axis=0).astype(BF)
    shape = (entries, WIN * LANES)
    entry, lane = iota(shape, 0), iota(shape, 1)
    step = (lane % LANES) // WIN
    wanted = step * (2 * WIN - 1) + lane % WIN - lane // LANES + WIN - 1
    pick = jnp.where((entry == wanted) & (step < 2 * WIN - 1), 1.0, 0.0).astype(BF)
    found = dot(parts, pick)
    found = found[0:8] + found[8:16] + found[16:24]
    for c in range(WIN):
        strips[pl.ds(c, 8, stride=WIN), :] = found[:, c * LANES : (c + 1) * LANES]


def bias_fill(strips, bias, own_last, prev_last):
    first_half = iota((WIN, LANES), 1) < TOK
    for r in range(WIN):
        by = 2 * LANES - (WIN - 1 - r) * WIN
        tiles = []
        for h in range(0, HEADS, 2):
            even = strips[h * WIN : (h + 1) * WIN, :]
            odd = strips[(h + 1) * WIN : (h + 2) * WIN, :]
            tiles.append(
                jnp.where(
                    first_half,
                    pltpu.roll(even, by % LANES, 1),
                    pltpu.roll(odd, (by + TOK) % LANES, 1),
                )
            )
        base = jnp.concatenate(tiles, axis=1)
        shape = (WIN, QUERIES)
        key, query = iota(shape, 0), iota(shape, 1) % TOK
        rows_differ = (query // WIN >= SHIFT) != (r >= SHIFT)
        cols_differ = (key >= SHIFT) != (query % WIN >= SHIFT)
        rows = slice(r * WIN, (r + 1) * WIN)
        for k, last in enumerate((own_last, prev_last)):
            row_pen = jnp.where(rows_differ, jnp.where(last, -100.0, 0.0).astype(F32), 0.0)
            bias[2 * k, rows] = base + row_pen
            bias[2 * k + 1, rows] = base + jnp.where(cols_differ, -100.0, row_pen)


def spread_heads(rows, cols):
    row, col = iota((rows, cols), 0), iota((rows, cols), 1)
    inside = row % DEPTH
    wanted = row // DEPTH * CHAN + inside // PAD * HEAD_DIM + inside % PAD
    return jnp.where((inside % PAD < HEAD_DIM) & (wanted == col), 1.0, 0.0).astype(BF)


def attend(x, gain, w_in, w_out, bias_of):
    normed = layer_norm(x, gain)
    mixed = dot(w_in, normed)
    q = mixed[0:DEPTH] * HEAD_DIM ** (-0.5)
    k = mixed[DEPTH : 2 * DEPTH].T.astype(BF)
    v = mixed[2 * DEPTH :].astype(BF)
    low = iota((PAD, LANES), 1) < TOK
    blank = jnp.zeros((PAD, LANES), F32)
    none = jnp.zeros((TOK, LANES), BF)

    def weigh(pair):
        lanes = slice(pair * LANES, (pair + 1) * LANES)
        q_pair = q[:, lanes]
        q_turn = pltpu.roll(q_pair, TOK, 1)
        weights = []
        for side in range(2):
            g = 2 * pair + side
            blocks = []
            for h in range(HEADS):
                part = slice(h * PAD, (h + 1) * PAD)
                value = q_pair[part] if h % 2 == side else q_turn[part]
                value = jnp.where(low if h % 2 == 0 else ~low, value, 0.0)
                row = [blank] * (HEADS // 2)
                row[h // 2] = value
                blocks.append(jnp.concatenate(row, axis=1))
            spread_q = jnp.concatenate(blocks, axis=0).astype(BF)
            scores = dot(k[g * TOK : (g + 1) * TOK], spread_q) + bias_of(g)
            top = jnp.max(scores, axis=0, keepdims=True)
            grown = jnp.exp(scores - top)
            weights.append((grown * (1.0 / jnp.sum(grown, axis=0, keepdims=True))).astype(BF))
        return weights

    def mix(pair, weights):
        lanes = slice(pair * LANES, (pair + 1) * LANES)
        rows = []
        for j in range(HEADS // 2):
            cut = slice(j * LANES, (j + 1) * LANES)
            both = jnp.concatenate(
                [
                    jnp.concatenate([weights[0][:, cut], none], axis=1),
                    jnp.concatenate([none, weights[1][:, cut]], axis=1),
                ],
                axis=0,
            )
            found = dot(v[2 * j * PAD : 2 * (j + 1) * PAD, lanes], both)
            one, two = found[:, :LANES], found[:, LANES:]
            rows.append(jnp.where(low, one[:PAD], pltpu.roll(two[:PAD], TOK, 1)))
            rows.append(jnp.where(low, pltpu.roll(one[PAD:], TOK, 1), two[PAD:]))
        return jnp.concatenate(rows, axis=0).astype(BF)

    count = x.shape[1] // LANES
    ready, joined = {}, []
    for pair in range(count + AHEAD):
        if pair < count:
            ready[pair] = weigh(pair)
        if pair >= AHEAD:
            joined.append(mix(pair - AHEAD, ready.pop(pair - AHEAD)))
    joined = jnp.concatenate(joined, axis=1)
    return (x + dot(w_out, joined)).astype(BF)


def feed(states, gain, wh, wo):
    flat = states.astype(F32)
    normed = layer_norm(flat, gain)
    inner = jax.nn.gelu(dot(wh, normed)).astype(BF)
    return (flat + dot(wo, inner)).astype(BF)


def window_order():
    shape = (SIZE, SIZE)
    source, target = iota(shape, 0), iota(shape, 1)
    col = source % PART
    row = source // (SIZE // 2) * SHIFT + source % (SIZE // 2) // PART
    wanted = col // WIN * TOK + row * WIN + col % WIN
    return jnp.where(wanted == target, 1.0, 0.0).astype(BF)


def ranks(flags, windows):
    kept = flags.astype(F32)
    other = jnp.where(iota(flags.shape, 1) < windows, 1.0, 0.0) - kept
    tri = (LANES, LANES)
    before = jnp.where(iota(tri, 0) < iota(tri, 1), 1.0, 0.0).astype(BF)
    total = dot(kept.astype(BF), jnp.ones(tri, BF))
    ahead = dot(kept.astype(BF), before)
    return jnp.where(flags == 1, ahead, total + dot(other.astype(BF), before))


def column_order(rank, cols):
    shape = (cols, LANES)
    shifted = (iota(shape, 0) + cols - SHIFT) % cols
    spread = jnp.where(shifted // WIN == iota(shape, 1), jnp.broadcast_to(rank[0:1], shape), 0.0)
    first = dot(spread.astype(BF), jnp.ones((LANES, cols), BF))
    shape = (cols, cols)
    inside = ((iota(shape, 0) + cols - SHIFT) % WIN).astype(F32)
    wanted = first * WIN + inside
    return jnp.where(wanted == iota(shape, 1).astype(F32), 1.0, 0.0).astype(BF)


def swap_parts(one, two):
    front = iota(one.shape, 1) < PART
    even = jnp.where(front, one, pltpu.roll(two, PART, 1))
    return even, jnp.where(front, pltpu.roll(one, PART, 1), two)


def plane_row(planes, row, channels):
    halves = planes.shape[0]
    return jnp.concatenate(
        [planes[h, pl.ds(row, channels, stride=WIN), :] for h in range(halves)], axis=1
    )


def block_kernel(
    count, keep_in, dests_in, slots_in, pixels_in, table_in, gain_a_in, wqkv_in, wp_in,
    gain_m_in, wh_in, wo_in,
    restored, incoming,
    keep, dests, slots, keep_row, pixels, table, gain_a, wqkv, wp, gain_m, wh, wo, loads,
    planes, nxt_out, prv_out, nxt_buf, prv_buf, told, told_buf, w_in, w_out, w_hid, gains,
    strips, bias, order, columns, states, origin, done_rows, packed, outgoing,
    halo_send, halo_recv, tile_send, tile_recv,
):
    bands = lax.axis_size("band")
    me = lax.axis_index("band")
    right, left = lax.rem(me + 1, bands), lax.rem(me + bands - 1, bands)
    channels, rows, cols = pixels.shape
    windows = cols // WIN
    groups = windows // GROUP
    half = bands // 2
    fourth = half // 2
    far = jnp.where(me < half, half, 0)
    near = half - far
    halves = cols // LANES
    tiles = windows // TILE
    pairs = -(-tiles // bands)
    span = min(bands, tiles)
    mesh_id = pl.DeviceIdType.MESH
    moves = [
        pltpu.make_async_copy(source, target, loads.at[i])
        for i, (source, target) in enumerate(
            (
                (keep_in, keep_row), (pixels_in, pixels), (keep_in, keep), (wqkv_in, wqkv), (wp_in, wp),
                (table_in, table), (gain_a_in, gain_a), (gain_m_in, gain_m), (wh_in, wh),
                (wo_in, wo), (dests_in, dests), (slots_in, slots),
            )
        )
    ]
    for move in moves:
        move.start()

    barrier = pltpu.get_barrier_semaphore()

    def greet(i, _):
        peer = lax.rem(me + i, bands)
        pl.semaphore_signal(barrier, inc=1, device_id={"band": peer}, device_id_type=mesh_id)
        return 0

    lax.fori_loop(1, bands, greet, 0)

    live = count[0]
    moves[0].wait()
    told[...] = jnp.zeros(told.shape, jnp.int32)
    told[:, 0:windows] = jnp.broadcast_to(keep_row[...], (8, windows))
    mine = told[...]
    rank = ranks(mine, windows)
    final = jnp.max(jnp.where(iota(rank.shape, 1) == windows - 1, rank, 0.0), axis=1, keepdims=True)
    line = iota(told.shape, 0)
    extra = jnp.where(line == 1, jnp.broadcast_to(final, told.shape).astype(jnp.int32), live)
    told[...] = jnp.where(line == 0, rank.astype(jnp.int32), extra)

    def nxt_copy(c):
        return pltpu.make_async_remote_copy(
            src_ref=nxt_out.at[c],
            dst_ref=nxt_buf.at[c],
            send_sem=halo_send.at[c],
            recv_sem=halo_recv.at[c],
            device_id={"band": left},
            device_id_type=mesh_id,
        )

    odd = lax.rem(me, 2) == 1
    fold = WIDER

    def prv_send(part, source, from_chunk, to_chunk, device, mark):
        first = part * fold
        return pltpu.make_async_remote_copy(
            src_ref=source.at[pl.ds(from_chunk + first, fold)],
            dst_ref=prv_buf.at[pl.ds(to_chunk + first, fold)],
            send_sem=halo_send.at[groups + 1 + 2 * mark + part],
            recv_sem=halo_recv.at[groups + 1 + 2 * mark + part],
            device_id={"band": device},
            device_id_type=mesh_id,
        )

    def direct(part):
        return prv_send(part, prv_out, 0, 0, right, 0)

    def relay(part):
        return prv_send(part, prv_out, 0, groups, lax.rem(me + 2, bands), 1)

    def forward(part):
        return prv_send(part, prv_buf, groups, 0, left, 0)

    told_copy = pltpu.make_async_remote_copy(
        src_ref=told,
        dst_ref=told_buf,
        send_sem=halo_send.at[groups],
        recv_sem=halo_recv.at[groups],
        device_id={"band": right},
        device_id_type=mesh_id,
    )
    pl.semaphore_wait(barrier, bands - 1)
    told_copy.start()
    moves[1].wait()
    moves[2].wait()
    for h in range(halves):
        part = pixels[:, :, h * LANES : (h + 1) * LANES].astype(F32)
        planes[h] = part.reshape(channels * rows, LANES)

    def arrange(first, matrix, target, done):
        moved = [
            dot(plane_row(planes, first + r, channels).astype(BF), matrix) for r in range(SHIFT)
        ]
        for h in range(halves):
            cols_h = slice(h * LANES, (h + 1) * LANES)
            for r in range(0, SHIFT, 2):
                even, uneven = swap_parts(moved[r][:, cols_h], moved[r + 1][:, cols_h])
                lanes = slice(r * PART, (r + 2) * PART)
                target[2 * h, :, lanes] = even.astype(BF)
                target[2 * h + 1, :, lanes] = uneven.astype(BF)
            done(h)

    columns[0] = column_order(rank, cols)

    def start_relay(h):
        @pl.when(odd)
        def _():
            relay(h).start()

    def start_nxt(h):
        nxt_copy(2 * h).start()
        nxt_copy(2 * h + 1).start()

    arrange(rows - SHIFT, columns[0], prv_out, start_relay)
    told_copy.wait()
    news = told_buf[...]
    columns[1] = column_order(news[0:1].astype(F32), cols)
    arrange(0, columns[1], nxt_out, start_nxt)
    live_prev, final_prev = news[2, 0], news[1, 0]
    final_own = jnp.where(keep[0, windows - 1] == 1, live - 1, windows - 1)

    order[...] = window_order()
    for move in moves[3:]:
        move.wait()
    w_in[...] = dot_t(spread_heads(3 * DEPTH, 3 * CHAN), wqkv[...]).astype(BF)
    w_out[...] = dot(spread_heads(DEPTH, CHAN), wp[...]).T.astype(BF)
    w_hid[...] = wh[...].astype(F32).T.astype(BF)
    gains[0] = jnp.broadcast_to(gain_a[...], (LANES, channels)).T
    gains[1] = jnp.broadcast_to(gain_m[...], (LANES, channels)).T
    bias_strips(table, strips)
    bias_fill(strips, bias, me == bands - 1, me == 0)

    padded = channels + 4

    def windows_of(upper_part, lower_part):
        return dot(jnp.concatenate([upper_part, lower_part], axis=1), order[...])

    def attend_windows(x, start, kind, last):
        def edge(g):
            return bias[2 * kind + (start + g == last).astype(jnp.int32)]

        return attend(x, gains[0], w_in[...], w_out[...], edge)

    def step(c, _):
        nxt_copy(c).wait()

        @pl.when((c >= groups - 2) & odd)
        def _():
            relay(c - groups + 2).wait()
            forward(c - groups + 2).start()

        @pl.when((c == groups - 1) & ~odd)
        def _():
            direct(0).start()
            direct(1).start()

        x = windows_of(prv_out[c], nxt_buf[c])
        origin[c] = x.astype(BF)
        own = attend_windows(x, c * GROUP, 0, final_own)
        states[c] = own
        wide = jnp.concatenate([own.astype(F32), jnp.zeros((4, SIZE), F32)], axis=0)
        for k in range(SIZE // LANES):
            packed[c * (SIZE // LANES) + k] = wide[:, k * LANES : (k + 1) * LANES].astype(BF)
        return 0

    slot_row = iota((padded, LANES), 0) >= channels
    member = iota((padded, LANES), 1) // TOK

    def pack(index, peer, j):
        t = jnp.int32(0)
        found = jnp.int32(0)
        for i in range(span):
            hit = dests[0, j * span + i] == peer
            t = jnp.where(hit, j * span + i, t)
            found = jnp.where(hit, 1, found)
        known = jnp.where(found > 0, live - t * TILE, 0)
        slot = jnp.where(known > 0, slots[0, t], CAP).astype(F32)
        value = packed[t]
        value = jnp.where(member < known, value, jnp.zeros_like(value))
        outgoing[index] = jnp.where(slot_row, jnp.full((padded, LANES), slot, F32).astype(BF), value)

    def peer_of(n):
        away = n >= half
        m = jnp.where(away, n - half + 1, n)
        cross = (m >= fourth).astype(jnp.int32)
        row = lax.rem(lax.div(lax.rem(me, half), 2) + m, fourth)
        side = lax.rem(lax.rem(me, 2) + cross, 2)
        return jnp.where(away, near, far) + 2 * row + side

    def tile_copy(n, j):
        return pltpu.make_async_remote_copy(
            src_ref=outgoing.at[n * pairs + j],
            dst_ref=incoming.at[me * pairs + j],
            send_sem=tile_send.at[n * pairs + j],
            recv_sem=tile_recv.at[n * pairs + j],
            device_id={"band": peer_of(n)},
            device_id_type=mesh_id,
        )

    stage = groups // pairs

    def round_of(j, _):
        lax.fori_loop(j * stage, (j + 1) * stage, step, 0)

        def dispatch(n, _):
            pack(n * pairs + j, peer_of(n), j)
            tile_copy(n, j).start()
            return 0

        lax.fori_loop(0, bands - 1, dispatch, 0)
        kept_here = (bands - 1) * pairs + j
        pack(kept_here, me, j)
        incoming[me * pairs + j] = outgoing[kept_here]
        return 0

    lax.fori_loop(0, pairs, round_of, 0)

    lane = iota((channels, WIDER * SIZE), 1)
    upper = lane % TOK < HALF

    def finish(i, _):
        direct(i).wait_recv()

        @pl.when(~odd)
        def _():
            direct(i).wait_send()

        @pl.when(odd)
        def _():
            forward(i).wait_send()

        number = WIDER * GROUP
        chunks = [i * WIDER + k for k in range(WIDER)]
        x = jnp.concatenate([windows_of(prv_buf[c], nxt_out[c]) for c in chunks], axis=1)
        prev = attend_windows(x, i * number, 1, final_prev)
        own = jnp.concatenate([states[c] for c in chunks], axis=1)
        done = feed(jnp.where(upper, own, prev), gains[1], w_hid[...], wo[...])
        before = jnp.concatenate([origin[c] for c in chunks], axis=1)
        before = jnp.where(upper, before, x.astype(BF))
        position = i * number + lane // TOK
        chosen = position < jnp.where(upper, live, live_prev)
        after = jnp.where(chosen, done, before)
        one, two = (dot_t(after[:, k * SIZE : (k + 1) * SIZE], order[...]) for k in range(WIDER))
        for k in range(SIZE // LANES):
            cut = slice(k * LANES, (k + 1) * LANES)
            even, uneven = swap_parts(one[:, cut], two[:, cut])
            r = (2 * k + SHIFT) % rows
            done_rows[i, r] = even.astype(BF)
            done_rows[i, r + 1] = uneven.astype(BF)
        return 0

    lax.fori_loop(0, groups // WIDER, finish, 0)
    for r in range(rows):
        row = jnp.concatenate([done_rows[h, r] for h in range(halves)], axis=1)
        row = dot_t(row, columns[0] if r >= rows - SHIFT else columns[1])
        for h in range(halves):
            planes[h, pl.ds(r, channels, stride=WIN), :] = row[:, h * LANES : (h + 1) * LANES]
    for h in range(halves):
        restored[:, :, h * LANES : (h + 1) * LANES] = (
            planes[h].reshape(channels, rows, LANES).astype(BF)
        )

    def collect(i, _):
        for j in range(pairs):
            tile_copy(i, j).wait()
        return 0

    lax.fori_loop(0, bands - 1, collect, 0)


def place_kernel(incoming, restored, restored_out, work, planes, sem):
    total, padded, _ = incoming.shape
    channels = work.shape[0]
    move = pltpu.make_async_copy(restored, restored_out, sem)
    move.start()
    head = incoming[:, padded - 8 :, :].astype(F32)
    head = jnp.max(jnp.where(iota(head.shape, 1) >= 4, head, 0.0), axis=1)
    slot = jnp.max(head, axis=1, keepdims=True).astype(jnp.int32)
    match = slot == iota((total, LANES), 1)
    source = jnp.where(match, iota((total, LANES), 0), -1).astype(F32)
    source = jnp.max(source, axis=0, keepdims=True).astype(jnp.int32)
    for k in range(CAP):
        known = source[0, k] >= 0
        block = incoming[jnp.maximum(source[0, k], 0)].astype(F32)[:channels]
        planes[pl.ds(k, channels, stride=CAP), :] = jnp.where(known, block, 0.0)
    work[...] = planes[...].reshape(channels, CAP, TILE * TOK).astype(BF)
    move.wait()


def shards(
    pixels, keep_mask, band_counts, plan_dest, plan_slot, bias_table, gain_attn, qkv_weight,
    proj_weight, gain_mlp, hidden_weight, output_weight,
):
    bands = lax.axis_size("band")
    rows, cols, channels = pixels.shape
    windows = cols // WIN
    halves = cols // LANES
    tiles = windows // TILE
    pairs = -(-tiles // bands)
    smem = pl.BlockSpec(memory_space=pltpu.SMEM)
    vmem = pl.BlockSpec(memory_space=pltpu.VMEM)
    tile_shape = (bands * pairs, channels + 4, LANES)
    groups = windows // GROUP
    nxt_shape = (groups, channels, SHIFT * PART)
    operands = (
        keep_mask, plan_dest, plan_slot, jnp.transpose(pixels, (2, 0, 1)),
        bias_table.T, gain_attn[None], qkv_weight, proj_weight, gain_mlp[None], hidden_weight,
        output_weight.T,
    )
    restored, incoming = pl.pallas_call(
        block_kernel,
        out_shape=(
            jax.ShapeDtypeStruct((channels, rows, cols), BF),
            jax.ShapeDtypeStruct(tile_shape, BF),
        ),
        in_specs=[smem] + [pl.BlockSpec(memory_space=pltpu.HBM)] * len(operands),
        out_specs=(vmem, vmem),
        scratch_shapes=[
            pltpu.SMEM(operands[0].shape, jnp.int32),
            pltpu.SMEM(operands[1].shape, jnp.int32),
            pltpu.SMEM(operands[2].shape, jnp.int32),
            pltpu.VMEM(operands[0].shape, jnp.int32),
            *(pltpu.VMEM(operand.shape, operand.dtype) for operand in operands[3:]),
            pltpu.SemaphoreType.DMA((len(operands) + 1,)),
            pltpu.VMEM((halves, channels * rows, LANES), F32),
            pltpu.VMEM(nxt_shape, BF),
            pltpu.VMEM(nxt_shape, BF),
            pltpu.VMEM(nxt_shape, BF),
            pltpu.VMEM((2 * groups, channels, SHIFT * PART), BF),
            pltpu.VMEM((8, LANES), jnp.int32),
            pltpu.VMEM((8, LANES), jnp.int32),
            pltpu.VMEM((3 * DEPTH, channels), BF),
            pltpu.VMEM((channels, DEPTH), BF),
            pltpu.VMEM((hidden_weight.shape[1], channels), BF),
            pltpu.VMEM((2, channels, LANES), F32),
            pltpu.VMEM((8 * WIN, LANES), F32),
            pltpu.VMEM((4, TOK, QUERIES), F32),
            pltpu.VMEM((SIZE, SIZE), BF),
            pltpu.VMEM((2, cols, cols), BF),
            pltpu.VMEM((groups, channels, SIZE), BF),
            pltpu.VMEM((groups, channels, SIZE), BF),
            pltpu.VMEM((halves, rows, channels, LANES), BF),
            pltpu.VMEM((tiles, channels + 4, LANES), BF),
            pltpu.VMEM(tile_shape, BF),
            pltpu.SemaphoreType.DMA((groups + 5,)),
            pltpu.SemaphoreType.DMA((groups + 5,)),
            pltpu.SemaphoreType.DMA((bands * pairs,)),
            pltpu.SemaphoreType.DMA((bands * pairs,)),
        ],
        compiler_params=pltpu.CompilerParams(
            vmem_limit_bytes=40 * 1024 * 1024, collective_id=0, has_side_effects=True
        ),
        cost_estimate=pl.CostEstimate(flops=10**10, bytes_accessed=10**7, transcendentals=10**6),
        name="block",
    )(band_counts, *(pltpu.with_memory_space_constraint(value, pltpu.HBM) for value in operands))
    restored, work = pl.pallas_call(
        place_kernel,
        out_shape=(
            jax.ShapeDtypeStruct((channels, rows, cols), BF),
            jax.ShapeDtypeStruct((channels, CAP, TILE * TOK), BF),
        ),
        in_specs=[vmem, vmem],
        out_specs=(pl.BlockSpec(memory_space=pl.ANY), vmem),
        scratch_shapes=[
            pltpu.VMEM((channels * CAP, TILE * TOK), F32),
            pltpu.SemaphoreType.DMA,
        ],
        compiler_params=pltpu.CompilerParams(vmem_limit_bytes=16 * 1024 * 1024),
        name="place",
    )(incoming, restored)
    return jnp.transpose(restored, (1, 2, 0)), jnp.transpose(work, (1, 2, 0))


def solution(mesh):
    split = P(("img", "band"))
    in_specs = (split,) * 5 + (P(),) * 7
    return jax.shard_map(shards, mesh=mesh, in_specs=in_specs, out_specs=(split, split), check_vma=False)
```

```python
import jax
import jax.numpy as jnp
from jax import lax
from jax.experimental import pallas as pl
from jax.experimental.pallas import tpu as pltpu
from jax.sharding import PartitionSpec as P

CHAN = 180
HEADS = 6
WIN = 8
TILE = 2
SHIFT = 4
CAP = 8
TOK = WIN * WIN
HALF = TOK // 2
HEAD_DIM = CHAN // HEADS
GROUP = 8
WIDER = 2
SIZE = GROUP * TOK
AHEAD = 4
CUT = 60
PART = GROUP * WIN
PAD = 32
DEPTH = HEADS * PAD
QUERIES = HEADS * TOK
LANES = 128
SLOT_LANE = 120

EPSILON = 1e-05
BF = jnp.bfloat16
F32 = jnp.float32


def layer_norm(values, gain):
    center = values - jnp.sum(values, axis=0, keepdims=True) * (1.0 / CHAN)
    spread = jnp.sum(center * center, axis=0, keepdims=True) * (1.0 / CHAN)
    scaled = center * lax.rsqrt(spread + EPSILON)
    parts = [scaled[:, i : i + LANES] * gain for i in range(0, values.shape[1], LANES)]
    return jnp.concatenate(parts, axis=1).astype(BF)


def dot(a, b):
    return jnp.dot(a, b, preferred_element_type=F32)


def dot_t(a, b):
    return lax.dot_general(a, b, (((1,), (1,)), ((), ())), preferred_element_type=F32)


def iota(shape, axis):
    return lax.broadcasted_iota(jnp.int32, shape, axis)


def bias_strips(table, strips):
    heads, entries = table.shape
    values = jnp.concatenate([table[...], jnp.zeros((8 - heads, entries), F32)], axis=0)
    high = values.astype(BF).astype(F32)
    middle = (values - high).astype(BF).astype(F32)
    low = values - high - middle
    parts = jnp.concatenate([high, middle, low], axis=0).astype(BF)
    shape = (entries, WIN * LANES)
    entry, lane = iota(shape, 0), iota(shape, 1)
    step = (lane % LANES) // WIN
    wanted = step * (2 * WIN - 1) + lane % WIN - lane // LANES + WIN - 1
    pick = jnp.where((entry == wanted) & (step < 2 * WIN - 1), 1.0, 0.0).astype(BF)
    found = dot(parts, pick)
    found = found[0:8] + found[8:16] + found[16:24]
    for c in range(WIN):
        strips[pl.ds(c, 8, stride=WIN), :] = found[:, c * LANES : (c + 1) * LANES]


def bias_fill(strips, bias, own_last, prev_last):
    first_half = iota((WIN, LANES), 1) < TOK
    for r in range(WIN):
        by = 2 * LANES - (WIN - 1 - r) * WIN
        tiles = []
        for h in range(0, HEADS, 2):
            even = strips[h * WIN : (h + 1) * WIN, :]
            odd = strips[(h + 1) * WIN : (h + 2) * WIN, :]
            tiles.append(
                jnp.where(
                    first_half,
                    pltpu.roll(even, by % LANES, 1),
                    pltpu.roll(odd, (by + TOK) % LANES, 1),
                )
            )
        base = jnp.concatenate(tiles, axis=1)
        shape = (WIN, QUERIES)
        key, query = iota(shape, 0), iota(shape, 1) % TOK
        rows_differ = (query // WIN >= SHIFT) != (r >= SHIFT)
        cols_differ = (key >= SHIFT) != (query % WIN >= SHIFT)
        rows = slice(r * WIN, (r + 1) * WIN)
        for k, last in enumerate((own_last, prev_last)):
            row_pen = jnp.where(rows_differ, jnp.where(last, -100.0, 0.0).astype(F32), 0.0)
            bias[2 * k, rows] = base + row_pen
            bias[2 * k + 1, rows] = base + jnp.where(cols_differ, -100.0, row_pen)


def spread_heads(rows, cols):
    row, col = iota((rows, cols), 0), iota((rows, cols), 1)
    inside = row % DEPTH
    wanted = row // DEPTH * CHAN + inside // PAD * HEAD_DIM + inside % PAD
    return jnp.where((inside % PAD < HEAD_DIM) & (wanted == col), 1.0, 0.0).astype(BF)


def attend(x, gain, w_in, w_out, bias_of):
    normed = layer_norm(x, gain)
    mixed = dot(w_in, normed)
    q = mixed[0:DEPTH] * HEAD_DIM ** (-0.5)
    k = mixed[DEPTH : 2 * DEPTH].T.astype(BF)
    v = mixed[2 * DEPTH :].astype(BF)
    low = iota((PAD, LANES), 1) < TOK
    blank = jnp.zeros((PAD, LANES), F32)
    none = jnp.zeros((TOK, LANES), BF)

    def weigh(pair):
        lanes = slice(pair * LANES, (pair + 1) * LANES)
        q_pair = q[:, lanes]
        q_turn = pltpu.roll(q_pair, TOK, 1)
        weights = []
        for side in range(2):
            g = 2 * pair + side
            blocks = []
            for h in range(HEADS):
                part = slice(h * PAD, (h + 1) * PAD)
                value = q_pair[part] if h % 2 == side else q_turn[part]
                value = jnp.where(low if h % 2 == 0 else ~low, value, 0.0)
                row = [blank] * (HEADS // 2)
                row[h // 2] = value
                blocks.append(jnp.concatenate(row, axis=1))
            spread_q = jnp.concatenate(blocks, axis=0).astype(BF)
            scores = dot(k[g * TOK : (g + 1) * TOK], spread_q) + bias_of(g)
            top = jnp.max(scores, axis=0, keepdims=True)
            grown = jnp.exp(scores - top)
            weights.append((grown * (1.0 / jnp.sum(grown, axis=0, keepdims=True))).astype(BF))
        return weights

    def mix(pair, weights):
        lanes = slice(pair * LANES, (pair + 1) * LANES)
        rows = []
        for j in range(HEADS // 2):
            cut = slice(j * LANES, (j + 1) * LANES)
            both = jnp.concatenate(
                [
                    jnp.concatenate([weights[0][:, cut], none], axis=1),
                    jnp.concatenate([none, weights[1][:, cut]], axis=1),
                ],
                axis=0,
            )
            found = dot(v[2 * j * PAD : 2 * (j + 1) * PAD, lanes], both)
            one, two = found[:, :LANES], found[:, LANES:]
            rows.append(jnp.where(low, one[:PAD], pltpu.roll(two[:PAD], TOK, 1)))
            rows.append(jnp.where(low, pltpu.roll(one[PAD:], TOK, 1), two[PAD:]))
        return jnp.concatenate(rows, axis=0).astype(BF)

    count = x.shape[1] // LANES
    ready, joined = {}, []
    for pair in range(count + AHEAD):
        if pair < count:
            ready[pair] = weigh(pair)
        if pair >= AHEAD:
            joined.append(mix(pair - AHEAD, ready.pop(pair - AHEAD)))
    joined = jnp.concatenate(joined, axis=1)
    return (x + dot(w_out, joined)).astype(BF)


def feed(states, gain, wh, wo):
    flat = states.astype(F32)
    normed = layer_norm(flat, gain)
    inner = jax.nn.gelu(dot(wh, normed)).astype(BF)
    return (flat + dot(wo, inner)).astype(BF)


def window_order():
    shape = (SIZE, SIZE)
    source, target = iota(shape, 0), iota(shape, 1)
    col = source % PART
    row = source // (SIZE // 2) * SHIFT + source % (SIZE // 2) // PART
    wanted = col // WIN * TOK + row * WIN + col % WIN
    return jnp.where(wanted == target, 1.0, 0.0).astype(BF)


def ranks(flags, windows):
    kept = flags.astype(F32)
    other = jnp.where(iota(flags.shape, 1) < windows, 1.0, 0.0) - kept
    tri = (LANES, LANES)
    before = jnp.where(iota(tri, 0) < iota(tri, 1), 1.0, 0.0).astype(BF)
    total = dot(kept.astype(BF), jnp.ones(tri, BF))
    ahead = dot(kept.astype(BF), before)
    return jnp.where(flags == 1, ahead, total + dot(other.astype(BF), before))


def column_order(rank, cols):
    shape = (cols, LANES)
    shifted = (iota(shape, 0) + cols - SHIFT) % cols
    spread = jnp.where(shifted // WIN == iota(shape, 1), jnp.broadcast_to(rank[0:1], shape), 0.0)
    first = dot(spread.astype(BF), jnp.ones((LANES, cols), BF))
    shape = (cols, cols)
    inside = ((iota(shape, 0) + cols - SHIFT) % WIN).astype(F32)
    wanted = first * WIN + inside
    return jnp.where(wanted == iota(shape, 1).astype(F32), 1.0, 0.0).astype(BF)


def swap_parts(one, two):
    front = iota(one.shape, 1) < PART
    even = jnp.where(front, one, pltpu.roll(two, PART, 1))
    return even, jnp.where(front, pltpu.roll(one, PART, 1), two)


def plane_row(planes, row, channels):
    halves = planes.shape[0]
    return jnp.concatenate(
        [planes[h, pl.ds(row, channels, stride=WIN), :] for h in range(halves)], axis=1
    )


def block_kernel(
    count, keep_in, dests_in, slots_in, pixels_in, table_in, gain_a_in, wqkv_in, wp_in,
    gain_m_in, wh_in, wo_in,
    restored, incoming,
    keep, dests, slots, keep_row, pixels, table, gain_a, wqkv, wp, gain_m, wh, wo, loads,
    planes, nxt_out, prv_out, nxt_buf, prv_buf, told, told_buf, w_in, w_out, w_hid, gains,
    strips, bias, order, columns, states, origin, done_rows, packed, outgoing,
    halo_send, halo_recv, tile_send, tile_recv,
):
    bands = lax.axis_size("band")
    me = lax.axis_index("band")
    right, left = lax.rem(me + 1, bands), lax.rem(me + bands - 1, bands)
    channels, rows, cols = pixels.shape
    windows = cols // WIN
    groups = windows // GROUP
    half = bands // 2
    fourth = half // 2
    far = jnp.where(me < half, half, 0)
    near = half - far
    halves = cols // LANES
    tiles = windows // TILE
    pairs = -(-tiles // bands)
    span = min(bands, tiles)
    mesh_id = pl.DeviceIdType.MESH
    moves = [
        pltpu.make_async_copy(source, target, loads.at[i])
        for i, (source, target) in enumerate(
            (
                (keep_in, keep_row), (pixels_in, pixels), (keep_in, keep), (wqkv_in, wqkv), (wp_in, wp),
                (table_in, table), (gain_a_in, gain_a), (gain_m_in, gain_m), (wh_in, wh),
                (wo_in, wo), (dests_in, dests), (slots_in, slots),
            )
        )
    ]
    for move in moves:
        move.start()

    barrier = pltpu.get_barrier_semaphore()

    def greet(i, _):
        peer = lax.rem(me + i, bands)
        pl.semaphore_signal(barrier, inc=1, device_id={"band": peer}, device_id_type=mesh_id)
        return 0

    lax.fori_loop(1, bands, greet, 0)

    live = count[0]
    moves[0].wait()
    told[...] = jnp.zeros(told.shape, jnp.int32)
    told[:, 0:windows] = jnp.broadcast_to(keep_row[...], (8, windows))
    mine = told[...]
    rank = ranks(mine, windows)
    final = jnp.max(jnp.where(iota(rank.shape, 1) == windows - 1, rank, 0.0), axis=1, keepdims=True)
    line = iota(told.shape, 0)
    extra = jnp.where(line == 1, jnp.broadcast_to(final, told.shape).astype(jnp.int32), live)
    told[...] = jnp.where(line == 0, rank.astype(jnp.int32), extra)

    def nxt_copy(c):
        return pltpu.make_async_remote_copy(
            src_ref=nxt_out.at[c],
            dst_ref=nxt_buf.at[c],
            send_sem=halo_send.at[c],
            recv_sem=halo_recv.at[c],
            device_id={"band": left},
            device_id_type=mesh_id,
        )

    odd = lax.rem(me, 2) == 1
    fold = WIDER

    def prv_send(part, source, from_chunk, to_chunk, device, mark):
        first = part * fold
        return pltpu.make_async_remote_copy(
            src_ref=source.at[pl.ds(from_chunk + first, fold)],
            dst_ref=prv_buf.at[pl.ds(to_chunk + first, fold)],
            send_sem=halo_send.at[groups + 1 + 2 * mark + part],
            recv_sem=halo_recv.at[groups + 1 + 2 * mark + part],
            device_id={"band": device},
            device_id_type=mesh_id,
        )

    def direct(part):
        return prv_send(part, prv_out, 0, 0, right, 0)

    def relay(part):
        return prv_send(part, prv_out, 0, groups, lax.rem(me + 2, bands), 1)

    def forward(part):
        return prv_send(part, prv_buf, groups, 0, left, 0)

    told_copy = pltpu.make_async_remote_copy(
        src_ref=told,
        dst_ref=told_buf,
        send_sem=halo_send.at[groups],
        recv_sem=halo_recv.at[groups],
        device_id={"band": right},
        device_id_type=mesh_id,
    )
    pl.semaphore_wait(barrier, bands - 1)
    told_copy.start()
    moves[1].wait()
    moves[2].wait()
    for h in range(halves):
        part = pixels[:, :, h * LANES : (h + 1) * LANES].astype(F32)
        planes[h] = part.reshape(channels * rows, LANES)

    def arrange(first, matrix, target, done):
        moved = [
            dot(plane_row(planes, first + r, channels).astype(BF), matrix) for r in range(SHIFT)
        ]
        for h in range(halves):
            cols_h = slice(h * LANES, (h + 1) * LANES)
            for r in range(0, SHIFT, 2):
                even, uneven = swap_parts(moved[r][:, cols_h], moved[r + 1][:, cols_h])
                lanes = slice(r * PART, (r + 2) * PART)
                target[2 * h, :, lanes] = even.astype(BF)
                target[2 * h + 1, :, lanes] = uneven.astype(BF)
            done(h)

    columns[0] = column_order(rank, cols)

    def start_relay(h):
        if h == 0:
            direct(0).start()
            return

        @pl.when(odd)
        def _():
            relay(1).start()

    def start_nxt(h):
        nxt_copy(2 * h).start()
        nxt_copy(2 * h + 1).start()

    arrange(rows - SHIFT, columns[0], prv_out, start_relay)
    told_copy.wait()
    news = told_buf[...]
    columns[1] = column_order(news[0:1].astype(F32), cols)
    arrange(0, columns[1], nxt_out, start_nxt)
    live_prev, final_prev = news[2, 0], news[1, 0]
    final_own = jnp.where(keep[0, windows - 1] == 1, live - 1, windows - 1)

    order[...] = window_order()
    for move in moves[3:]:
        move.wait()
    w_in[...] = dot_t(spread_heads(3 * DEPTH, 3 * CHAN), wqkv[...]).astype(BF)
    w_out[...] = dot(spread_heads(DEPTH, CHAN), wp[...]).T.astype(BF)
    w_hid[...] = wh[...].astype(F32).T.astype(BF)
    gains[0] = jnp.broadcast_to(gain_a[...], (LANES, channels)).T
    gains[1] = jnp.broadcast_to(gain_m[...], (LANES, channels)).T
    bias_strips(table, strips)
    bias_fill(strips, bias, me == bands - 1, me == 0)

    padded = channels + 4

    def windows_of(upper_part, lower_part):
        return dot(jnp.concatenate([upper_part, lower_part], axis=1), order[...])

    def attend_windows(x, start, kind, last):
        def edge(g):
            return bias[2 * kind + (start + g == last).astype(jnp.int32)]

        return attend(x, gains[0], w_in[...], w_out[...], edge)

    def step(c, _):
        nxt_copy(c).wait()

        @pl.when((c == 1) & odd)
        def _():
            relay(1).wait()
            forward(1).start()

        @pl.when((c == groups - 1) & ~odd)
        def _():
            direct(1).start()

        x = windows_of(prv_out[c], nxt_buf[c])
        origin[c] = x.astype(BF)
        own = attend_windows(x, c * GROUP, 0, final_own)
        states[c] = own
        wide = jnp.concatenate([own.astype(F32), jnp.zeros((4, SIZE), F32)], axis=0)
        for k in range(SIZE // LANES):
            packed[c * (SIZE // LANES) + k] = wide[:, k * LANES : (k + 1) * LANES].astype(BF)
        return 0

    slot_row = iota((padded, LANES), 0) >= channels
    member = iota((padded, LANES), 1) // TOK

    def pack(index, peer, j):
        t = jnp.int32(0)
        found = jnp.int32(0)
        for i in range(span):
            hit = dests[0, j * span + i] == peer
            t = jnp.where(hit, j * span + i, t)
            found = jnp.where(hit, 1, found)
        known = jnp.where(found > 0, live - t * TILE, 0)
        slot = jnp.where(known > 0, slots[0, t], CAP).astype(F32)
        value = packed[t]
        value = jnp.where(member < known, value, jnp.zeros_like(value))
        outgoing[index] = jnp.where(slot_row, jnp.full((padded, LANES), slot, F32).astype(BF), value)

    def peer_of(n):
        away = n >= half
        m = jnp.where(away, n - half + 1, n)
        cross = (m >= fourth).astype(jnp.int32)
        row = lax.rem(lax.div(lax.rem(me, half), 2) + m, fourth)
        side = lax.rem(lax.rem(me, 2) + cross, 2)
        return jnp.where(away, near, far) + 2 * row + side

    def tile_copy(n, j):
        return pltpu.make_async_remote_copy(
            src_ref=outgoing.at[n * pairs + j],
            dst_ref=incoming.at[me * pairs + j],
            send_sem=tile_send.at[n * pairs + j],
            recv_sem=tile_recv.at[n * pairs + j],
            device_id={"band": peer_of(n)},
            device_id_type=mesh_id,
        )

    stage = groups // pairs

    def round_of(j, _):
        lax.fori_loop(j * stage, (j + 1) * stage, step, 0)

        def dispatch(n, _):
            pack(n * pairs + j, peer_of(n), j)
            tile_copy(n, j).start()
            return 0

        lax.fori_loop(0, bands - 1, dispatch, 0)
        kept_here = (bands - 1) * pairs + j
        pack(kept_here, me, j)
        incoming[me * pairs + j] = outgoing[kept_here]
        return 0

    lax.fori_loop(0, pairs, round_of, 0)

    lane = iota((channels, WIDER * SIZE), 1)
    upper = lane % TOK < HALF

    def finish(i, _):
        direct(i).wait_recv()

        @pl.when(~odd | (i == 0))
        def _():
            direct(i).wait_send()

        @pl.when(odd & (i > 0))
        def _():
            forward(i).wait_send()

        number = WIDER * GROUP
        chunks = [i * WIDER + k for k in range(WIDER)]
        x = jnp.concatenate([windows_of(prv_buf[c], nxt_out[c]) for c in chunks], axis=1)
        prev = attend_windows(x, i * number, 1, final_prev)
        own = jnp.concatenate([states[c] for c in chunks], axis=1)
        done = feed(jnp.where(upper, own, prev), gains[1], w_hid[...], wo[...])
        before = jnp.concatenate([origin[c] for c in chunks], axis=1)
        before = jnp.where(upper, before, x.astype(BF))
        position = i * number + lane // TOK
        chosen = position < jnp.where(upper, live, live_prev)
        after = jnp.where(chosen, done, before)
        one, two = (dot_t(after[:, k * SIZE : (k + 1) * SIZE], order[...]) for k in range(WIDER))
        for k in range(SIZE // LANES):
            cut = slice(k * LANES, (k + 1) * LANES)
            even, uneven = swap_parts(one[:, cut], two[:, cut])
            r = (2 * k + SHIFT) % rows
            done_rows[i, r] = even.astype(BF)
            done_rows[i, r + 1] = uneven.astype(BF)
        return 0

    lax.fori_loop(0, groups // WIDER, finish, 0)
    for r in range(rows):
        row = jnp.concatenate([done_rows[h, r] for h in range(halves)], axis=1)
        row = dot_t(row, columns[0] if r >= rows - SHIFT else columns[1])
        for h in range(halves):
            planes[h, pl.ds(r, channels, stride=WIN), :] = row[:, h * LANES : (h + 1) * LANES]
    for h in range(halves):
        restored[:, :, h * LANES : (h + 1) * LANES] = (
            planes[h].reshape(channels, rows, LANES).astype(BF)
        )

    def collect(i, _):
        for j in range(pairs):
            tile_copy(i, j).wait()
        return 0

    lax.fori_loop(0, bands - 1, collect, 0)


def place_kernel(incoming, restored, restored_out, work_out, planes, work, sems):
    total, padded, _ = incoming.shape
    channels = work.shape[0]
    blocks = range(0, channels, CUT)
    moves = [
        pltpu.make_async_copy(restored.at[b : b + CUT], restored_out.at[b : b + CUT], sems.at[0, i])
        for i, b in enumerate(blocks)
    ]
    for move in moves:
        move.start()
    head = incoming[:, padded - 8 :, :].astype(F32)
    head = jnp.max(jnp.where(iota(head.shape, 1) >= 4, head, 0.0), axis=1)
    slot = jnp.max(head, axis=1, keepdims=True).astype(jnp.int32)
    match = slot == iota((total, LANES), 1)
    source = jnp.where(match, iota((total, LANES), 0), -1).astype(F32)
    source = jnp.max(source, axis=0, keepdims=True).astype(jnp.int32)
    chosen = [source[0, k] for k in range(CAP)]
    sent = []
    for i, b in enumerate(blocks):
        for k in range(CAP):
            block = incoming[jnp.maximum(chosen[k], 0), b : b + CUT].astype(F32)
            block = jnp.where(chosen[k] >= 0, block, 0.0)
            planes[pl.ds(b * CAP + k, CUT, stride=CAP), :] = block
        value = planes[b * CAP : (b + CUT) * CAP].reshape(CUT, CAP, TILE * TOK)
        work[b : b + CUT] = value.astype(BF)
        sent.append(
            pltpu.make_async_copy(work.at[b : b + CUT], work_out.at[b : b + CUT], sems.at[1, i])
        )
        if i > 0:
            sent[i - 1].start()
    for move in moves:
        move.wait()
    sent[-1].start()
    for move in sent:
        move.wait()


def shards(
    pixels, keep_mask, band_counts, plan_dest, plan_slot, bias_table, gain_attn, qkv_weight,
    proj_weight, gain_mlp, hidden_weight, output_weight,
):
    bands = lax.axis_size("band")
    rows, cols, channels = pixels.shape
    windows = cols // WIN
    halves = cols // LANES
    tiles = windows // TILE
    pairs = -(-tiles // bands)
    smem = pl.BlockSpec(memory_space=pltpu.SMEM)
    vmem = pl.BlockSpec(memory_space=pltpu.VMEM)
    tile_shape = (bands * pairs, channels + 4, LANES)
    groups = windows // GROUP
    nxt_shape = (groups, channels, SHIFT * PART)
    operands = (
        keep_mask, plan_dest, plan_slot, jnp.transpose(pixels, (2, 0, 1)),
        bias_table.T, gain_attn[None], qkv_weight, proj_weight, gain_mlp[None], hidden_weight,
        output_weight.T,
    )
    restored, incoming = pl.pallas_call(
        block_kernel,
        out_shape=(
            jax.ShapeDtypeStruct((channels, rows, cols), BF),
            jax.ShapeDtypeStruct(tile_shape, BF),
        ),
        in_specs=[smem] + [pl.BlockSpec(memory_space=pltpu.HBM)] * len(operands),
        out_specs=(vmem, vmem),
        scratch_shapes=[
            pltpu.SMEM(operands[0].shape, jnp.int32),
            pltpu.SMEM(operands[1].shape, jnp.int32),
            pltpu.SMEM(operands[2].shape, jnp.int32),
            pltpu.VMEM(operands[0].shape, jnp.int32),
            *(pltpu.VMEM(operand.shape, operand.dtype) for operand in operands[3:]),
            pltpu.SemaphoreType.DMA((len(operands) + 1,)),
            pltpu.VMEM((halves, channels * rows, LANES), F32),
            pltpu.VMEM(nxt_shape, BF),
            pltpu.VMEM(nxt_shape, BF),
            pltpu.VMEM(nxt_shape, BF),
            pltpu.VMEM((2 * groups, channels, SHIFT * PART), BF),
            pltpu.VMEM((8, LANES), jnp.int32),
            pltpu.VMEM((8, LANES), jnp.int32),
            pltpu.VMEM((3 * DEPTH, channels), BF),
            pltpu.VMEM((channels, DEPTH), BF),
            pltpu.VMEM((hidden_weight.shape[1], channels), BF),
            pltpu.VMEM((2, channels, LANES), F32),
            pltpu.VMEM((8 * WIN, LANES), F32),
            pltpu.VMEM((4, TOK, QUERIES), F32),
            pltpu.VMEM((SIZE, SIZE), BF),
            pltpu.VMEM((2, cols, cols), BF),
            pltpu.VMEM((groups, channels, SIZE), BF),
            pltpu.VMEM((groups, channels, SIZE), BF),
            pltpu.VMEM((halves, rows, channels, LANES), BF),
            pltpu.VMEM((tiles, channels + 4, LANES), BF),
            pltpu.VMEM(tile_shape, BF),
            pltpu.SemaphoreType.DMA((groups + 5,)),
            pltpu.SemaphoreType.DMA((groups + 5,)),
            pltpu.SemaphoreType.DMA((bands * pairs,)),
            pltpu.SemaphoreType.DMA((bands * pairs,)),
        ],
        compiler_params=pltpu.CompilerParams(
            vmem_limit_bytes=40 * 1024 * 1024, collective_id=0, has_side_effects=True
        ),
        cost_estimate=pl.CostEstimate(flops=10**10, bytes_accessed=10**7, transcendentals=10**6),
        name="block",
    )(band_counts, *(pltpu.with_memory_space_constraint(value, pltpu.HBM) for value in operands))
    restored, work = pl.pallas_call(
        place_kernel,
        out_shape=(
            jax.ShapeDtypeStruct((channels, rows, cols), BF),
            jax.ShapeDtypeStruct((channels, CAP, TILE * TOK), BF),
        ),
        in_specs=[vmem, vmem],
        out_specs=(pl.BlockSpec(memory_space=pl.ANY), pl.BlockSpec(memory_space=pl.ANY)),
        scratch_shapes=[
            pltpu.VMEM((channels * CAP, TILE * TOK), F32),
            pltpu.VMEM((channels, CAP, TILE * TOK), BF),
            pltpu.SemaphoreType.DMA((2, -(-channels // CUT))),
        ],
        compiler_params=pltpu.CompilerParams(vmem_limit_bytes=16 * 1024 * 1024),
        name="place",
    )(incoming, restored)
    return jnp.transpose(restored, (1, 2, 0)), jnp.transpose(work, (1, 2, 0))


def solution(mesh):
    split = P(("img", "band"))
    in_specs = (split,) * 5 + (P(),) * 7
    return jax.shard_map(shards, mesh=mesh, in_specs=in_specs, out_specs=(split, split), check_vma=False)
```

```python
import jax
import jax.numpy as jnp
from jax import lax
from jax.experimental import pallas as pl
from jax.experimental.pallas import tpu as pltpu
from jax.sharding import PartitionSpec as P

CHAN = 180
HEADS = 6
WIN = 8
TILE = 2
SHIFT = 4
CAP = 8
TOK = WIN * WIN
HALF = TOK // 2
HEAD_DIM = CHAN // HEADS
GROUP = 8
WIDER = 2
SIZE = GROUP * TOK
AHEAD = 4
CUT = 60
PART = GROUP * WIN
PAD = 32
DEPTH = HEADS * PAD
QUERIES = HEADS * TOK
LANES = 128
SLOT_LANE = 120

EPSILON = 1e-05
BF = jnp.bfloat16
F32 = jnp.float32


def layer_norm(values, gain):
    center = values - jnp.sum(values, axis=0, keepdims=True) * (1.0 / CHAN)
    spread = jnp.sum(center * center, axis=0, keepdims=True) * (1.0 / CHAN)
    scaled = center * lax.rsqrt(spread + EPSILON)
    parts = [scaled[:, i : i + LANES] * gain for i in range(0, values.shape[1], LANES)]
    return jnp.concatenate(parts, axis=1).astype(BF)


def dot(a, b):
    return jnp.dot(a, b, preferred_element_type=F32)


def dot_t(a, b):
    return lax.dot_general(a, b, (((1,), (1,)), ((), ())), preferred_element_type=F32)


def iota(shape, axis):
    return lax.broadcasted_iota(jnp.int32, shape, axis)


def bias_strips(table, strips):
    heads, entries = table.shape
    values = jnp.concatenate([table[...], jnp.zeros((8 - heads, entries), F32)], axis=0)
    high = values.astype(BF).astype(F32)
    middle = (values - high).astype(BF).astype(F32)
    low = values - high - middle
    parts = jnp.concatenate([high, middle, low], axis=0).astype(BF)
    shape = (entries, WIN * LANES)
    entry, lane = iota(shape, 0), iota(shape, 1)
    step = (lane % LANES) // WIN
    wanted = step * (2 * WIN - 1) + lane % WIN - lane // LANES + WIN - 1
    pick = jnp.where((entry == wanted) & (step < 2 * WIN - 1), 1.0, 0.0).astype(BF)
    found = dot(parts, pick)
    found = found[0:8] + found[8:16] + found[16:24]
    for c in range(WIN):
        strips[pl.ds(c, 8, stride=WIN), :] = found[:, c * LANES : (c + 1) * LANES]


def bias_fill(strips, bias, own_last, prev_last):
    first_half = iota((WIN, LANES), 1) < TOK
    for r in range(WIN):
        by = 2 * LANES - (WIN - 1 - r) * WIN
        tiles = []
        for h in range(0, HEADS, 2):
            even = strips[h * WIN : (h + 1) * WIN, :]
            odd = strips[(h + 1) * WIN : (h + 2) * WIN, :]
            tiles.append(
                jnp.where(
                    first_half,
                    pltpu.roll(even, by % LANES, 1),
                    pltpu.roll(odd, (by + TOK) % LANES, 1),
                )
            )
        base = jnp.concatenate(tiles, axis=1)
        shape = (WIN, QUERIES)
        key, query = iota(shape, 0), iota(shape, 1) % TOK
        rows_differ = (query // WIN >= SHIFT) != (r >= SHIFT)
        cols_differ = (key >= SHIFT) != (query % WIN >= SHIFT)
        rows = slice(r * WIN, (r + 1) * WIN)
        for k, last in enumerate((own_last, prev_last)):
            row_pen = jnp.where(rows_differ, jnp.where(last, -100.0, 0.0).astype(F32), 0.0)
            bias[2 * k, rows] = base + row_pen
            bias[2 * k + 1, rows] = base + jnp.where(cols_differ, -100.0, row_pen)


def spread_heads(rows, cols):
    row, col = iota((rows, cols), 0), iota((rows, cols), 1)
    inside = row % DEPTH
    wanted = row // DEPTH * CHAN + inside // PAD * HEAD_DIM + inside % PAD
    return jnp.where((inside % PAD < HEAD_DIM) & (wanted == col), 1.0, 0.0).astype(BF)


def attend(x, gain, w_in, w_out, bias_of):
    normed = layer_norm(x, gain)
    mixed = dot(w_in, normed)
    q = mixed[0:DEPTH] * HEAD_DIM ** (-0.5)
    k = mixed[DEPTH : 2 * DEPTH].T.astype(BF)
    v = mixed[2 * DEPTH :].astype(BF)
    low = iota((PAD, LANES), 1) < TOK
    blank = jnp.zeros((PAD, LANES), F32)
    none = jnp.zeros((TOK, LANES), BF)

    def weigh(pair):
        lanes = slice(pair * LANES, (pair + 1) * LANES)
        q_pair = q[:, lanes]
        q_turn = pltpu.roll(q_pair, TOK, 1)
        weights = []
        for side in range(2):
            g = 2 * pair + side
            blocks = []
            for h in range(HEADS):
                part = slice(h * PAD, (h + 1) * PAD)
                value = q_pair[part] if h % 2 == side else q_turn[part]
                value = jnp.where(low if h % 2 == 0 else ~low, value, 0.0)
                row = [blank] * (HEADS // 2)
                row[h // 2] = value
                blocks.append(jnp.concatenate(row, axis=1))
            spread_q = jnp.concatenate(blocks, axis=0).astype(BF)
            scores = dot(k[g * TOK : (g + 1) * TOK], spread_q) + bias_of(g)
            top = jnp.max(scores, axis=0, keepdims=True)
            grown = jnp.exp(scores - top)
            weights.append((grown * (1.0 / jnp.sum(grown, axis=0, keepdims=True))).astype(BF))
        return weights

    def mix(pair, weights):
        lanes = slice(pair * LANES, (pair + 1) * LANES)
        rows = []
        for j in range(HEADS // 2):
            cut = slice(j * LANES, (j + 1) * LANES)
            both = jnp.concatenate(
                [
                    jnp.concatenate([weights[0][:, cut], none], axis=1),
                    jnp.concatenate([none, weights[1][:, cut]], axis=1),
                ],
                axis=0,
            )
            found = dot(v[2 * j * PAD : 2 * (j + 1) * PAD, lanes], both)
            one, two = found[:, :LANES], found[:, LANES:]
            rows.append(jnp.where(low, one[:PAD], pltpu.roll(two[:PAD], TOK, 1)))
            rows.append(jnp.where(low, pltpu.roll(one[PAD:], TOK, 1), two[PAD:]))
        return jnp.concatenate(rows, axis=0).astype(BF)

    count = x.shape[1] // LANES
    ready, joined = {}, []
    for pair in range(count + AHEAD):
        if pair < count:
            ready[pair] = weigh(pair)
        if pair >= AHEAD:
            joined.append(mix(pair - AHEAD, ready.pop(pair - AHEAD)))
    joined = jnp.concatenate(joined, axis=1)
    return (x + dot(w_out, joined)).astype(BF)


def feed(states, gain, wh, wo):
    flat = states.astype(F32)
    normed = layer_norm(flat, gain)
    inner = jax.nn.gelu(dot(wh, normed)).astype(BF)
    return (flat + dot(wo, inner)).astype(BF)


def window_order():
    shape = (SIZE, SIZE)
    source, target = iota(shape, 0), iota(shape, 1)
    col = source % PART
    row = source // (SIZE // 2) * SHIFT + source % (SIZE // 2) // PART
    wanted = col // WIN * TOK + row * WIN + col % WIN
    return jnp.where(wanted == target, 1.0, 0.0).astype(BF)


def ranks(flags, windows):
    kept = flags.astype(F32)
    other = jnp.where(iota(flags.shape, 1) < windows, 1.0, 0.0) - kept
    tri = (LANES, LANES)
    before = jnp.where(iota(tri, 0) < iota(tri, 1), 1.0, 0.0).astype(BF)
    total = dot(kept.astype(BF), jnp.ones(tri, BF))
    ahead = dot(kept.astype(BF), before)
    return jnp.where(flags == 1, ahead, total + dot(other.astype(BF), before))


def column_order(rank, cols):
    shape = (cols, LANES)
    shifted = (iota(shape, 0) + cols - SHIFT) % cols
    spread = jnp.where(shifted // WIN == iota(shape, 1), jnp.broadcast_to(rank[0:1], shape), 0.0)
    first = dot(spread.astype(BF), jnp.ones((LANES, cols), BF))
    shape = (cols, cols)
    inside = ((iota(shape, 0) + cols - SHIFT) % WIN).astype(F32)
    wanted = first * WIN + inside
    return jnp.where(wanted == iota(shape, 1).astype(F32), 1.0, 0.0).astype(BF)


def swap_parts(one, two):
    front = iota(one.shape, 1) < PART
    even = jnp.where(front, one, pltpu.roll(two, PART, 1))
    return even, jnp.where(front, pltpu.roll(one, PART, 1), two)


def plane_row(planes, row, channels):
    halves = planes.shape[0]
    return jnp.concatenate(
        [planes[h, pl.ds(row, channels, stride=WIN), :] for h in range(halves)], axis=1
    )


def block_kernel(
    count, keep_in, dests_in, slots_in, pixels_in, table_in, gain_a_in, wqkv_in, wp_in,
    gain_m_in, wh_in, wo_in,
    restored, incoming,
    keep, dests, slots, keep_row, pixels, table, gain_a, wqkv, wp, gain_m, wh, wo, loads,
    planes, nxt_out, prv_out, nxt_buf, prv_buf, told, told_buf, w_in, w_out, w_hid, gains,
    strips, bias, order, columns, states, origin, done_rows, packed, outgoing,
    halo_send, halo_recv, tile_send, tile_recv,
):
    bands = lax.axis_size("band")
    me = lax.axis_index("band")
    right, left = lax.rem(me + 1, bands), lax.rem(me + bands - 1, bands)
    channels, rows, cols = pixels.shape
    windows = cols // WIN
    groups = windows // GROUP
    half = bands // 2
    fourth = half // 2
    far = jnp.where(me < half, half, 0)
    near = half - far
    halves = cols // LANES
    tiles = windows // TILE
    pairs = -(-tiles // bands)
    span = min(bands, tiles)
    mesh_id = pl.DeviceIdType.MESH
    moves = [
        pltpu.make_async_copy(source, target, loads.at[i])
        for i, (source, target) in enumerate(
            (
                (keep_in, keep_row), (pixels_in, pixels), (keep_in, keep), (wqkv_in, wqkv), (wp_in, wp),
                (table_in, table), (gain_a_in, gain_a), (gain_m_in, gain_m), (wh_in, wh),
                (wo_in, wo), (dests_in, dests), (slots_in, slots),
            )
        )
    ]
    for move in moves:
        move.start()

    barrier = pltpu.get_barrier_semaphore()

    def greet(i, _):
        peer = lax.rem(me + i, bands)
        pl.semaphore_signal(barrier, inc=1, device_id={"band": peer}, device_id_type=mesh_id)
        return 0

    lax.fori_loop(1, bands, greet, 0)

    live = count[0]
    moves[0].wait()
    told[...] = jnp.zeros(told.shape, jnp.int32)
    told[:, 0:windows] = jnp.broadcast_to(keep_row[...], (8, windows))
    mine = told[...]
    rank = ranks(mine, windows)
    line = iota(told.shape, 0)
    told[...] = jnp.where(line == 0, rank.astype(jnp.int32), live)

    def nxt_copy(c):
        return pltpu.make_async_remote_copy(
            src_ref=nxt_out.at[c],
            dst_ref=nxt_buf.at[c],
            send_sem=halo_send.at[c],
            recv_sem=halo_recv.at[c],
            device_id={"band": left},
            device_id_type=mesh_id,
        )

    odd = lax.rem(me, 2) == 1
    fold = WIDER

    def prv_send(part, source, from_chunk, to_chunk, device, mark):
        first = part * fold
        return pltpu.make_async_remote_copy(
            src_ref=source.at[pl.ds(from_chunk + first, fold)],
            dst_ref=prv_buf.at[pl.ds(to_chunk + first, fold)],
            send_sem=halo_send.at[groups + 1 + 2 * mark + part],
            recv_sem=halo_recv.at[groups + 1 + 2 * mark + part],
            device_id={"band": device},
            device_id_type=mesh_id,
        )

    def direct(part):
        return prv_send(part, prv_out, 0, 0, right, 0)

    def relay(part):
        return prv_send(part, prv_out, 0, groups, lax.rem(me + 2, bands), 1)

    def forward(part):
        return prv_send(part, prv_buf, groups, 0, left, 0)

    told_copy = pltpu.make_async_remote_copy(
        src_ref=told,
        dst_ref=told_buf,
        send_sem=halo_send.at[groups],
        recv_sem=halo_recv.at[groups],
        device_id={"band": right},
        device_id_type=mesh_id,
    )
    pl.semaphore_wait(barrier, bands - 1)
    told_copy.start()
    moves[1].wait()
    moves[2].wait()
    for h in range(halves):
        part = pixels[:, :, h * LANES : (h + 1) * LANES].astype(F32)
        planes[h] = part.reshape(channels * rows, LANES)

    def arrange(first, matrix, target, done):
        moved = [
            dot(plane_row(planes, first + r, channels).astype(BF), matrix) for r in range(SHIFT)
        ]
        for h in range(halves):
            cols_h = slice(h * LANES, (h + 1) * LANES)
            for r in range(0, SHIFT, 2):
                even, uneven = swap_parts(moved[r][:, cols_h], moved[r + 1][:, cols_h])
                lanes = slice(r * PART, (r + 2) * PART)
                target[2 * h, :, lanes] = even.astype(BF)
                target[2 * h + 1, :, lanes] = uneven.astype(BF)
            done(h)

    columns[0] = column_order(rank, cols)

    def start_relay(h):
        if h == 0:
            direct(0).start()
            return

        @pl.when(odd)
        def _():
            relay(1).start()

    def start_nxt(h):
        nxt_copy(2 * h).start()
        nxt_copy(2 * h + 1).start()

    arrange(rows - SHIFT, columns[0], prv_out, start_relay)
    told_copy.wait()
    news = told_buf[...]
    columns[1] = column_order(news[0:1].astype(F32), cols)
    arrange(0, columns[1], nxt_out, start_nxt)
    live_prev, final_prev = news[1, 0], news[0, windows - 1]
    final_own = jnp.where(keep[0, windows - 1] == 1, live - 1, windows - 1)

    order[...] = window_order()
    for move in moves[3:]:
        move.wait()
    w_in[...] = dot_t(spread_heads(3 * DEPTH, 3 * CHAN), wqkv[...]).astype(BF)
    w_out[...] = dot(spread_heads(DEPTH, CHAN), wp[...]).T.astype(BF)
    w_hid[...] = wh[...].astype(F32).T.astype(BF)
    gains[0] = jnp.broadcast_to(gain_a[...], (LANES, channels)).T
    gains[1] = jnp.broadcast_to(gain_m[...], (LANES, channels)).T
    bias_strips(table, strips)
    bias_fill(strips, bias, me == bands - 1, me == 0)

    padded = channels + 4

    def windows_of(upper_part, lower_part):
        return dot(jnp.concatenate([upper_part, lower_part], axis=1), order[...])

    def attend_windows(x, start, kind, last):
        def edge(g):
            return bias[2 * kind + (start + g == last).astype(jnp.int32)]

        return attend(x, gains[0], w_in[...], w_out[...], edge)

    def step(c, _):
        nxt_copy(c).wait()

        @pl.when((c == 1) & odd)
        def _():
            relay(1).wait()
            forward(1).start()

        @pl.when((c == groups - 1) & ~odd)
        def _():
            direct(1).start()

        x = windows_of(prv_out[c], nxt_buf[c])
        origin[c] = x.astype(BF)
        own = attend_windows(x, c * GROUP, 0, final_own)
        states[c] = own
        wide = jnp.concatenate([own.astype(F32), jnp.zeros((4, SIZE), F32)], axis=0)
        for k in range(SIZE // LANES):
            packed[c * (SIZE // LANES) + k] = wide[:, k * LANES : (k + 1) * LANES].astype(BF)
        return 0

    slot_row = iota((padded, LANES), 0) >= channels
    member = iota((padded, LANES), 1) // TOK

    def pack(index, peer, j):
        t = jnp.int32(0)
        found = jnp.int32(0)
        for i in range(span):
            hit = dests[0, j * span + i] == peer
            t = jnp.where(hit, j * span + i, t)
            found = jnp.where(hit, 1, found)
        known = jnp.where(found > 0, live - t * TILE, 0)
        slot = jnp.where(known > 0, slots[0, t], CAP).astype(F32)
        value = packed[t]
        value = jnp.where(member < known, value, jnp.zeros_like(value))
        outgoing[index] = jnp.where(slot_row, jnp.full((padded, LANES), slot, F32).astype(BF), value)

    def peer_of(n):
        away = n >= half
        m = jnp.where(away, n - half + 1, n)
        cross = (m >= fourth).astype(jnp.int32)
        row = lax.rem(lax.div(lax.rem(me, half), 2) + m, fourth)
        side = lax.rem(lax.rem(me, 2) + cross, 2)
        return jnp.where(away, near, far) + 2 * row + side

    def tile_copy(n, j):
        return pltpu.make_async_remote_copy(
            src_ref=outgoing.at[n * pairs + j],
            dst_ref=incoming.at[me * pairs + j],
            send_sem=tile_send.at[n * pairs + j],
            recv_sem=tile_recv.at[n * pairs + j],
            device_id={"band": peer_of(n)},
            device_id_type=mesh_id,
        )

    stage = groups // pairs

    def round_of(j, _):
        lax.fori_loop(j * stage, (j + 1) * stage, step, 0)

        def dispatch(n, _):
            pack(n * pairs + j, peer_of(n), j)
            tile_copy(n, j).start()
            return 0

        lax.fori_loop(0, bands - 1, dispatch, 0)
        kept_here = (bands - 1) * pairs + j
        pack(kept_here, me, j)
        incoming[me * pairs + j] = outgoing[kept_here]
        return 0

    lax.fori_loop(0, pairs, round_of, 0)

    lane = iota((channels, WIDER * SIZE), 1)
    upper = lane % TOK < HALF

    def finish(i, _):
        direct(i).wait_recv()

        @pl.when(~odd | (i == 0))
        def _():
            direct(i).wait_send()

        @pl.when(odd & (i > 0))
        def _():
            forward(i).wait_send()

        number = WIDER * GROUP
        chunks = [i * WIDER + k for k in range(WIDER)]
        x = jnp.concatenate([windows_of(prv_buf[c], nxt_out[c]) for c in chunks], axis=1)
        prev = attend_windows(x, i * number, 1, final_prev)
        own = jnp.concatenate([states[c] for c in chunks], axis=1)
        done = feed(jnp.where(upper, own, prev), gains[1], w_hid[...], wo[...])
        before = jnp.concatenate([origin[c] for c in chunks], axis=1)
        before = jnp.where(upper, before, x.astype(BF))
        position = i * number + lane // TOK
        chosen = position < jnp.where(upper, live, live_prev)
        after = jnp.where(chosen, done, before)
        one, two = (dot_t(after[:, k * SIZE : (k + 1) * SIZE], order[...]) for k in range(WIDER))
        for k in range(SIZE // LANES):
            cut = slice(k * LANES, (k + 1) * LANES)
            even, uneven = swap_parts(one[:, cut], two[:, cut])
            r = (2 * k + SHIFT) % rows
            done_rows[i, r] = even.astype(BF)
            done_rows[i, r + 1] = uneven.astype(BF)
        return 0

    lax.fori_loop(0, groups // WIDER, finish, 0)
    for r in range(rows):
        row = jnp.concatenate([done_rows[h, r] for h in range(halves)], axis=1)
        row = dot_t(row, columns[0] if r >= rows - SHIFT else columns[1])
        for h in range(halves):
            planes[h, pl.ds(r, channels, stride=WIN), :] = row[:, h * LANES : (h + 1) * LANES]
    for h in range(halves):
        restored[:, :, h * LANES : (h + 1) * LANES] = (
            planes[h].reshape(channels, rows, LANES).astype(BF)
        )

    def collect(i, _):
        for j in range(pairs):
            tile_copy(i, j).wait()
        return 0

    lax.fori_loop(0, bands - 1, collect, 0)


def place_kernel(incoming, restored, restored_out, work_out, planes, work, sems):
    total, padded, _ = incoming.shape
    channels = work.shape[0]
    blocks = range(0, channels, CUT)
    moves = [
        pltpu.make_async_copy(restored.at[b : b + CUT], restored_out.at[b : b + CUT], sems.at[0, i])
        for i, b in enumerate(blocks)
    ]
    for move in moves:
        move.start()
    head = incoming[:, padded - 8 :, :].astype(F32)
    head = jnp.max(jnp.where(iota(head.shape, 1) >= 4, head, 0.0), axis=1)
    slot = jnp.max(head, axis=1, keepdims=True).astype(jnp.int32)
    match = slot == iota((total, LANES), 1)
    source = jnp.where(match, iota((total, LANES), 0), -1).astype(F32)
    source = jnp.max(source, axis=0, keepdims=True).astype(jnp.int32)
    chosen = [source[0, k] for k in range(CAP)]
    sent = []
    for i, b in enumerate(blocks):
        for k in range(CAP):
            block = incoming[jnp.maximum(chosen[k], 0), b : b + CUT].astype(F32)
            block = jnp.where(chosen[k] >= 0, block, 0.0)
            planes[pl.ds(b * CAP + k, CUT, stride=CAP), :] = block
        value = planes[b * CAP : (b + CUT) * CAP].reshape(CUT, CAP, TILE * TOK)
        work[b : b + CUT] = value.astype(BF)
        sent.append(
            pltpu.make_async_copy(work.at[b : b + CUT], work_out.at[b : b + CUT], sems.at[1, i])
        )
        sent[-1].start()
    for move in moves:
        move.wait()
    for move in sent:
        move.wait()


def shards(
    pixels, keep_mask, band_counts, plan_dest, plan_slot, bias_table, gain_attn, qkv_weight,
    proj_weight, gain_mlp, hidden_weight, output_weight,
):
    bands = lax.axis_size("band")
    rows, cols, channels = pixels.shape
    windows = cols // WIN
    halves = cols // LANES
    tiles = windows // TILE
    pairs = -(-tiles // bands)
    smem = pl.BlockSpec(memory_space=pltpu.SMEM)
    vmem = pl.BlockSpec(memory_space=pltpu.VMEM)
    tile_shape = (bands * pairs, channels + 4, LANES)
    groups = windows // GROUP
    nxt_shape = (groups, channels, SHIFT * PART)
    operands = (
        keep_mask, plan_dest, plan_slot, jnp.transpose(pixels, (2, 0, 1)),
        bias_table.T, gain_attn[None], qkv_weight, proj_weight, gain_mlp[None], hidden_weight,
        output_weight.T,
    )
    restored, incoming = pl.pallas_call(
        block_kernel,
        out_shape=(
            jax.ShapeDtypeStruct((channels, rows, cols), BF),
            jax.ShapeDtypeStruct(tile_shape, BF),
        ),
        in_specs=[smem] + [pl.BlockSpec(memory_space=pltpu.HBM)] * len(operands),
        out_specs=(vmem, vmem),
        scratch_shapes=[
            pltpu.SMEM(operands[0].shape, jnp.int32),
            pltpu.SMEM(operands[1].shape, jnp.int32),
            pltpu.SMEM(operands[2].shape, jnp.int32),
            pltpu.VMEM(operands[0].shape, jnp.int32),
            *(pltpu.VMEM(operand.shape, operand.dtype) for operand in operands[3:]),
            pltpu.SemaphoreType.DMA((len(operands) + 1,)),
            pltpu.VMEM((halves, channels * rows, LANES), F32),
            pltpu.VMEM(nxt_shape, BF),
            pltpu.VMEM(nxt_shape, BF),
            pltpu.VMEM(nxt_shape, BF),
            pltpu.VMEM((2 * groups, channels, SHIFT * PART), BF),
            pltpu.VMEM((8, LANES), jnp.int32),
            pltpu.VMEM((8, LANES), jnp.int32),
            pltpu.VMEM((3 * DEPTH, channels), BF),
            pltpu.VMEM((channels, DEPTH), BF),
            pltpu.VMEM((hidden_weight.shape[1], channels), BF),
            pltpu.VMEM((2, channels, LANES), F32),
            pltpu.VMEM((8 * WIN, LANES), F32),
            pltpu.VMEM((4, TOK, QUERIES), F32),
            pltpu.VMEM((SIZE, SIZE), BF),
            pltpu.VMEM((2, cols, cols), BF),
            pltpu.VMEM((groups, channels, SIZE), BF),
            pltpu.VMEM((groups, channels, SIZE), BF),
            pltpu.VMEM((halves, rows, channels, LANES), BF),
            pltpu.VMEM((tiles, channels + 4, LANES), BF),
            pltpu.VMEM(tile_shape, BF),
            pltpu.SemaphoreType.DMA((groups + 5,)),
            pltpu.SemaphoreType.DMA((groups + 5,)),
            pltpu.SemaphoreType.DMA((bands * pairs,)),
            pltpu.SemaphoreType.DMA((bands * pairs,)),
        ],
        compiler_params=pltpu.CompilerParams(
            vmem_limit_bytes=40 * 1024 * 1024, collective_id=0, has_side_effects=True
        ),
        cost_estimate=pl.CostEstimate(flops=10**10, bytes_accessed=10**7, transcendentals=10**6),
        name="block",
    )(band_counts, *(pltpu.with_memory_space_constraint(value, pltpu.HBM) for value in operands))
    restored, work = pl.pallas_call(
        place_kernel,
        out_shape=(
            jax.ShapeDtypeStruct((channels, rows, cols), BF),
            jax.ShapeDtypeStruct((channels, CAP, TILE * TOK), BF),
        ),
        in_specs=[vmem, vmem],
        out_specs=(pl.BlockSpec(memory_space=pl.ANY), pl.BlockSpec(memory_space=pl.ANY)),
        scratch_shapes=[
            pltpu.VMEM((channels * CAP, TILE * TOK), F32),
            pltpu.VMEM((channels, CAP, TILE * TOK), BF),
            pltpu.SemaphoreType.DMA((2, -(-channels // CUT))),
        ],
        compiler_params=pltpu.CompilerParams(vmem_limit_bytes=16 * 1024 * 1024),
        name="place",
    )(incoming, restored)
    return jnp.transpose(restored, (1, 2, 0)), jnp.transpose(work, (1, 2, 0))


def solution(mesh):
    split = P(("img", "band"))
    in_specs = (split,) * 5 + (P(),) * 7
    return jax.shard_map(shards, mesh=mesh, in_specs=in_specs, out_specs=(split, split), check_vma=False)
```

```python
import jax
import jax.numpy as jnp
from jax import lax
from jax.experimental import pallas as pl
from jax.experimental.pallas import tpu as pltpu
from jax.sharding import PartitionSpec as P

CHAN = 180
HEADS = 6
WIN = 8
TILE = 2
SHIFT = 4
CAP = 8
TOK = WIN * WIN
HALF = TOK // 2
HEAD_DIM = CHAN // HEADS
GROUP = 8
WIDER = 2
SIZE = GROUP * TOK
AHEAD = 4
CUT = 60
PART = GROUP * WIN
PAD = 32
DEPTH = HEADS * PAD
QUERIES = HEADS * TOK
LANES = 128
SLOT_LANE = 120

EPSILON = 1e-05
BF = jnp.bfloat16
F32 = jnp.float32


def layer_norm(values, gain):
    center = values - jnp.sum(values, axis=0, keepdims=True) * (1.0 / CHAN)
    spread = jnp.sum(center * center, axis=0, keepdims=True) * (1.0 / CHAN)
    scaled = center * lax.rsqrt(spread + EPSILON)
    parts = [scaled[:, i : i + LANES] * gain for i in range(0, values.shape[1], LANES)]
    return jnp.concatenate(parts, axis=1).astype(BF)


def dot(a, b):
    return jnp.dot(a, b, preferred_element_type=F32)


def dot_t(a, b):
    return lax.dot_general(a, b, (((1,), (1,)), ((), ())), preferred_element_type=F32)


def iota(shape, axis):
    return lax.broadcasted_iota(jnp.int32, shape, axis)


def bias_strips(table, strips):
    heads, entries = table.shape
    values = jnp.concatenate([table[...], jnp.zeros((8 - heads, entries), F32)], axis=0)
    high = values.astype(BF).astype(F32)
    middle = (values - high).astype(BF).astype(F32)
    low = values - high - middle
    parts = jnp.concatenate([high, middle, low], axis=0).astype(BF)
    shape = (entries, WIN * LANES)
    entry, lane = iota(shape, 0), iota(shape, 1)
    step = (lane % LANES) // WIN
    wanted = step * (2 * WIN - 1) + lane % WIN - lane // LANES + WIN - 1
    pick = jnp.where((entry == wanted) & (step < 2 * WIN - 1), 1.0, 0.0).astype(BF)
    found = dot(parts, pick)
    found = found[0:8] + found[8:16] + found[16:24]
    for c in range(WIN):
        strips[pl.ds(c, 8, stride=WIN), :] = found[:, c * LANES : (c + 1) * LANES]


def bias_fill(strips, bias, own_last, prev_last):
    first_half = iota((WIN, LANES), 1) < TOK
    for r in range(WIN):
        by = 2 * LANES - (WIN - 1 - r) * WIN
        tiles = []
        for h in range(0, HEADS, 2):
            even = strips[h * WIN : (h + 1) * WIN, :]
            odd = strips[(h + 1) * WIN : (h + 2) * WIN, :]
            tiles.append(
                jnp.where(
                    first_half,
                    pltpu.roll(even, by % LANES, 1),
                    pltpu.roll(odd, (by + TOK) % LANES, 1),
                )
            )
        base = jnp.concatenate(tiles, axis=1)
        shape = (WIN, QUERIES)
        key, query = iota(shape, 0), iota(shape, 1) % TOK
        rows_differ = (query // WIN >= SHIFT) != (r >= SHIFT)
        cols_differ = (key >= SHIFT) != (query % WIN >= SHIFT)
        rows = slice(r * WIN, (r + 1) * WIN)
        for k, last in enumerate((own_last, prev_last)):
            row_pen = jnp.where(rows_differ, jnp.where(last, -100.0, 0.0).astype(F32), 0.0)
            bias[2 * k, rows] = base + row_pen
            bias[2 * k + 1, rows] = base + jnp.where(cols_differ, -100.0, row_pen)


def spread_heads(rows, cols):
    row, col = iota((rows, cols), 0), iota((rows, cols), 1)
    inside = row % DEPTH
    wanted = row // DEPTH * CHAN + inside // PAD * HEAD_DIM + inside % PAD
    return jnp.where((inside % PAD < HEAD_DIM) & (wanted == col), 1.0, 0.0).astype(BF)


def attend(x, gain, w_in, w_out, bias_of):
    normed = layer_norm(x, gain)
    mixed = dot(w_in, normed)
    q = mixed[0:DEPTH] * HEAD_DIM ** (-0.5)
    k = mixed[DEPTH : 2 * DEPTH].T.astype(BF)
    v = mixed[2 * DEPTH :].astype(BF)
    low = iota((PAD, LANES), 1) < TOK
    blank = jnp.zeros((PAD, LANES), F32)
    none = jnp.zeros((TOK, LANES), BF)

    def weigh(pair):
        lanes = slice(pair * LANES, (pair + 1) * LANES)
        q_pair = q[:, lanes]
        q_turn = pltpu.roll(q_pair, TOK, 1)
        weights = []
        for side in range(2):
            g = 2 * pair + side
            blocks = []
            for h in range(HEADS):
                part = slice(h * PAD, (h + 1) * PAD)
                value = q_pair[part] if h % 2 == side else q_turn[part]
                value = jnp.where(low if h % 2 == 0 else ~low, value, 0.0)
                row = [blank] * (HEADS // 2)
                row[h // 2] = value
                blocks.append(jnp.concatenate(row, axis=1))
            spread_q = jnp.concatenate(blocks, axis=0).astype(BF)
            scores = dot(k[g * TOK : (g + 1) * TOK], spread_q) + bias_of(g)
            top = jnp.max(scores, axis=0, keepdims=True)
            grown = jnp.exp(scores - top)
            weights.append((grown * (1.0 / jnp.sum(grown, axis=0, keepdims=True))).astype(BF))
        return weights

    def mix(pair, weights):
        lanes = slice(pair * LANES, (pair + 1) * LANES)
        rows = []
        for j in range(HEADS // 2):
            cut = slice(j * LANES, (j + 1) * LANES)
            both = jnp.concatenate(
                [
                    jnp.concatenate([weights[0][:, cut], none], axis=1),
                    jnp.concatenate([none, weights[1][:, cut]], axis=1),
                ],
                axis=0,
            )
            found = dot(v[2 * j * PAD : 2 * (j + 1) * PAD, lanes], both)
            one, two = found[:, :LANES], found[:, LANES:]
            rows.append(jnp.where(low, one[:PAD], pltpu.roll(two[:PAD], TOK, 1)))
            rows.append(jnp.where(low, pltpu.roll(one[PAD:], TOK, 1), two[PAD:]))
        return jnp.concatenate(rows, axis=0).astype(BF)

    count = x.shape[1] // LANES
    ready, joined = {}, []
    for pair in range(count + AHEAD):
        if pair < count:
            ready[pair] = weigh(pair)
        if pair >= AHEAD:
            joined.append(mix(pair - AHEAD, ready.pop(pair - AHEAD)))
    joined = jnp.concatenate(joined, axis=1)
    return (x + dot(w_out, joined)).astype(BF)


def feed(states, gain, wh, wo):
    flat = states.astype(F32)
    normed = layer_norm(flat, gain)
    inner = jax.nn.gelu(dot(wh, normed)).astype(BF)
    return (flat + dot(wo, inner)).astype(BF)


def window_order():
    shape = (SIZE, SIZE)
    source, target = iota(shape, 0), iota(shape, 1)
    col = source % PART
    row = source // (SIZE // 2) * SHIFT + source % (SIZE // 2) // PART
    wanted = col // WIN * TOK + row * WIN + col % WIN
    return jnp.where(wanted == target, 1.0, 0.0).astype(BF)


def ranks(flags, windows):
    kept = flags.astype(F32)
    other = jnp.where(iota(flags.shape, 1) < windows, 1.0, 0.0) - kept
    tri = (LANES, LANES)
    before = jnp.where(iota(tri, 0) < iota(tri, 1), 1.0, 0.0).astype(BF)
    total = dot(kept.astype(BF), jnp.ones(tri, BF))
    ahead = dot(kept.astype(BF), before)
    return jnp.where(flags == 1, ahead, total + dot(other.astype(BF), before))


def column_order(rank, cols):
    shape = (cols, LANES)
    shifted = (iota(shape, 0) + cols - SHIFT) % cols
    spread = jnp.where(shifted // WIN == iota(shape, 1), jnp.broadcast_to(rank[0:1], shape), 0.0)
    first = dot(spread.astype(BF), jnp.ones((LANES, cols), BF))
    shape = (cols, cols)
    inside = ((iota(shape, 0) + cols - SHIFT) % WIN).astype(F32)
    wanted = first * WIN + inside
    return jnp.where(wanted == iota(shape, 1).astype(F32), 1.0, 0.0).astype(BF)


def swap_parts(one, two):
    front = iota(one.shape, 1) < PART
    even = jnp.where(front, one, pltpu.roll(two, PART, 1))
    return even, jnp.where(front, pltpu.roll(one, PART, 1), two)


def plane_row(planes, row, channels):
    halves = planes.shape[0]
    return jnp.concatenate(
        [planes[h, pl.ds(row, channels, stride=WIN), :] for h in range(halves)], axis=1
    )


def block_kernel(
    count, keep_in, dests_in, slots_in, pixels_in, table_in, gain_a_in, wqkv_in, wp_in,
    gain_m_in, wh_in, wo_in,
    restored, incoming,
    keep, dests, slots, keep_row, pixels, table, gain_a, wqkv, wp, gain_m, wh, wo, loads,
    planes, nxt_out, prv_out, nxt_buf, prv_buf, told, told_buf, w_in, w_out, w_hid, gains,
    strips, bias, order, columns, states, origin, done_rows, packed, outgoing,
    halo_send, halo_recv, tile_send, tile_recv,
):
    bands = lax.axis_size("band")
    me = lax.axis_index("band")
    right, left = lax.rem(me + 1, bands), lax.rem(me + bands - 1, bands)
    channels, rows, cols = pixels.shape
    windows = cols // WIN
    groups = windows // GROUP
    half = bands // 2
    fourth = half // 2
    far = jnp.where(me < half, half, 0)
    near = half - far
    halves = cols // LANES
    tiles = windows // TILE
    pairs = -(-tiles // bands)
    span = min(bands, tiles)
    mesh_id = pl.DeviceIdType.MESH
    moves = [
        pltpu.make_async_copy(source, target, loads.at[i])
        for i, (source, target) in enumerate(
            (
                (keep_in, keep_row), (pixels_in, pixels), (keep_in, keep), (wqkv_in, wqkv), (wp_in, wp),
                (table_in, table), (gain_a_in, gain_a), (gain_m_in, gain_m), (wh_in, wh),
                (wo_in, wo), (dests_in, dests), (slots_in, slots),
            )
        )
    ]
    for move in moves:
        move.start()

    barrier = pltpu.get_barrier_semaphore()

    def greet(i, _):
        peer = lax.rem(me + i, bands)
        pl.semaphore_signal(barrier, inc=1, device_id={"band": peer}, device_id_type=mesh_id)
        return 0

    lax.fori_loop(1, bands, greet, 0)

    live = count[0]
    moves[0].wait()
    told[...] = jnp.zeros(told.shape, jnp.int32)
    told[:, 0:windows] = jnp.broadcast_to(keep_row[...], (8, windows))
    mine = told[...]
    rank = ranks(mine, windows)
    line = iota(told.shape, 0)
    told[...] = jnp.where(line == 0, rank.astype(jnp.int32), live)

    def nxt_copy(c):
        return pltpu.make_async_remote_copy(
            src_ref=nxt_out.at[c],
            dst_ref=nxt_buf.at[c],
            send_sem=halo_send.at[c],
            recv_sem=halo_recv.at[c],
            device_id={"band": left},
            device_id_type=mesh_id,
        )

    odd = lax.rem(me, 2) == 1
    fold = WIDER

    def prv_send(part, source, from_chunk, to_chunk, device, mark):
        first = part * fold
        return pltpu.make_async_remote_copy(
            src_ref=source.at[pl.ds(from_chunk + first, fold)],
            dst_ref=prv_buf.at[pl.ds(to_chunk + first, fold)],
            send_sem=halo_send.at[groups + 1 + 2 * mark + part],
            recv_sem=halo_recv.at[groups + 1 + 2 * mark + part],
            device_id={"band": device},
            device_id_type=mesh_id,
        )

    def direct(part):
        return prv_send(part, prv_out, 0, 0, right, 0)

    def relay(part):
        return prv_send(part, prv_out, 0, groups, lax.rem(me + 2, bands), 1)

    def forward(part):
        return prv_send(part, prv_buf, groups, 0, left, 0)

    told_copy = pltpu.make_async_remote_copy(
        src_ref=told,
        dst_ref=told_buf,
        send_sem=halo_send.at[groups],
        recv_sem=halo_recv.at[groups],
        device_id={"band": right},
        device_id_type=mesh_id,
    )
    pl.semaphore_wait(barrier, bands - 1)
    told_copy.start()
    moves[1].wait()
    moves[2].wait()
    for h in range(halves):
        part = pixels[:, :, h * LANES : (h + 1) * LANES].astype(F32)
        planes[h] = part.reshape(channels * rows, LANES)

    def arrange(first, matrix, target, done):
        moved = [
            dot(plane_row(planes, first + r, channels).astype(BF), matrix) for r in range(SHIFT)
        ]
        for h in range(halves):
            cols_h = slice(h * LANES, (h + 1) * LANES)
            for r in range(0, SHIFT, 2):
                even, uneven = swap_parts(moved[r][:, cols_h], moved[r + 1][:, cols_h])
                lanes = slice(r * PART, (r + 2) * PART)
                target[2 * h, :, lanes] = even.astype(BF)
                target[2 * h + 1, :, lanes] = uneven.astype(BF)
        for h in range(halves):
            done(h)

    columns[0] = column_order(rank, cols)

    def start_relay(h):
        if h == 0:
            direct(0).start()
            return

        @pl.when(odd)
        def _():
            relay(1).start()

    def start_nxt(h):
        nxt_copy(2 * h).start()
        nxt_copy(2 * h + 1).start()

    arrange(rows - SHIFT, columns[0], prv_out, start_relay)
    told_copy.wait()
    news = told_buf[...]
    columns[1] = column_order(news[0:1].astype(F32), cols)
    arrange(0, columns[1], nxt_out, start_nxt)
    live_prev, final_prev = news[1, 0], news[0, windows - 1]
    final_own = jnp.where(keep[0, windows - 1] == 1, live - 1, windows - 1)

    order[...] = window_order()
    for move in moves[3:]:
        move.wait()
    w_in[...] = dot_t(spread_heads(3 * DEPTH, 3 * CHAN), wqkv[...]).astype(BF)
    w_out[...] = dot(spread_heads(DEPTH, CHAN), wp[...]).T.astype(BF)
    w_hid[...] = wh[...].astype(F32).T.astype(BF)
    gains[0] = jnp.broadcast_to(gain_a[...], (LANES, channels)).T
    gains[1] = jnp.broadcast_to(gain_m[...], (LANES, channels)).T
    bias_strips(table, strips)
    bias_fill(strips, bias, me == bands - 1, me == 0)

    padded = channels + 4

    def windows_of(upper_part, lower_part):
        return dot(jnp.concatenate([upper_part, lower_part], axis=1), order[...])

    def attend_windows(x, start, kind, last):
        def edge(g):
            return bias[2 * kind + (start + g == last).astype(jnp.int32)]

        return attend(x, gains[0], w_in[...], w_out[...], edge)

    def step(c, _):
        nxt_copy(c).wait()

        @pl.when((c == 1) & odd)
        def _():
            relay(1).wait()
            forward(1).start()

        @pl.when((c == groups - 1) & ~odd)
        def _():
            direct(1).start()

        x = windows_of(prv_out[c], nxt_buf[c])
        origin[c] = x.astype(BF)
        own = attend_windows(x, c * GROUP, 0, final_own)
        states[c] = own
        wide = jnp.concatenate([own.astype(F32), jnp.zeros((4, SIZE), F32)], axis=0)
        for k in range(SIZE // LANES):
            packed[c * (SIZE // LANES) + k] = wide[:, k * LANES : (k + 1) * LANES].astype(BF)
        return 0

    slot_row = iota((padded, LANES), 0) >= channels
    member = iota((padded, LANES), 1) // TOK

    def pack(index, peer, j):
        t = jnp.int32(0)
        found = jnp.int32(0)
        for i in range(span):
            hit = dests[0, j * span + i] == peer
            t = jnp.where(hit, j * span + i, t)
            found = jnp.where(hit, 1, found)
        known = jnp.where(found > 0, live - t * TILE, 0)
        slot = jnp.where(known > 0, slots[0, t], CAP).astype(F32)
        value = packed[t]
        value = jnp.where(member < known, value, jnp.zeros_like(value))
        outgoing[index] = jnp.where(slot_row, jnp.full((padded, LANES), slot, F32).astype(BF), value)

    def peer_of(n):
        away = n >= half
        m = jnp.where(away, n - half + 1, n)
        cross = (m >= fourth).astype(jnp.int32)
        row = lax.rem(lax.div(lax.rem(me, half), 2) + m, fourth)
        side = lax.rem(lax.rem(me, 2) + cross, 2)
        return jnp.where(away, near, far) + 2 * row + side

    def tile_copy(n, j):
        return pltpu.make_async_remote_copy(
            src_ref=outgoing.at[n * pairs + j],
            dst_ref=incoming.at[me * pairs + j],
            send_sem=tile_send.at[n * pairs + j],
            recv_sem=tile_recv.at[n * pairs + j],
            device_id={"band": peer_of(n)},
            device_id_type=mesh_id,
        )

    stage = groups // pairs

    def round_of(j, _):
        lax.fori_loop(j * stage, (j + 1) * stage, step, 0)

        def dispatch(n, _):
            pack(n * pairs + j, peer_of(n), j)

            @pl.when(n > 0)
            def _():
                tile_copy(n - 1, j).start()

            return 0

        lax.fori_loop(0, bands - 1, dispatch, 0)
        kept_here = (bands - 1) * pairs + j
        pack(kept_here, me, j)
        tile_copy(bands - 2, j).start()
        incoming[me * pairs + j] = outgoing[kept_here]
        return 0

    lax.fori_loop(0, pairs, round_of, 0)

    lane = iota((channels, WIDER * SIZE), 1)
    upper = lane % TOK < HALF

    def finish(i, _):
        direct(i).wait_recv()

        @pl.when(~odd | (i == 0))
        def _():
            direct(i).wait_send()

        @pl.when(odd & (i > 0))
        def _():
            forward(i).wait_send()

        number = WIDER * GROUP
        chunks = [i * WIDER + k for k in range(WIDER)]
        x = jnp.concatenate([windows_of(prv_buf[c], nxt_out[c]) for c in chunks], axis=1)
        prev = attend_windows(x, i * number, 1, final_prev)
        own = jnp.concatenate([states[c] for c in chunks], axis=1)
        done = feed(jnp.where(upper, own, prev), gains[1], w_hid[...], wo[...])
        before = jnp.concatenate([origin[c] for c in chunks], axis=1)
        before = jnp.where(upper, before, x.astype(BF))
        position = i * number + lane // TOK
        chosen = position < jnp.where(upper, live, live_prev)
        after = jnp.where(chosen, done, before)
        one, two = (dot_t(after[:, k * SIZE : (k + 1) * SIZE], order[...]) for k in range(WIDER))
        for k in range(SIZE // LANES):
            cut = slice(k * LANES, (k + 1) * LANES)
            even, uneven = swap_parts(one[:, cut], two[:, cut])
            r = (2 * k + SHIFT) % rows
            done_rows[i, r] = even.astype(BF)
            done_rows[i, r + 1] = uneven.astype(BF)
        return 0

    lax.fori_loop(0, groups // WIDER, finish, 0)
    for r in range(rows):
        row = jnp.concatenate([done_rows[h, r] for h in range(halves)], axis=1)
        row = dot_t(row, columns[0] if r >= rows - SHIFT else columns[1])
        for h in range(halves):
            planes[h, pl.ds(r, channels, stride=WIN), :] = row[:, h * LANES : (h + 1) * LANES]
    for h in range(halves):
        restored[:, :, h * LANES : (h + 1) * LANES] = (
            planes[h].reshape(channels, rows, LANES).astype(BF)
        )

    def collect(i, _):
        for j in range(pairs):
            tile_copy(i, j).wait()
        return 0

    lax.fori_loop(0, bands - 1, collect, 0)


def place_kernel(incoming, restored, restored_out, work_out, planes, work, sems):
    total, padded, _ = incoming.shape
    channels = work.shape[0]
    blocks = range(0, channels, CUT)
    moves = [
        pltpu.make_async_copy(restored.at[b : b + CUT], restored_out.at[b : b + CUT], sems.at[0, i])
        for i, b in enumerate(blocks)
    ]
    for move in moves:
        move.start()
    head = incoming[:, padded - 8 :, :].astype(F32)
    head = jnp.max(jnp.where(iota(head.shape, 1) >= 4, head, 0.0), axis=1)
    slot = jnp.max(head, axis=1, keepdims=True).astype(jnp.int32)
    match = slot == iota((total, LANES), 1)
    source = jnp.where(match, iota((total, LANES), 0), -1).astype(F32)
    source = jnp.max(source, axis=0, keepdims=True).astype(jnp.int32)
    chosen = [source[0, k] for k in range(CAP)]
    sent = []
    for i, b in enumerate(blocks):
        for k in range(CAP):
            block = incoming[jnp.maximum(chosen[k], 0), b : b + CUT].astype(F32)
            block = jnp.where(chosen[k] >= 0, block, 0.0)
            planes[pl.ds(b * CAP + k, CUT, stride=CAP), :] = block
        value = planes[b * CAP : (b + CUT) * CAP].reshape(CUT, CAP, TILE * TOK)
        work[b : b + CUT] = value.astype(BF)
        sent.append(
            pltpu.make_async_copy(work.at[b : b + CUT], work_out.at[b : b + CUT], sems.at[1, i])
        )
        sent[-1].start()
    for move in moves:
        move.wait()
    for move in sent:
        move.wait()


def shards(
    pixels, keep_mask, band_counts, plan_dest, plan_slot, bias_table, gain_attn, qkv_weight,
    proj_weight, gain_mlp, hidden_weight, output_weight,
):
    bands = lax.axis_size("band")
    rows, cols, channels = pixels.shape
    windows = cols // WIN
    halves = cols // LANES
    tiles = windows // TILE
    pairs = -(-tiles // bands)
    smem = pl.BlockSpec(memory_space=pltpu.SMEM)
    vmem = pl.BlockSpec(memory_space=pltpu.VMEM)
    tile_shape = (bands * pairs, channels + 4, LANES)
    groups = windows // GROUP
    nxt_shape = (groups, channels, SHIFT * PART)
    operands = (
        keep_mask, plan_dest, plan_slot, jnp.transpose(pixels, (2, 0, 1)),
        bias_table.T, gain_attn[None], qkv_weight, proj_weight, gain_mlp[None], hidden_weight,
        output_weight.T,
    )
    restored, incoming = pl.pallas_call(
        block_kernel,
        out_shape=(
            jax.ShapeDtypeStruct((channels, rows, cols), BF),
            jax.ShapeDtypeStruct(tile_shape, BF),
        ),
        in_specs=[smem] + [pl.BlockSpec(memory_space=pltpu.HBM)] * len(operands),
        out_specs=(vmem, vmem),
        scratch_shapes=[
            pltpu.SMEM(operands[0].shape, jnp.int32),
            pltpu.SMEM(operands[1].shape, jnp.int32),
            pltpu.SMEM(operands[2].shape, jnp.int32),
            pltpu.VMEM(operands[0].shape, jnp.int32),
            *(pltpu.VMEM(operand.shape, operand.dtype) for operand in operands[3:]),
            pltpu.SemaphoreType.DMA((len(operands) + 1,)),
            pltpu.VMEM((halves, channels * rows, LANES), F32),
            pltpu.VMEM(nxt_shape, BF),
            pltpu.VMEM(nxt_shape, BF),
            pltpu.VMEM(nxt_shape, BF),
            pltpu.VMEM((2 * groups, channels, SHIFT * PART), BF),
            pltpu.VMEM((8, LANES), jnp.int32),
            pltpu.VMEM((8, LANES), jnp.int32),
            pltpu.VMEM((3 * DEPTH, channels), BF),
            pltpu.VMEM((channels, DEPTH), BF),
            pltpu.VMEM((hidden_weight.shape[1], channels), BF),
            pltpu.VMEM((2, channels, LANES), F32),
            pltpu.VMEM((8 * WIN, LANES), F32),
            pltpu.VMEM((4, TOK, QUERIES), F32),
            pltpu.VMEM((SIZE, SIZE), BF),
            pltpu.VMEM((2, cols, cols), BF),
            pltpu.VMEM((groups, channels, SIZE), BF),
            pltpu.VMEM((groups, channels, SIZE), BF),
            pltpu.VMEM((halves, rows, channels, LANES), BF),
            pltpu.VMEM((tiles, channels + 4, LANES), BF),
            pltpu.VMEM(tile_shape, BF),
            pltpu.SemaphoreType.DMA((groups + 5,)),
            pltpu.SemaphoreType.DMA((groups + 5,)),
            pltpu.SemaphoreType.DMA((bands * pairs,)),
            pltpu.SemaphoreType.DMA((bands * pairs,)),
        ],
        compiler_params=pltpu.CompilerParams(
            vmem_limit_bytes=40 * 1024 * 1024, collective_id=0, has_side_effects=True
        ),
        cost_estimate=pl.CostEstimate(flops=10**10, bytes_accessed=10**7, transcendentals=10**6),
        name="block",
    )(band_counts, *(pltpu.with_memory_space_constraint(value, pltpu.HBM) for value in operands))
    restored, work = pl.pallas_call(
        place_kernel,
        out_shape=(
            jax.ShapeDtypeStruct((channels, rows, cols), BF),
            jax.ShapeDtypeStruct((channels, CAP, TILE * TOK), BF),
        ),
        in_specs=[vmem, vmem],
        out_specs=(pl.BlockSpec(memory_space=pl.ANY), pl.BlockSpec(memory_space=pl.ANY)),
        scratch_shapes=[
            pltpu.VMEM((channels * CAP, TILE * TOK), F32),
            pltpu.VMEM((channels, CAP, TILE * TOK), BF),
            pltpu.SemaphoreType.DMA((2, -(-channels // CUT))),
        ],
        compiler_params=pltpu.CompilerParams(vmem_limit_bytes=16 * 1024 * 1024),
        name="place",
    )(incoming, restored)
    return jnp.transpose(restored, (1, 2, 0)), jnp.transpose(work, (1, 2, 0))


def solution(mesh):
    split = P(("img", "band"))
    in_specs = (split,) * 5 + (P(),) * 7
    return jax.shard_map(shards, mesh=mesh, in_specs=in_specs, out_specs=(split, split), check_vma=False)
```
